32 devices in a mesh: depth: 4 (over z), col: 2 (over y), row: 4 (over x, core).
Axes of the slice: x: 2, y: 2, z: 4, core: 2. Of those that a mesh axis runs over, the one named last changes fastest.
Arguments:
- reach_in: bfloat16 [2048, 2048], P(('row', 'depth'), 'col')
Outputs:
- output: bfloat16 [2048, 2048], P(('row', 'depth'), 'col')
All inputs are finite; a program needn't handle non-finite values.
Results may differ from the reference program's by a relative error of at most 0.001.
Values are sent between devices in bfloat16 or wider.
A program may use at most 1 GiB of HBM per device.

```python
import jax
import jax.numpy as jnp
from jax import lax

N = 2048
SQUARINGS = 4


def setup_inputs(seed: int = 0) -> dict:
    root_key = jax.random.key(seed)
    position = jax.random.permutation(root_key, N)
    chain_edges = position[None, :] == position[:, None] + 1
    return {'reach_in': chain_edges.astype(jnp.float32).astype(jnp.bfloat16)}


def reference(reach_in):
    def square_once(current, unused_x):
        path_count = jnp.dot(current, current, preferred_element_type=jnp.float32)
        next_reach = jnp.minimum(path_count + current.astype(jnp.float32), 1.0).astype(jnp.bfloat16)
        return next_reach, None
    final_reach, unused_ys = lax.scan(square_once, reach_in, None, length=SQUARINGS)
    return final_reach
```

```python
import jax
import jax.numpy as jnp
from jax import lax
from jax.experimental import pallas as pl
from jax.experimental.pallas import tpu as pltpu
from jax.sharding import PartitionSpec as P

N = 2048
SLAB = 128
HALF = 1024
STEPS = 15
MESH = pl.DeviceIdType.MESH

PIECES = (('zxy', 0, 48), ('zyx', 48, 48), ('xyz', 96, 16), ('yxz', 112, 16))
END_ORDER = (
    1, 4, 8, 17, 20, 24, 33, 36, 40, 49, 52, 56, 2, 9, 5, 12, 18, 25, 28, 34, 37, 41, 21, 44, 60, 57, 50, 53, 10, 6,
    13, 3, 26, 19, 22, 29, 35, 38, 42, 58, 14, 11, 51, 54, 7, 27, 39, 43, 55, 59, 23, 30, 45, 61, 47, 15, 63, 46, 62, 31,
)
MID_ORDER = (
    1, 2, 4, 8, 17, 18, 20, 24, 33, 34, 36, 40, 49, 50, 52, 56, 3, 37, 41, 9, 10, 53, 57, 5, 6, 19, 12, 35, 38, 42,
    58, 51, 54, 25, 26, 28, 21, 22, 39, 43, 45, 61, 55, 59, 44, 60, 7, 11, 47, 63, 46, 27, 62, 13, 14, 29, 30, 23, 15, 31,
)


def forwards(order, dx, dy, k, end):
    far = {'x': dx == 1, 'y': dy == 1, 'z': k != 0}
    last = max([i for i, axis in enumerate(order) if far[axis]], default=-1)
    hops = []
    for i, axis in enumerate(order):
        if axis == 'z' and i > last:
            hops += ['in'] if end else ['in', 'out']
        elif axis == 'z' and i == last and not end:
            hops += ['in'] if k == 1 else ['out']
        elif i > last:
            hops.append(axis)
    return hops


def kernel(in_ref, out_ref, reach, rows, in_sem, send_sem, recv_sem, pass_sem, got_sem):
    z, y, row = lax.axis_index('depth'), lax.axis_index('col'), lax.axis_index('row')
    x, core = row // 2, row % 2
    upper = z >= 2
    z_in = jnp.where(upper, z - 1, z + 1)
    z_out = jnp.where(upper, z + 1, z - 1)
    end = (z == 0) | (z == 3)
    x_row = (1 - x) * 2 + core
    mate_row = x * 2 + 1 - core
    peers = {
        'x': {'depth': z, 'col': y, 'row': x_row},
        'y': {'depth': z, 'col': 1 - y, 'row': row},
        'in': {'depth': z_in, 'col': y, 'row': row},
        'out': {'depth': z_out, 'col': y, 'row': row},
    }
    mate = {'depth': z, 'col': y, 'row': mate_row}

    def slab_at(sx, sy, sz, score):
        return sy, (sx * 2 + score) * 4 + sz

    own_half, own_block = slab_at(x, y, z, core)
    own_row = pl.multiple_of(own_block * SLAB, SLAB)
    load = pltpu.make_async_copy(in_ref, reach.at[own_half, pl.ds(own_row, SLAB), :], in_sem)
    load.start()

    barrier = pltpu.get_barrier_semaphore()
    for name in ('x', 'y', 'in'):
        pl.semaphore_signal(barrier, inc=1, device_id=peers[name], device_id_type=MESH)
    pl.semaphore_signal(barrier, inc=1, device_id=mate, device_id_type=MESH)

    @pl.when(jnp.logical_not(end))
    def _():
        pl.semaphore_signal(barrier, inc=1, device_id=peers['out'], device_id_type=MESH)
        pl.semaphore_wait(barrier, 5)

    @pl.when(end)
    def _():
        pl.semaphore_wait(barrier, 4)

    load.wait()

    def piece_ref(p, sx, sy, sz, score):
        half, block = slab_at(sx, sy, sz, score)
        start = pl.multiple_of(block * SLAB + PIECES[p][1], 16)
        return reach.at[half, pl.ds(start, PIECES[p][2]), :]

    def copy(p, sx, sy, sz, score, peer, send, recv):
        ref = piece_ref(p, sx, sy, sz, score)
        return pltpu.make_async_remote_copy(
            src_ref=ref, dst_ref=ref, send_sem=send, recv_sem=recv, device_id=peer, device_id_type=MESH
        )

    def gather(end_case):
        places = (0, 1, 2, 3) if end_case else (1, 0, 2, 3)

        def source(dx, dy, k):
            sx = (1 - x) if dx else x
            sy = (1 - y) if dy else y
            if k == 0:
                return sx, sy, z
            place = places[k]
            return sx, sy, jnp.where(upper, 3 - place, place)

        sent = [0] * len(PIECES)

        def push(p, dx, dy, k):
            sx, sy, sz = source(dx, dy, k)
            for hop in forwards(PIECES[p][0], dx, dy, k, end_case):
                sent[p] += 1
                copy(p, sx, sy, sz, core, peers[hop], send_sem.at[p], recv_sem.at[p, sx, sy, sz]).start()
            copy(p, sx, sy, sz, core, mate, pass_sem.at[p], got_sem.at[p, sx, sy, sz]).start()

        for p in range(len(PIECES)):
            push(p, 0, 0, 0)
        for code in END_ORDER if end_case else MID_ORDER:
            p, dx, dy, k = code // 16, code // 8 % 2, code // 4 % 2, code % 4
            sx, sy, sz = source(dx, dy, k)
            copy(p, sx, sy, sz, core, mate, send_sem.at[p], recv_sem.at[p, sx, sy, sz]).wait_recv()
            push(p, dx, dy, k)
        for p in range(len(PIECES)):
            drain = copy(p, x, y, z, core, mate, send_sem.at[p], got_sem.at[p, x, y, z])
            for _ in range(sent[p]):
                drain.wait_send()
            drain = copy(p, x, y, z, core, mate, pass_sem.at[p], got_sem.at[p, x, y, z])
            for _ in range(16):
                drain.wait_send()

    @pl.when(end)
    def _():
        gather(True)

    @pl.when(jnp.logical_not(end))
    def _():
        gather(False)

    for p in range(len(PIECES)):
        for sx in range(2):
            for sy in range(2):
                for sz in range(4):
                    copy(p, sx, sy, sz, 1 - core, mate, pass_sem.at[p], got_sem.at[p, sx, sy, sz]).wait_recv()

    for half in range(2):
        rows[0, :, half * HALF:(half + 1) * HALF] = reach[half, pl.ds(own_row, SLAB), :]

    def block(now, half, start):
        product = jnp.dot(rows[now], reach[half, :, start:start + 256], preferred_element_type=jnp.float32)
        old = rows[now, :, half * HALF + start:half * HALF + start + 256].astype(jnp.float32)
        return jnp.minimum(product + old, 1.0).astype(jnp.bfloat16)

    def two_steps(_, carry):
        for now in range(2):
            for half in range(2):
                for start in range(0, HALF, 256):
                    column = half * HALF + start
                    rows[1 - now, :, column:column + 256] = block(now, half, start)
        return carry

    lax.fori_loop(0, STEPS // 2, two_steps, 0)

    for half in range(2):
        @pl.when(y == half)
        def _():
            for start in range(0, HALF, 256):
                out_ref[:, start:start + 256] = block(0, half, start)


def solution(mesh):
    layout = P(('row', 'depth'), 'col')
    sends = len(PIECES)

    def local(slab):
        return pl.pallas_call(
            kernel,
            out_shape=jax.ShapeDtypeStruct((SLAB, HALF), jnp.bfloat16),
            in_specs=[pl.BlockSpec(memory_space=pl.ANY)],
            out_specs=pl.BlockSpec(memory_space=pltpu.VMEM),
            scratch_shapes=[
                pltpu.VMEM((2, N, HALF), jnp.bfloat16),
                pltpu.VMEM((2, SLAB, N), jnp.bfloat16),
                pltpu.SemaphoreType.DMA,
                pltpu.SemaphoreType.DMA((sends,)),
                pltpu.SemaphoreType.DMA((sends, 2, 2, 4)),
                pltpu.SemaphoreType.DMA((sends,)),
                pltpu.SemaphoreType.DMA((sends, 2, 2, 4)),
            ],
            compiler_params=pltpu.CompilerParams(collective_id=0, has_side_effects=True),
        )(slab)

    return jax.shard_map(local, mesh=mesh, in_specs=(layout,), out_specs=layout, check_vma=False)
```

```python
import jax
import jax.numpy as jnp
from jax import lax
from jax.experimental import pallas as pl
from jax.experimental.pallas import tpu as pltpu
from jax.sharding import PartitionSpec as P

N = 2048
SLAB = 128
HALF = 1024
STEPS = 15
MESH = pl.DeviceIdType.MESH

PIECES = (('zxy', 0, 48), ('zyx', 48, 48), ('xyz', 96, 16), ('yxz', 112, 16))
END_ORDER = (
    1, 4, 8, 17, 20, 24, 33, 36, 40, 49, 52, 56, 2, 9, 5, 12, 18, 25, 28, 34, 37, 41, 21, 44, 60, 57, 50, 53, 10, 6,
    13, 3, 26, 19, 22, 29, 35, 38, 42, 58, 14, 11, 51, 54, 7, 27, 39, 43, 55, 59, 23, 30, 45, 61, 47, 15, 63, 46, 62, 31,
)
MID_ORDER = (
    1, 2, 4, 8, 17, 18, 20, 24, 33, 34, 36, 40, 49, 50, 52, 56, 3, 37, 41, 9, 10, 53, 57, 5, 6, 19, 12, 35, 38, 42,
    58, 51, 54, 25, 26, 28, 21, 22, 39, 43, 45, 61, 55, 59, 44, 60, 7, 11, 47, 63, 46, 27, 62, 13, 14, 29, 30, 23, 15, 31,
)


def forwards(order, dx, dy, k, end):
    far = {'x': dx == 1, 'y': dy == 1, 'z': k != 0}
    last = max([i for i, axis in enumerate(order) if far[axis]], default=-1)
    hops = []
    for i, axis in enumerate(order):
        if axis == 'z' and i > last:
            hops += ['in'] if end else ['in', 'out']
        elif axis == 'z' and i == last and not end:
            hops += ['in'] if k == 1 else ['out']
        elif i > last:
            hops.append(axis)
    return hops


def kernel(in_ref, out_ref, reach, rows, in_sem, send_sem, recv_sem, pass_sem, got_sem):
    z, y, row = lax.axis_index('depth'), lax.axis_index('col'), lax.axis_index('row')
    x, core = row // 2, row % 2
    upper = z >= 2
    z_in = jnp.where(upper, z - 1, z + 1)
    z_out = jnp.where(upper, z + 1, z - 1)
    end = (z == 0) | (z == 3)
    x_row = (1 - x) * 2 + core
    mate_row = x * 2 + 1 - core
    peers = {
        'x': {'depth': z, 'col': y, 'row': x_row},
        'y': {'depth': z, 'col': 1 - y, 'row': row},
        'in': {'depth': z_in, 'col': y, 'row': row},
        'out': {'depth': z_out, 'col': y, 'row': row},
    }
    mate = {'depth': z, 'col': y, 'row': mate_row}

    def slab_at(sx, sy, sz, score):
        return sy, (sx * 2 + score) * 4 + sz

    own_half, own_block = slab_at(x, y, z, core)
    own_row = pl.multiple_of(own_block * SLAB, SLAB)
    load = pltpu.make_async_copy(in_ref, reach.at[own_half, pl.ds(own_row, SLAB), :], in_sem)
    load.start()

    barrier = pltpu.get_barrier_semaphore()
    for name in ('x', 'y', 'in'):
        pl.semaphore_signal(barrier, inc=1, device_id=peers[name], device_id_type=MESH)
    pl.semaphore_signal(barrier, inc=1, device_id=mate, device_id_type=MESH)

    @pl.when(jnp.logical_not(end))
    def _():
        pl.semaphore_signal(barrier, inc=1, device_id=peers['out'], device_id_type=MESH)
        pl.semaphore_wait(barrier, 5)

    @pl.when(end)
    def _():
        pl.semaphore_wait(barrier, 4)

    load.wait()

    def piece_ref(p, sx, sy, sz, score):
        half, block = slab_at(sx, sy, sz, score)
        start = pl.multiple_of(block * SLAB + PIECES[p][1], 16)
        return reach.at[half, pl.ds(start, PIECES[p][2]), :]

    def copy(p, sx, sy, sz, score, peer, send, recv):
        ref = piece_ref(p, sx, sy, sz, score)
        return pltpu.make_async_remote_copy(
            src_ref=ref, dst_ref=ref, send_sem=send, recv_sem=recv, device_id=peer, device_id_type=MESH
        )

    def gather(end_case):
        places = (0, 1, 2, 3) if end_case else (1, 0, 2, 3)

        def source(dx, dy, k):
            sx = (1 - x) if dx else x
            sy = (1 - y) if dy else y
            if k == 0:
                return sx, sy, z
            place = places[k]
            return sx, sy, jnp.where(upper, 3 - place, place)

        sent = [0] * len(PIECES)

        def push(p, dx, dy, k):
            sx, sy, sz = source(dx, dy, k)
            for hop in forwards(PIECES[p][0], dx, dy, k, end_case):
                sent[p] += 1
                copy(p, sx, sy, sz, core, peers[hop], send_sem.at[p], recv_sem.at[p, sx, sy, sz]).start()
            copy(p, sx, sy, sz, core, mate, pass_sem.at[p], got_sem.at[p, sx, sy, sz]).start()

        for p in range(len(PIECES)):
            push(p, 0, 0, 0)
        for code in END_ORDER if end_case else MID_ORDER:
            p, dx, dy, k = code // 16, code // 8 % 2, code // 4 % 2, code % 4
            sx, sy, sz = source(dx, dy, k)
            copy(p, sx, sy, sz, core, mate, send_sem.at[p], recv_sem.at[p, sx, sy, sz]).wait_recv()
            push(p, dx, dy, k)
        for p in range(len(PIECES)):
            drain = copy(p, x, y, z, core, mate, send_sem.at[p], got_sem.at[p, x, y, z])
            for _ in range(sent[p]):
                drain.wait_send()
            drain = copy(p, x, y, z, core, mate, pass_sem.at[p], got_sem.at[p, x, y, z])
            for _ in range(16):
                drain.wait_send()

    @pl.when(end)
    def _():
        gather(True)

    @pl.when(jnp.logical_not(end))
    def _():
        gather(False)

    for p in range(len(PIECES)):
        for sx in range(2):
            for sy in range(2):
                for sz in range(4):
                    copy(p, sx, sy, sz, 1 - core, mate, pass_sem.at[p], got_sem.at[p, sx, sy, sz]).wait_recv()

    for half in range(2):
        rows[0, :, half * HALF:(half + 1) * HALF] = reach[half, pl.ds(own_row, SLAB), :]

    def block(now, half, start):
        product = jnp.dot(rows[now], reach[half, :, start:start + 256], preferred_element_type=jnp.float32)
        old = rows[now, :, half * HALF + start:half * HALF + start + 256].astype(jnp.float32)
        return jnp.minimum(product + old, 1.0).astype(jnp.bfloat16)

    def two_steps(_, carry):
        for now in range(2):
            for half in range(2):
                for start in range(0, HALF, 256):
                    column = half * HALF + start
                    rows[1 - now, :, column:column + 256] = block(now, half, start)
        return carry

    lax.fori_loop(0, STEPS // 2, two_steps, 0)

    for half in range(2):
        @pl.when(y == half)
        def _():
            for start in range(0, HALF, 256):
                out_ref[:, start:start + 256] = block(0, half, start)


def solution(mesh):
    layout = P(('row', 'depth'), 'col')
    sends = len(PIECES)

    def local(slab):
        return pl.pallas_call(
            kernel,
            out_shape=pltpu.VMEM((SLAB, HALF), jnp.bfloat16),
            in_specs=[pl.BlockSpec(memory_space=pl.ANY)],
            out_specs=pl.BlockSpec(memory_space=pltpu.VMEM),
            scratch_shapes=[
                pltpu.VMEM((2, N, HALF), jnp.bfloat16),
                pltpu.VMEM((2, SLAB, N), jnp.bfloat16),
                pltpu.SemaphoreType.DMA,
                pltpu.SemaphoreType.DMA((sends,)),
                pltpu.SemaphoreType.DMA((sends, 2, 2, 4)),
                pltpu.SemaphoreType.DMA((sends,)),
                pltpu.SemaphoreType.DMA((sends, 2, 2, 4)),
            ],
            compiler_params=pltpu.CompilerParams(collective_id=0, has_side_effects=True),
        )(slab)

    return jax.shard_map(local, mesh=mesh, in_specs=(layout,), out_specs=layout, check_vma=False)
```

```python
import jax
import jax.numpy as jnp
from jax import lax
from jax.experimental import pallas as pl
from jax.experimental.pallas import tpu as pltpu
from jax.sharding import PartitionSpec as P

N = 2048
SLAB = 128
HALF = 1024
STEPS = 15
MESH = pl.DeviceIdType.MESH

PIECES = (
    ('zxy', 0, 32, 0, 1024),
    ('zxy', 96, 32, 0, 128),
    ('zyx', 32, 32, 0, 1024),
    ('zyx', 64, 16, 0, 1024),
    ('zxy', 80, 16, 0, 1024),
    ('xyz', 96, 16, 128, 896),
    ('yxz', 112, 16, 128, 896),
)
END_ORDER = (
    1, 4, 8, 17, 20, 24, 33, 36, 40, 49, 52, 56, 65, 68, 72, 81, 84, 88, 97, 100, 104, 2, 9, 18, 25, 5, 12, 34, 21,
    28, 50, 41, 44, 66, 37, 53, 57, 60, 82, 85, 89, 69, 76, 73, 108, 92, 98, 101, 105, 10, 26, 6, 13, 3, 19, 42, 22,
    29, 58, 35, 74, 51, 38, 67, 54, 45, 70, 61, 83, 86, 90, 77, 11, 27, 14, 99, 102, 30, 106, 43, 7, 87, 91, 23, 59,
    103, 107, 39, 46, 78, 109, 75, 93, 55, 62, 111, 71, 95, 110, 15, 31, 47, 94, 79, 63,
)
MID_ORDER = (
    1, 2, 4, 8, 17, 18, 20, 24, 33, 34, 36, 40, 49, 50, 52, 56, 65, 66, 68, 72, 81, 82, 84, 88, 97, 98, 100, 104, 3,
    19, 9, 10, 85, 89, 5, 6, 12, 35, 25, 26, 51, 101, 105, 67, 21, 22, 28, 83, 86, 90, 41, 42, 44, 37, 38, 99, 102,
    106, 53, 54, 60, 57, 58, 87, 91, 109, 103, 107, 76, 69, 70, 73, 74, 93, 108, 92, 11, 111, 27, 95, 7, 110, 43,
    23, 13, 14, 94, 59, 75, 29, 30, 39, 45, 46, 55, 71, 61, 62, 77, 78, 47, 15, 63, 31, 79,
)


def forwards(order, dx, dy, k, end):
    far = {'x': dx == 1, 'y': dy == 1, 'z': k != 0}
    last = max([i for i, axis in enumerate(order) if far[axis]], default=-1)
    hops = []
    for i, axis in enumerate(order):
        if axis == 'z' and i > last:
            hops += ['in'] if end else ['in', 'out']
        elif axis == 'z' and i == last and not end:
            hops += ['in'] if k == 1 else ['out']
        elif i > last:
            hops.append(axis)
    return hops


def kernel(in_ref, out_ref, reach, rows, in_sem, send_sem, recv_sem, pass_sem, got_sem):
    z, y, row = lax.axis_index('depth'), lax.axis_index('col'), lax.axis_index('row')
    x, core = row // 2, row % 2
    upper = z >= 2
    z_in = jnp.where(upper, z - 1, z + 1)
    z_out = jnp.where(upper, z + 1, z - 1)
    end = (z == 0) | (z == 3)
    x_row = (1 - x) * 2 + core
    mate_row = x * 2 + 1 - core
    peers = {
        'x': {'depth': z, 'col': y, 'row': x_row},
        'y': {'depth': z, 'col': 1 - y, 'row': row},
        'in': {'depth': z_in, 'col': y, 'row': row},
        'out': {'depth': z_out, 'col': y, 'row': row},
    }
    mate = {'depth': z, 'col': y, 'row': mate_row}

    def slab_at(sx, sy, sz, score):
        return sy, (sx * 2 + score) * 4 + sz

    own_half, own_block = slab_at(x, y, z, core)
    own_row = pl.multiple_of(own_block * SLAB, SLAB)
    load = pltpu.make_async_copy(in_ref, reach.at[own_half, pl.ds(own_row, SLAB), :], in_sem)
    load.start()

    barrier = pltpu.get_barrier_semaphore()
    for name in ('x', 'y', 'in'):
        pl.semaphore_signal(barrier, inc=1, device_id=peers[name], device_id_type=MESH)
    pl.semaphore_signal(barrier, inc=1, device_id=mate, device_id_type=MESH)

    @pl.when(jnp.logical_not(end))
    def _():
        pl.semaphore_signal(barrier, inc=1, device_id=peers['out'], device_id_type=MESH)
        pl.semaphore_wait(barrier, 5)

    @pl.when(end)
    def _():
        pl.semaphore_wait(barrier, 4)

    load.wait()

    def piece_ref(p, sx, sy, sz, score):
        half, block = slab_at(sx, sy, sz, score)
        _, first, count, column, width = PIECES[p]
        start = pl.multiple_of(block * SLAB + first, 16)
        return reach.at[half, pl.ds(start, count), pl.ds(column, width)]

    def copy(p, sx, sy, sz, score, peer, send, recv):
        ref = piece_ref(p, sx, sy, sz, score)
        return pltpu.make_async_remote_copy(
            src_ref=ref, dst_ref=ref, send_sem=send, recv_sem=recv, device_id=peer, device_id_type=MESH
        )

    def gather(end_case):
        places = (0, 1, 2, 3) if end_case else (1, 0, 2, 3)

        def source(dx, dy, k):
            sx = (1 - x) if dx else x
            sy = (1 - y) if dy else y
            if k == 0:
                return sx, sy, z
            place = places[k]
            return sx, sy, jnp.where(upper, 3 - place, place)

        sent = [0] * len(PIECES)

        def push(p, dx, dy, k):
            sx, sy, sz = source(dx, dy, k)
            for hop in forwards(PIECES[p][0], dx, dy, k, end_case):
                sent[p] += 1
                copy(p, sx, sy, sz, core, peers[hop], send_sem.at[p], recv_sem.at[p, sx, sy, sz]).start()
            copy(p, sx, sy, sz, core, mate, pass_sem.at[p], got_sem.at[p, sx, sy, sz]).start()

        for p in range(len(PIECES)):
            push(p, 0, 0, 0)
        for code in END_ORDER if end_case else MID_ORDER:
            p, dx, dy, k = code // 16, code // 8 % 2, code // 4 % 2, code % 4
            sx, sy, sz = source(dx, dy, k)
            copy(p, sx, sy, sz, core, mate, send_sem.at[p], recv_sem.at[p, sx, sy, sz]).wait_recv()
            push(p, dx, dy, k)
        for p in range(len(PIECES)):
            drain = copy(p, x, y, z, core, mate, send_sem.at[p], got_sem.at[p, x, y, z])
            for _ in range(sent[p]):
                drain.wait_send()
            drain = copy(p, x, y, z, core, mate, pass_sem.at[p], got_sem.at[p, x, y, z])
            for _ in range(16):
                drain.wait_send()

    @pl.when(end)
    def _():
        gather(True)

    @pl.when(jnp.logical_not(end))
    def _():
        gather(False)

    for p in range(len(PIECES)):
        for sx in range(2):
            for sy in range(2):
                for sz in range(4):
                    copy(p, sx, sy, sz, 1 - core, mate, pass_sem.at[p], got_sem.at[p, sx, sy, sz]).wait_recv()

    for half in range(2):
        rows[0, :, half * HALF:(half + 1) * HALF] = reach[half, pl.ds(own_row, SLAB), :]

    def block(now, half, start):
        product = jnp.dot(rows[now], reach[half, :, start:start + 256], preferred_element_type=jnp.float32)
        old = rows[now, :, half * HALF + start:half * HALF + start + 256].astype(jnp.float32)
        return jnp.minimum(product + old, 1.0).astype(jnp.bfloat16)

    def two_steps(_, carry):
        for now in range(2):
            for half in range(2):
                for start in range(0, HALF, 256):
                    column = half * HALF + start
                    rows[1 - now, :, column:column + 256] = block(now, half, start)
        return carry

    lax.fori_loop(0, STEPS // 2, two_steps, 0)

    for half in range(2):
        @pl.when(y == half)
        def _():
            for start in range(0, HALF, 256):
                out_ref[:, start:start + 256] = block(0, half, start)


def solution(mesh):
    layout = P(('row', 'depth'), 'col')
    sends = len(PIECES)

    def local(slab):
        return pl.pallas_call(
            kernel,
            out_shape=pltpu.VMEM((SLAB, HALF), jnp.bfloat16),
            in_specs=[pl.BlockSpec(memory_space=pl.ANY)],
            out_specs=pl.BlockSpec(memory_space=pltpu.VMEM),
            scratch_shapes=[
                pltpu.VMEM((2, N, HALF), jnp.bfloat16),
                pltpu.VMEM((2, SLAB, N), jnp.bfloat16),
                pltpu.SemaphoreType.DMA,
                pltpu.SemaphoreType.DMA((sends,)),
                pltpu.SemaphoreType.DMA((sends, 2, 2, 4)),
                pltpu.SemaphoreType.DMA((sends,)),
                pltpu.SemaphoreType.DMA((sends, 2, 2, 4)),
            ],
            compiler_params=pltpu.CompilerParams(collective_id=0, has_side_effects=True),
        )(slab)

    return jax.shard_map(local, mesh=mesh, in_specs=(layout,), out_specs=layout, check_vma=False)
```

```python
import jax
import jax.numpy as jnp
from jax import lax
from jax.experimental import pallas as pl
from jax.experimental.pallas import tpu as pltpu
from jax.sharding import PartitionSpec as P

N = 2048
SLAB = 128
HALF = 1024
STEPS = 15
MESH = pl.DeviceIdType.MESH

PIECES = (('zxy', 0, 48), ('zyx', 48, 48), ('yxz', 96, 32))
END_ORDER = (
    8, 4, 1, 24, 20, 17, 40, 36, 33, 9, 2, 12, 5, 18, 28, 25, 21, 41, 37, 34, 44, 13, 6, 10, 3, 26, 22, 19, 29, 35,
    14, 38, 42, 11, 7, 30, 23, 43, 39, 27, 45, 15, 47, 31, 46,
)
MID_ORDER = (
    1, 8, 4, 2, 17, 24, 20, 18, 33, 40, 36, 34, 3, 9, 10, 5, 41, 37, 19, 6, 12, 35, 38, 42, 25, 26, 28, 21, 22, 39,
    43, 45, 44, 7, 11, 47, 13, 14, 27, 46, 23, 29, 30, 15, 31,
)


def forwards(order, dx, dy, k, end):
    far = {'x': dx == 1, 'y': dy == 1, 'z': k != 0}
    last = max([i for i, axis in enumerate(order) if far[axis]], default=-1)
    hops = []
    for i, axis in enumerate(order):
        if axis == 'z' and i > last:
            hops += ['in'] if end else ['in', 'out']
        elif axis == 'z' and i == last and not end:
            hops += ['in'] if k == 1 else ['out']
        elif i > last:
            hops.append(axis)
    return hops


def kernel(in_ref, out_ref, reach, rows, in_sem, send_sem, recv_sem, pass_sem, got_sem):
    z, y, row = lax.axis_index('depth'), lax.axis_index('col'), lax.axis_index('row')
    x, core = row // 2, row % 2
    upper = z >= 2
    z_in = jnp.where(upper, z - 1, z + 1)
    z_out = jnp.where(upper, z + 1, z - 1)
    end = (z == 0) | (z == 3)
    x_row = (1 - x) * 2 + core
    mate_row = x * 2 + 1 - core
    peers = {
        'x': {'depth': z, 'col': y, 'row': x_row},
        'y': {'depth': z, 'col': 1 - y, 'row': row},
        'in': {'depth': z_in, 'col': y, 'row': row},
        'out': {'depth': z_out, 'col': y, 'row': row},
    }
    mate = {'depth': z, 'col': y, 'row': mate_row}

    def slab_at(sx, sy, sz, score):
        return sy, (sx * 2 + score) * 4 + sz

    own_half, own_block = slab_at(x, y, z, core)
    own_row = pl.multiple_of(own_block * SLAB, SLAB)
    load = pltpu.make_async_copy(in_ref, reach.at[own_half, pl.ds(own_row, SLAB), :], in_sem)
    load.start()

    barrier = pltpu.get_barrier_semaphore()
    for name in ('x', 'y', 'in'):
        pl.semaphore_signal(barrier, inc=1, device_id=peers[name], device_id_type=MESH)
    pl.semaphore_signal(barrier, inc=1, device_id=mate, device_id_type=MESH)

    @pl.when(jnp.logical_not(end))
    def _():
        pl.semaphore_signal(barrier, inc=1, device_id=peers['out'], device_id_type=MESH)
        pl.semaphore_wait(barrier, 5)

    @pl.when(end)
    def _():
        pl.semaphore_wait(barrier, 4)

    load.wait()

    def piece_ref(p, sx, sy, sz, score):
        half, block = slab_at(sx, sy, sz, score)
        start = pl.multiple_of(block * SLAB + PIECES[p][1], 16)
        return reach.at[half, pl.ds(start, PIECES[p][2]), :]

    def copy(p, sx, sy, sz, score, peer, send, recv):
        ref = piece_ref(p, sx, sy, sz, score)
        return pltpu.make_async_remote_copy(
            src_ref=ref, dst_ref=ref, send_sem=send, recv_sem=recv, device_id=peer, device_id_type=MESH
        )

    def gather(end_case):
        places = (0, 1, 2, 3) if end_case else (1, 0, 2, 3)

        def source(dx, dy, k):
            sx = (1 - x) if dx else x
            sy = (1 - y) if dy else y
            if k == 0:
                return sx, sy, z
            place = places[k]
            return sx, sy, jnp.where(upper, 3 - place, place)

        sent = [0] * len(PIECES)

        def push(p, dx, dy, k):
            sx, sy, sz = source(dx, dy, k)
            for hop in forwards(PIECES[p][0], dx, dy, k, end_case):
                sent[p] += 1
                copy(p, sx, sy, sz, core, peers[hop], send_sem.at[p], recv_sem.at[p, sx, sy, sz]).start()
            copy(p, sx, sy, sz, core, mate, pass_sem.at[p], got_sem.at[p, sx, sy, sz]).start()

        for p in range(len(PIECES)):
            push(p, 0, 0, 0)
        for code in END_ORDER if end_case else MID_ORDER:
            p, dx, dy, k = code // 16, code // 8 % 2, code // 4 % 2, code % 4
            sx, sy, sz = source(dx, dy, k)
            copy(p, sx, sy, sz, core, mate, send_sem.at[p], recv_sem.at[p, sx, sy, sz]).wait_recv()
            push(p, dx, dy, k)
        for p in range(len(PIECES)):
            drain = copy(p, x, y, z, core, mate, send_sem.at[p], got_sem.at[p, x, y, z])
            for _ in range(sent[p]):
                drain.wait_send()
            drain = copy(p, x, y, z, core, mate, pass_sem.at[p], got_sem.at[p, x, y, z])
            for _ in range(16):
                drain.wait_send()

    @pl.when(end)
    def _():
        gather(True)

    @pl.when(jnp.logical_not(end))
    def _():
        gather(False)

    for p in range(len(PIECES)):
        for sx in range(2):
            for sy in range(2):
                for sz in range(4):
                    copy(p, sx, sy, sz, 1 - core, mate, pass_sem.at[p], got_sem.at[p, sx, sy, sz]).wait_recv()

    for half in range(2):
        rows[0, :, half * HALF:(half + 1) * HALF] = reach[half, pl.ds(own_row, SLAB), :]

    def block(now, half, start):
        product = jnp.dot(rows[now], reach[half, :, start:start + 256], preferred_element_type=jnp.float32)
        old = rows[now, :, half * HALF + start:half * HALF + start + 256].astype(jnp.float32)
        return jnp.minimum(product + old, 1.0).astype(jnp.bfloat16)

    def two_steps(_, carry):
        for now in range(2):
            for half in range(2):
                for start in range(0, HALF, 256):
                    column = half * HALF + start
                    rows[1 - now, :, column:column + 256] = block(now, half, start)
        return carry

    lax.fori_loop(0, STEPS // 2, two_steps, 0)

    for half in range(2):
        @pl.when(y == half)
        def _():
            for start in range(0, HALF, 256):
                out_ref[:, start:start + 256] = block(0, half, start)


def solution(mesh):
    layout = P(('row', 'depth'), 'col')
    sends = len(PIECES)

    def local(slab):
        return pl.pallas_call(
            kernel,
            out_shape=pltpu.VMEM((SLAB, HALF), jnp.bfloat16),
            in_specs=[pl.BlockSpec(memory_space=pl.ANY)],
            out_specs=pl.BlockSpec(memory_space=pltpu.VMEM),
            scratch_shapes=[
                pltpu.VMEM((2, N, HALF), jnp.bfloat16),
                pltpu.VMEM((2, SLAB, N), jnp.bfloat16),
                pltpu.SemaphoreType.DMA,
                pltpu.SemaphoreType.DMA((sends,)),
                pltpu.SemaphoreType.DMA((sends, 2, 2, 4)),
                pltpu.SemaphoreType.DMA((sends,)),
                pltpu.SemaphoreType.DMA((sends, 2, 2, 4)),
            ],
            compiler_params=pltpu.CompilerParams(collective_id=0, has_side_effects=True),
        )(slab)

    return jax.shard_map(local, mesh=mesh, in_specs=(layout,), out_specs=layout, check_vma=False)
```

```python
import jax
import jax.numpy as jnp
from jax import lax
from jax.experimental import pallas as pl
from jax.experimental.pallas import tpu as pltpu
from jax.sharding import PartitionSpec as P

N = 2048
SLAB = 128
HALF = 1024
STEPS = 15
MESH = pl.DeviceIdType.MESH

PIECES = (('zxy', 0, 48), ('zyx', 48, 48), ('yxz', 96, 32))
END_ORDER = (
    8, 4, 1, 24, 20, 17, 40, 36, 33, 9, 2, 12, 5, 18, 28, 25, 21, 41, 37, 34, 44, 13, 6, 10, 3, 26, 22, 19, 29, 35,
    14, 38, 42, 11, 7, 30, 23, 43, 39, 27, 45, 15, 47, 31, 46,
)
MID_ORDER = (
    1, 8, 4, 2, 17, 24, 20, 18, 33, 40, 36, 34, 3, 9, 10, 5, 41, 37, 19, 6, 12, 35, 38, 42, 25, 26, 28, 21, 22, 39,
    43, 45, 44, 7, 11, 47, 13, 14, 27, 46, 23, 29, 30, 15, 31,
)

END_GROUPS = ((10, (0, 1, 8, 4)), (24, (2, 9, 5, 12)), (36, (3, 10, 6)), (42, (11, 7, 13)), (44, (14, 15)))
MID_GROUPS = ((13, (0, 1, 8, 2, 4)), (29, (3, 9)), (34, (10, 5, 6, 12)), (43, (11, 7, 13)), (44, (14, 15)))


def forwards(order, dx, dy, k, end):
    far = {'x': dx == 1, 'y': dy == 1, 'z': k != 0}
    last = max([i for i, axis in enumerate(order) if far[axis]], default=-1)
    hops = []
    for i, axis in enumerate(order):
        if axis == 'z' and i > last:
            hops += ['in'] if end else ['in', 'out']
        elif axis == 'z' and i == last and not end:
            hops += ['in'] if k == 1 else ['out']
        elif i > last:
            hops.append(axis)
    return hops


def kernel(in_ref, out_ref, reach, rows, total, in_sem, send_sem, recv_sem, pass_sem, got_sem):
    z, y, row = lax.axis_index('depth'), lax.axis_index('col'), lax.axis_index('row')
    x, core = row // 2, row % 2
    upper = z >= 2
    z_in = jnp.where(upper, z - 1, z + 1)
    z_out = jnp.where(upper, z + 1, z - 1)
    end = (z == 0) | (z == 3)
    x_row = (1 - x) * 2 + core
    mate_row = x * 2 + 1 - core
    peers = {
        'x': {'depth': z, 'col': y, 'row': x_row},
        'y': {'depth': z, 'col': 1 - y, 'row': row},
        'in': {'depth': z_in, 'col': y, 'row': row},
        'out': {'depth': z_out, 'col': y, 'row': row},
    }
    mate = {'depth': z, 'col': y, 'row': mate_row}

    def slab_at(sx, sy, sz, score):
        return sy, (sx * 2 + score) * 4 + sz

    own_half, own_block = slab_at(x, y, z, core)
    own_row = pl.multiple_of(own_block * SLAB, SLAB)
    load = pltpu.make_async_copy(in_ref, reach.at[own_half, pl.ds(own_row, SLAB), :], in_sem)
    load.start()

    barrier = pltpu.get_barrier_semaphore()
    for name in ('x', 'y', 'in'):
        pl.semaphore_signal(barrier, inc=1, device_id=peers[name], device_id_type=MESH)
    pl.semaphore_signal(barrier, inc=1, device_id=mate, device_id_type=MESH)

    @pl.when(jnp.logical_not(end))
    def _():
        pl.semaphore_signal(barrier, inc=1, device_id=peers['out'], device_id_type=MESH)
        pl.semaphore_wait(barrier, 5)

    @pl.when(end)
    def _():
        pl.semaphore_wait(barrier, 4)

    load.wait()

    def piece_ref(p, sx, sy, sz, score):
        half, block = slab_at(sx, sy, sz, score)
        start = pl.multiple_of(block * SLAB + PIECES[p][1], 16)
        return reach.at[half, pl.ds(start, PIECES[p][2]), :]

    def copy(p, sx, sy, sz, score, peer, send, recv):
        ref = piece_ref(p, sx, sy, sz, score)
        return pltpu.make_async_remote_copy(
            src_ref=ref, dst_ref=ref, send_sem=send, recv_sem=recv, device_id=peer, device_id_type=MESH
        )

    def gather(end_case):
        places = (0, 1, 2, 3) if end_case else (1, 0, 2, 3)

        def source(dx, dy, k):
            sx = (1 - x) if dx else x
            sy = (1 - y) if dy else y
            if k == 0:
                return sx, sy, z
            place = places[k]
            return sx, sy, jnp.where(upper, 3 - place, place)

        sent = [0] * len(PIECES)

        def push(p, dx, dy, k):
            sx, sy, sz = source(dx, dy, k)
            for hop in forwards(PIECES[p][0], dx, dy, k, end_case):
                sent[p] += 1
                copy(p, sx, sy, sz, core, peers[hop], send_sem.at[p], recv_sem.at[p, sx, sy, sz]).start()
            copy(p, sx, sy, sz, core, mate, pass_sem.at[p], got_sem.at[p, sx, sy, sz]).start()

        def first_product(units, fresh):
            terms = {0: [], 1: []}
            for unit in units:
                dx, dy, k = unit // 8, unit // 4 % 2, unit % 4
                sx, sy, sz = source(dx, dy, k)
                for p in range(len(PIECES)):
                    copy(p, sx, sy, sz, 1 - core, mate, pass_sem.at[p], got_sem.at[p, sx, sy, sz]).wait_recv()
                left, right = [], []
                for score in range(2):
                    spot = pl.multiple_of((score * 4 + sz) * SLAB, SLAB)
                    left.append(rows[0, sx, :, pl.ds(spot, SLAB)])
                    right.append(pl.ds(pl.multiple_of(sx * HALF + spot, SLAB), SLAB))
                terms[dy].append((jnp.concatenate(left, axis=1), right))
            for dy in range(2):
                if not terms[dy]:
                    continue
                half = (1 - y) if dy else y
                left = jnp.concatenate([term[0] for term in terms[dy]], axis=1)
                for start in range(0, HALF, 256):
                    right = [reach[half, spot, start:start + 256] for term in terms[dy] for spot in term[1]]
                    product = jnp.dot(left, jnp.concatenate(right, axis=0), preferred_element_type=jnp.float32)
                    if fresh:
                        total[half, :, start:start + 256] = product
                    else:
                        total[half, :, start:start + 256] += product

        for p in range(len(PIECES)):
            push(p, 0, 0, 0)
        rows[0, y] = reach[y, pl.ds(own_row, SLAB), :]
        groups = dict(END_GROUPS if end_case else MID_GROUPS)
        fresh = True
        for place, code in enumerate(END_ORDER if end_case else MID_ORDER):
            p, dx, dy, k = code // 16, code // 8 % 2, code // 4 % 2, code % 4
            sx, sy, sz = source(dx, dy, k)
            copy(p, sx, sy, sz, core, mate, send_sem.at[p], recv_sem.at[p, sx, sy, sz]).wait_recv()
            push(p, dx, dy, k)
            if place in groups:
                if fresh:
                    rows[0, 1 - y] = reach[1 - y, pl.ds(own_row, SLAB), :]
                first_product(groups[place], fresh)
                fresh = False

        def drain(p, count, semaphore):
            ref = reach.at[0, pl.ds(0, count * PIECES[p][2]), :]
            pltpu.make_async_remote_copy(
                src_ref=ref, dst_ref=ref, send_sem=semaphore, recv_sem=semaphore, device_id=mate, device_id_type=MESH
            ).wait_send()

        for p in range(len(PIECES)):
            drain(p, sent[p], send_sem.at[p])
            drain(p, 16, pass_sem.at[p])

    @pl.when(end)
    def _():
        gather(True)

    @pl.when(jnp.logical_not(end))
    def _():
        gather(False)

    for half in range(2):
        for start in range(0, HALF, 256):
            part = (0, half, slice(None), slice(start, start + 256))
            grown = total[half, :, start:start + 256] + rows[part].astype(jnp.float32)
            rows[part] = jnp.minimum(grown, 1.0).astype(jnp.bfloat16)

    def block(now, half, start):
        known = jnp.concatenate([rows[now, 0], rows[now, 1]], axis=1)
        product = jnp.dot(known, reach[half, :, start:start + 256], preferred_element_type=jnp.float32)
        old = rows[now, half, :, start:start + 256].astype(jnp.float32)
        return jnp.minimum(product + old, 1.0).astype(jnp.bfloat16)

    def step(now):
        for half in range(2):
            for start in range(0, HALF, 256):
                rows[1 - now, half, :, start:start + 256] = block(now, half, start)

    def two_steps(_, carry):
        step(0)
        step(1)
        return carry

    lax.fori_loop(0, (STEPS - 2) // 2, two_steps, 0)
    step(0)

    for half in range(2):
        @pl.when(y == half)
        def _():
            for start in range(0, HALF, 256):
                out_ref[:, start:start + 256] = block(1, half, start)


def solution(mesh):
    layout = P(('row', 'depth'), 'col')
    sends = len(PIECES)

    def local(slab):
        return pl.pallas_call(
            kernel,
            out_shape=pltpu.VMEM((SLAB, HALF), jnp.bfloat16),
            in_specs=[pl.BlockSpec(memory_space=pl.ANY)],
            out_specs=pl.BlockSpec(memory_space=pltpu.VMEM),
            scratch_shapes=[
                pltpu.VMEM((2, N, HALF), jnp.bfloat16),
                pltpu.VMEM((2, 2, SLAB, HALF), jnp.bfloat16),
                pltpu.VMEM((2, SLAB, HALF), jnp.float32),
                pltpu.SemaphoreType.DMA,
                pltpu.SemaphoreType.DMA((sends,)),
                pltpu.SemaphoreType.DMA((sends, 2, 2, 4)),
                pltpu.SemaphoreType.DMA((sends,)),
                pltpu.SemaphoreType.DMA((sends, 2, 2, 4)),
            ],
            compiler_params=pltpu.CompilerParams(collective_id=0, has_side_effects=True),
        )(slab)

    return jax.shard_map(local, mesh=mesh, in_specs=(layout,), out_specs=layout, check_vma=False)
```

```python
import jax
import jax.numpy as jnp
from jax import lax
from jax.experimental import pallas as pl
from jax.experimental.pallas import tpu as pltpu
from jax.sharding import PartitionSpec as P

N = 2048
SLAB = 128
HALF = 1024
STEPS = 15
MESH = pl.DeviceIdType.MESH

PIECES = (('zxy', 0, 48), ('zyx', 48, 48), ('yxz', 96, 32))
END_ORDER = (
    8, 4, 1, 24, 20, 17, 40, 36, 33, 9, 2, 12, 5, 18, 28, 25, 21, 41, 37, 34, 44, 13, 6, 10, 3, 26, 22, 19, 29, 35,
    14, 38, 42, 11, 7, 30, 23, 43, 39, 27, 45, 15, 47, 31, 46,
)
MID_ORDER = (
    1, 8, 4, 2, 17, 24, 20, 18, 33, 40, 36, 34, 3, 9, 10, 5, 41, 37, 19, 6, 12, 35, 38, 42, 25, 26, 28, 21, 22, 39,
    43, 45, 44, 7, 11, 47, 13, 14, 27, 46, 23, 29, 30, 15, 31,
)

END_GROUPS = ((10, (0, 1, 8, 4)), (24, (2, 9, 5, 12)), (36, (3, 10, 6)), (42, (11, 7, 13)), (44, (14, 15)))
MID_GROUPS = ((13, (0, 1, 8, 2, 4)), (29, (3, 9)), (34, (10, 5, 6, 12)), (43, (11, 7, 13)), (44, (14, 15)))


def forwards(order, dx, dy, k, end):
    far = {'x': dx == 1, 'y': dy == 1, 'z': k != 0}
    last = max([i for i, axis in enumerate(order) if far[axis]], default=-1)
    hops = []
    for i, axis in enumerate(order):
        if axis == 'z' and i > last:
            hops += ['in'] if end else ['in', 'out']
        elif axis == 'z' and i == last and not end:
            hops += ['in'] if k == 1 else ['out']
        elif i > last:
            hops.append(axis)
    return hops


def kernel(in_ref, out_ref, reach, rows, total, in_sem, send_sem, recv_sem, pass_sem, got_sem):
    z, y, row = lax.axis_index('depth'), lax.axis_index('col'), lax.axis_index('row')
    x, core = row // 2, row % 2
    upper = z >= 2
    z_in = jnp.where(upper, z - 1, z + 1)
    z_out = jnp.where(upper, z + 1, z - 1)
    end = (z == 0) | (z == 3)
    x_row = (1 - x) * 2 + core
    mate_row = x * 2 + 1 - core
    peers = {
        'x': {'depth': z, 'col': y, 'row': x_row},
        'y': {'depth': z, 'col': 1 - y, 'row': row},
        'in': {'depth': z_in, 'col': y, 'row': row},
        'out': {'depth': z_out, 'col': y, 'row': row},
    }
    mate = {'depth': z, 'col': y, 'row': mate_row}

    def slab_at(sx, sy, sz, score):
        return sy, (sx * 2 + score) * 4 + sz

    own_half, own_block = slab_at(x, y, z, core)
    own_row = pl.multiple_of(own_block * SLAB, SLAB)
    load = pltpu.make_async_copy(in_ref, reach.at[own_half, pl.ds(own_row, SLAB), :], in_sem)
    load.start()

    barrier = pltpu.get_barrier_semaphore()
    for name in ('x', 'y', 'in'):
        pl.semaphore_signal(barrier, inc=1, device_id=peers[name], device_id_type=MESH)
    pl.semaphore_signal(barrier, inc=1, device_id=mate, device_id_type=MESH)

    @pl.when(jnp.logical_not(end))
    def _():
        pl.semaphore_signal(barrier, inc=1, device_id=peers['out'], device_id_type=MESH)
        pl.semaphore_wait(barrier, 5)

    @pl.when(end)
    def _():
        pl.semaphore_wait(barrier, 4)

    load.wait()

    def piece_ref(p, sx, sy, sz, score):
        half, block = slab_at(sx, sy, sz, score)
        start = pl.multiple_of(block * SLAB + PIECES[p][1], 16)
        return reach.at[half, pl.ds(start, PIECES[p][2]), :]

    def copy(p, sx, sy, sz, score, peer, send, recv):
        ref = piece_ref(p, sx, sy, sz, score)
        return pltpu.make_async_remote_copy(
            src_ref=ref, dst_ref=ref, send_sem=send, recv_sem=recv, device_id=peer, device_id_type=MESH
        )

    def gather(end_case):
        places = (0, 1, 2, 3) if end_case else (1, 0, 2, 3)

        def source(dx, dy, k):
            sx = (1 - x) if dx else x
            sy = (1 - y) if dy else y
            if k == 0:
                return sx, sy, z
            place = places[k]
            return sx, sy, jnp.where(upper, 3 - place, place)

        sent = [0] * len(PIECES)

        def push(p, dx, dy, k):
            sx, sy, sz = source(dx, dy, k)
            for hop in forwards(PIECES[p][0], dx, dy, k, end_case):
                sent[p] += 1
                copy(p, sx, sy, sz, core, peers[hop], send_sem.at[p], recv_sem.at[p, sx, sy, sz]).start()
            copy(p, sx, sy, sz, core, mate, pass_sem.at[p], got_sem.at[p, sx, sy, sz]).start()

        def first_product(units, fresh):
            terms = {0: [], 1: []}
            for unit in units:
                dx, dy, k = unit // 8, unit // 4 % 2, unit % 4
                sx, sy, sz = source(dx, dy, k)
                for p in range(len(PIECES)):
                    copy(p, sx, sy, sz, 1 - core, mate, pass_sem.at[p], got_sem.at[p, sx, sy, sz]).wait_recv()
                left, right = [], []
                for score in range(2):
                    spot = pl.multiple_of((score * 4 + sz) * SLAB, SLAB)
                    left.append(rows[0, sx, :, pl.ds(spot, SLAB)])
                    right.append(pl.ds(pl.multiple_of(sx * HALF + spot, SLAB), SLAB))
                terms[dy].append((jnp.concatenate(left, axis=1), right))
            for dy in range(2):
                if not terms[dy]:
                    continue
                half = (1 - y) if dy else y
                left = jnp.concatenate([term[0] for term in terms[dy]], axis=1)
                for start in range(0, HALF, 256):
                    right = [reach[half, spot, start:start + 256] for term in terms[dy] for spot in term[1]]
                    product = jnp.dot(left, jnp.concatenate(right, axis=0), preferred_element_type=jnp.float32)
                    if fresh:
                        total[half, :, start:start + 256] = product
                    else:
                        total[half, :, start:start + 256] += product

        for p in range(len(PIECES)):
            push(p, 0, 0, 0)
        rows[0, y] = reach[y, pl.ds(own_row, SLAB), :]
        groups = dict(END_GROUPS if end_case else MID_GROUPS)
        fresh = True
        for place, code in enumerate(END_ORDER if end_case else MID_ORDER):
            p, dx, dy, k = code // 16, code // 8 % 2, code // 4 % 2, code % 4
            sx, sy, sz = source(dx, dy, k)
            copy(p, sx, sy, sz, core, mate, send_sem.at[p], recv_sem.at[p, sx, sy, sz]).wait_recv()
            push(p, dx, dy, k)
            if place in groups:
                if fresh:
                    rows[0, 1 - y] = reach[1 - y, pl.ds(own_row, SLAB), :]
                first_product(groups[place], fresh)
                fresh = False

        def drain(p, count, semaphore):
            ref = reach.at[0, pl.ds(0, count * PIECES[p][2]), :]
            pltpu.make_async_remote_copy(
                src_ref=ref, dst_ref=ref, send_sem=semaphore, recv_sem=semaphore, device_id=mate, device_id_type=MESH
            ).wait_send()

        for p in range(len(PIECES)):
            drain(p, sent[p], send_sem.at[p])
            drain(p, 16, pass_sem.at[p])

    @pl.when(end)
    def _():
        gather(True)

    @pl.when(jnp.logical_not(end))
    def _():
        gather(False)

    for half in range(2):
        for start in range(0, HALF, 256):
            part = (0, half, slice(None), slice(start, start + 256))
            grown = total[half, :, start:start + 256] + rows[part].astype(jnp.float32)
            rows[part] = jnp.minimum(grown, 1.0).astype(jnp.bfloat16)

    def block(now, half, start, width=256):
        known = jnp.concatenate([rows[now, 0], rows[now, 1]], axis=1)
        product = jnp.dot(known, reach[half, :, start:start + width], preferred_element_type=jnp.float32)
        old = rows[now, half, :, start:start + width].astype(jnp.float32)
        return jnp.minimum(product + old, 1.0).astype(jnp.bfloat16)

    def step(now):
        for half in range(2):
            for start in range(0, HALF, 1024):
                rows[1 - now, half, :, start:start + 1024] = block(now, half, start, 1024)

    def two_steps(_, carry):
        step(0)
        step(1)
        return carry

    lax.fori_loop(0, (STEPS - 2) // 2, two_steps, 0)
    step(0)

    for half in range(2):
        @pl.when(y == half)
        def _():
            for start in range(0, HALF, 256):
                out_ref[:, start:start + 256] = block(1, half, start)


def solution(mesh):
    layout = P(('row', 'depth'), 'col')
    sends = len(PIECES)

    def local(slab):
        return pl.pallas_call(
            kernel,
            out_shape=pltpu.VMEM((SLAB, HALF), jnp.bfloat16),
            in_specs=[pl.BlockSpec(memory_space=pl.ANY)],
            out_specs=pl.BlockSpec(memory_space=pltpu.VMEM),
            scratch_shapes=[
                pltpu.VMEM((2, N, HALF), jnp.bfloat16),
                pltpu.VMEM((2, 2, SLAB, HALF), jnp.bfloat16),
                pltpu.VMEM((2, SLAB, HALF), jnp.float32),
                pltpu.SemaphoreType.DMA,
                pltpu.SemaphoreType.DMA((sends,)),
                pltpu.SemaphoreType.DMA((sends, 2, 2, 4)),
                pltpu.SemaphoreType.DMA((sends,)),
                pltpu.SemaphoreType.DMA((sends, 2, 2, 4)),
            ],
            compiler_params=pltpu.CompilerParams(collective_id=0, has_side_effects=True),
        )(slab)

    return jax.shard_map(local, mesh=mesh, in_specs=(layout,), out_specs=layout, check_vma=False)
```

```python
import jax
import jax.numpy as jnp
from jax import lax
from jax.experimental import pallas as pl
from jax.experimental.pallas import tpu as pltpu
from jax.sharding import PartitionSpec as P

N = 2048
SLAB = 128
HALF = 1024
TILES = 8
WIDTH = 4
PAD = 16
STEPS = 15
MESH = pl.DeviceIdType.MESH

PIECES = (('zxy', 0, 48), ('zyx', 48, 48), ('yxz', 96, 32))
END_ORDER = (
    8, 4, 1, 24, 20, 17, 40, 36, 33, 9, 2, 12, 5, 18, 28, 25, 21, 41, 37, 34, 44, 13, 6, 10, 3, 26, 22, 19, 29, 35,
    14, 38, 42, 11, 7, 30, 23, 43, 39, 27, 45, 15, 47, 31, 46,
)
MID_ORDER = (
    1, 8, 4, 2, 17, 24, 20, 18, 33, 40, 36, 34, 3, 9, 10, 5, 41, 37, 19, 6, 12, 35, 38, 42, 25, 26, 28, 21, 22, 39,
    43, 45, 44, 7, 11, 47, 13, 14, 27, 46, 23, 29, 30, 15, 31,
)

END_GROUPS = ((10, (0, 1, 8, 4)), (24, (2, 9, 5, 12)), (36, (3, 10, 6)), (42, (11, 7, 13)), (44, (14, 15)))
MID_GROUPS = ((13, (0, 1, 8, 2, 4)), (29, (3, 9)), (34, (10, 5, 6, 12)), (43, (11, 7, 13)), (44, (14, 15)))


def forwards(order, dx, dy, k, end):
    far = {'x': dx == 1, 'y': dy == 1, 'z': k != 0}
    last = max([i for i, axis in enumerate(order) if far[axis]], default=-1)
    hops = []
    for i, axis in enumerate(order):
        if axis == 'z' and i > last:
            hops += ['in'] if end else ['in', 'out']
        elif axis == 'z' and i == last and not end:
            hops += ['in'] if k == 1 else ['out']
        elif i > last:
            hops.append(axis)
    return hops


def kernel(in_ref, out_ref, reach, rows, total, in_sem, send_sem, recv_sem, pass_sem, got_sem):
    z, y, row = lax.axis_index('depth'), lax.axis_index('col'), lax.axis_index('row')
    x, core = row // 2, row % 2
    upper = z >= 2
    z_in = jnp.where(upper, z - 1, z + 1)
    z_out = jnp.where(upper, z + 1, z - 1)
    end = (z == 0) | (z == 3)
    x_row = (1 - x) * 2 + core
    mate_row = x * 2 + 1 - core
    peers = {
        'x': {'depth': z, 'col': y, 'row': x_row},
        'y': {'depth': z, 'col': 1 - y, 'row': row},
        'in': {'depth': z_in, 'col': y, 'row': row},
        'out': {'depth': z_out, 'col': y, 'row': row},
    }
    mate = {'depth': z, 'col': y, 'row': mate_row}

    def slab_at(sx, sy, sz, score):
        return sy, (sx * 2 + score) * 4 + sz

    own_half, own_block = slab_at(x, y, z, core)
    own_row = pl.multiple_of(own_block * SLAB, SLAB)
    loads = [
        pltpu.make_async_copy(
            in_ref.at[:, i * SLAB:(i + 1) * SLAB], reach.at[own_half * TILES + i, pl.ds(own_row, SLAB), :], in_sem.at[i]
        )
        for i in range(TILES)
    ]
    for load in loads:
        load.start()

    barrier = pltpu.get_barrier_semaphore()
    for name in ('x', 'y', 'in'):
        pl.semaphore_signal(barrier, inc=1, device_id=peers[name], device_id_type=MESH)
    pl.semaphore_signal(barrier, inc=1, device_id=mate, device_id_type=MESH)

    @pl.when(jnp.logical_not(end))
    def _():
        pl.semaphore_signal(barrier, inc=1, device_id=peers['out'], device_id_type=MESH)
        pl.semaphore_wait(barrier, 5)

    @pl.when(end)
    def _():
        pl.semaphore_wait(barrier, 4)

    for load in loads:
        load.wait()

    def piece_ref(p, sx, sy, sz, score):
        half, block = slab_at(sx, sy, sz, score)
        start = pl.multiple_of(block * SLAB + PIECES[p][1], 16)
        return reach.at[pl.ds(half * TILES, TILES), pl.ds(start, PIECES[p][2]), :]

    def copy(p, sx, sy, sz, score, peer, send, recv):
        ref = piece_ref(p, sx, sy, sz, score)
        return pltpu.make_async_remote_copy(
            src_ref=ref, dst_ref=ref, send_sem=send, recv_sem=recv, device_id=peer, device_id_type=MESH
        )

    def gather(end_case):
        places = (0, 1, 2, 3) if end_case else (1, 0, 2, 3)

        def source(dx, dy, k):
            sx = (1 - x) if dx else x
            sy = (1 - y) if dy else y
            if k == 0:
                return sx, sy, z
            place = places[k]
            return sx, sy, jnp.where(upper, 3 - place, place)

        sent = [0] * len(PIECES)

        def push(p, dx, dy, k):
            sx, sy, sz = source(dx, dy, k)
            for hop in forwards(PIECES[p][0], dx, dy, k, end_case):
                sent[p] += 1
                copy(p, sx, sy, sz, core, peers[hop], send_sem.at[p], recv_sem.at[p, sx, sy, sz]).start()
            copy(p, sx, sy, sz, core, mate, pass_sem.at[p], got_sem.at[p, sx, sy, sz]).start()

        def first_product(units, fresh):
            terms = {0: [], 1: []}
            for unit in units:
                dx, dy, k = unit // 8, unit // 4 % 2, unit % 4
                sx, sy, sz = source(dx, dy, k)
                for p in range(len(PIECES)):
                    copy(p, sx, sy, sz, 1 - core, mate, pass_sem.at[p], got_sem.at[p, sx, sy, sz]).wait_recv()
                blocks = [(sx * 2 + score) * 4 + sz for score in range(2)]
                left = jnp.concatenate([rows[0, spot] for spot in blocks], axis=1)
                terms[dy].append((left, [pl.ds(pl.multiple_of(spot * SLAB, SLAB), SLAB) for spot in blocks]))
            for dy in range(2):
                if not terms[dy]:
                    continue
                first = ((1 - y) if dy else y) * TILES
                left = jnp.concatenate([term[0] for term in terms[dy]], axis=1)
                for i in range(0, TILES, 2):
                    right = [
                        jnp.concatenate([reach[first + i, spot], reach[first + i + 1, spot]], axis=1)
                        for term in terms[dy] for spot in term[1]
                    ]
                    product = jnp.dot(left, jnp.concatenate(right, axis=0), preferred_element_type=jnp.float32)
                    for n in range(2):
                        part = product[:, n * SLAB:(n + 1) * SLAB]
                        total[first + i + n] = part if fresh else total[first + i + n] + part

        for p in range(len(PIECES)):
            push(p, 0, 0, 0)
        def own(half):
            for i in range(TILES):
                rows[0, half * TILES + i] = reach[half * TILES + i, pl.ds(own_row, SLAB), :]

        own(y)
        groups = dict(END_GROUPS if end_case else MID_GROUPS)
        fresh = True
        for place, code in enumerate(END_ORDER if end_case else MID_ORDER):
            p, dx, dy, k = code // 16, code // 8 % 2, code // 4 % 2, code % 4
            sx, sy, sz = source(dx, dy, k)
            copy(p, sx, sy, sz, core, mate, send_sem.at[p], recv_sem.at[p, sx, sy, sz]).wait_recv()
            push(p, dx, dy, k)
            if place in groups:
                if fresh:
                    own(1 - y)
                first_product(groups[place], fresh)
                fresh = False

        def drain(p, count, semaphore):
            ref = reach.at[pl.ds(0, TILES), pl.ds(0, count * PIECES[p][2]), :]
            pltpu.make_async_remote_copy(
                src_ref=ref, dst_ref=ref, send_sem=semaphore, recv_sem=semaphore, device_id=mate, device_id_type=MESH
            ).wait_send()

        for p in range(len(PIECES)):
            drain(p, sent[p], send_sem.at[p])
            drain(p, 16, pass_sem.at[p])

    @pl.when(end)
    def _():
        gather(True)

    @pl.when(jnp.logical_not(end))
    def _():
        gather(False)

    def capped(sums, old):
        return jnp.minimum(sums + old.astype(jnp.float32), 1.0).astype(jnp.bfloat16)

    for g in range(2 * TILES):
        rows[0, g] = capped(total[g], rows[0, g])

    def block(now, first, put):
        known = jnp.concatenate([rows[now, g] for g in range(2 * TILES)], axis=1)
        right = jnp.concatenate([reach[first + i, 0:N] for i in range(WIDTH)], axis=1)
        product = jnp.dot(known, right, preferred_element_type=jnp.float32)
        for i in range(WIDTH):
            put(i, capped(product[:, i * SLAB:(i + 1) * SLAB], rows[now, first + i]))

    def step(now):
        for first in range(0, 2 * TILES, WIDTH):
            def put(i, value):
                rows[1 - now, first + i] = value

            block(now, first, put)

    def two_steps(_, carry):
        step(0)
        step(1)
        return carry

    lax.fori_loop(0, (STEPS - 2) // 2, two_steps, 0)
    step(0)

    for start in range(0, TILES, WIDTH):
        def put(i, value):
            out_ref[:, (start + i) * SLAB:(start + i + 1) * SLAB] = value

        block(1, y * TILES + start, put)


def solution(mesh):
    layout = P(('row', 'depth'), 'col')
    sends = len(PIECES)

    def local(slab):
        return pl.pallas_call(
            kernel,
            out_shape=pltpu.VMEM((SLAB, HALF), jnp.bfloat16),
            in_specs=[pl.BlockSpec(memory_space=pl.ANY)],
            out_specs=pl.BlockSpec(memory_space=pltpu.VMEM),
            scratch_shapes=[
                pltpu.VMEM((2 * TILES, N + PAD, SLAB), jnp.bfloat16),
                pltpu.VMEM((2, 2 * TILES, SLAB, SLAB), jnp.bfloat16),
                pltpu.VMEM((2 * TILES, SLAB, SLAB), jnp.float32),
                pltpu.SemaphoreType.DMA((TILES,)),
                pltpu.SemaphoreType.DMA((sends,)),
                pltpu.SemaphoreType.DMA((sends, 2, 2, 4)),
                pltpu.SemaphoreType.DMA((sends,)),
                pltpu.SemaphoreType.DMA((sends, 2, 2, 4)),
            ],
            compiler_params=pltpu.CompilerParams(collective_id=0, has_side_effects=True),
        )(slab)

    return jax.shard_map(local, mesh=mesh, in_specs=(layout,), out_specs=layout, check_vma=False)
```

```python
import jax
import jax.numpy as jnp
from jax import lax
from jax.experimental import pallas as pl
from jax.experimental.pallas import tpu as pltpu
from jax.sharding import PartitionSpec as P

N = 2048
SLAB = 128
HALF = 1024
TILES = 8
WIDTH = 4
GROUP = 16
GROUPS = SLAB // GROUP
STEPS = 15
MESH = pl.DeviceIdType.MESH

PIECES = (('zxy', 0, 48), ('zyx', 48, 48), ('yxz', 96, 32))
END_ORDER = (
    8, 4, 1, 24, 20, 17, 40, 36, 33, 9, 2, 12, 5, 18, 28, 25, 21, 41, 37, 34, 44, 13, 6, 10, 3, 26, 22, 19, 29, 35,
    14, 38, 42, 11, 7, 30, 23, 43, 39, 27, 45, 15, 47, 31, 46,
)
MID_ORDER = (
    1, 8, 4, 2, 17, 24, 20, 18, 33, 40, 36, 34, 3, 9, 10, 5, 41, 37, 19, 6, 12, 35, 38, 42, 25, 26, 28, 21, 22, 39,
    43, 45, 44, 7, 11, 47, 13, 14, 27, 46, 23, 29, 30, 15, 31,
)

END_GROUPS = ((10, (0, 1, 8, 4)), (24, (2, 9, 5, 12)), (36, (3, 10, 6)), (42, (11, 7, 13)), (44, (14, 15)))
MID_GROUPS = ((13, (0, 1, 8, 2, 4)), (29, (3, 9)), (34, (10, 5, 6, 12)), (43, (11, 7, 13)), (44, (14, 15)))


def forwards(order, dx, dy, k, end):
    far = {'x': dx == 1, 'y': dy == 1, 'z': k != 0}
    last = max([i for i, axis in enumerate(order) if far[axis]], default=-1)
    hops = []
    for i, axis in enumerate(order):
        if axis == 'z' and i > last:
            hops += ['in'] if end else ['in', 'out']
        elif axis == 'z' and i == last and not end:
            hops += ['in'] if k == 1 else ['out']
        elif i > last:
            hops.append(axis)
    return hops


def kernel(in_ref, out_ref, reach, rows, total, in_sem, send_sem, recv_sem, pass_sem, got_sem):
    z, y, row = lax.axis_index('depth'), lax.axis_index('col'), lax.axis_index('row')
    x, core = row // 2, row % 2
    upper = z >= 2
    z_in = jnp.where(upper, z - 1, z + 1)
    z_out = jnp.where(upper, z + 1, z - 1)
    end = (z == 0) | (z == 3)
    x_row = (1 - x) * 2 + core
    mate_row = x * 2 + 1 - core
    peers = {
        'x': {'depth': z, 'col': y, 'row': x_row},
        'y': {'depth': z, 'col': 1 - y, 'row': row},
        'in': {'depth': z_in, 'col': y, 'row': row},
        'out': {'depth': z_out, 'col': y, 'row': row},
    }
    mate = {'depth': z, 'col': y, 'row': mate_row}

    def slab_at(sx, sy, sz, score):
        return sy, (sx * 2 + score) * 4 + sz

    own_half, own_block = slab_at(x, y, z, core)
    loads = [
        pltpu.make_async_copy(
            in_ref.at[:, :, i * SLAB:(i + 1) * SLAB], reach.at[own_half, pl.ds(own_block * GROUPS, GROUPS), i], in_sem.at[i]
        )
        for i in range(TILES)
    ]
    for load in loads:
        load.start()

    barrier = pltpu.get_barrier_semaphore()
    for name in ('x', 'y', 'in'):
        pl.semaphore_signal(barrier, inc=1, device_id=peers[name], device_id_type=MESH)
    pl.semaphore_signal(barrier, inc=1, device_id=mate, device_id_type=MESH)

    @pl.when(jnp.logical_not(end))
    def _():
        pl.semaphore_signal(barrier, inc=1, device_id=peers['out'], device_id_type=MESH)
        pl.semaphore_wait(barrier, 5)

    @pl.when(end)
    def _():
        pl.semaphore_wait(barrier, 4)

    for load in loads:
        load.wait()

    def piece_ref(p, sx, sy, sz, score):
        half, block = slab_at(sx, sy, sz, score)
        _, first, count = PIECES[p]
        return reach.at[half, pl.ds(block * GROUPS + first // GROUP, count // GROUP)]

    def copy(p, sx, sy, sz, score, peer, send, recv):
        ref = piece_ref(p, sx, sy, sz, score)
        return pltpu.make_async_remote_copy(
            src_ref=ref, dst_ref=ref, send_sem=send, recv_sem=recv, device_id=peer, device_id_type=MESH
        )

    def tile(half, block, i):
        return reach[half, pl.ds(block * GROUPS, GROUPS), i].reshape(SLAB, SLAB)

    def gather(end_case):
        places = (0, 1, 2, 3) if end_case else (1, 0, 2, 3)

        def source(dx, dy, k):
            sx = (1 - x) if dx else x
            sy = (1 - y) if dy else y
            if k == 0:
                return sx, sy, z
            place = places[k]
            return sx, sy, jnp.where(upper, 3 - place, place)

        sent = [0] * len(PIECES)

        def push(p, dx, dy, k):
            sx, sy, sz = source(dx, dy, k)
            for hop in forwards(PIECES[p][0], dx, dy, k, end_case):
                sent[p] += 1
                copy(p, sx, sy, sz, core, peers[hop], send_sem.at[p], recv_sem.at[p, sx, sy, sz]).start()
            copy(p, sx, sy, sz, core, mate, pass_sem.at[p], got_sem.at[p, sx, sy, sz]).start()

        def first_product(units, fresh):
            terms = {0: [], 1: []}
            for unit in units:
                dx, dy, k = unit // 8, unit // 4 % 2, unit % 4
                sx, sy, sz = source(dx, dy, k)
                for p in range(len(PIECES)):
                    copy(p, sx, sy, sz, 1 - core, mate, pass_sem.at[p], got_sem.at[p, sx, sy, sz]).wait_recv()
                blocks = [(sx * 2 + score) * 4 + sz for score in range(2)]
                left = jnp.concatenate([rows[0, spot] for spot in blocks], axis=1)
                terms[dy].append((left, blocks))
            for dy in range(2):
                if not terms[dy]:
                    continue
                half = (1 - y) if dy else y
                left = jnp.concatenate([term[0] for term in terms[dy]], axis=1)
                for i in range(0, TILES, 2):
                    right = [
                        jnp.concatenate([tile(half, spot, i), tile(half, spot, i + 1)], axis=1)
                        for term in terms[dy] for spot in term[1]
                    ]
                    product = jnp.dot(left, jnp.concatenate(right, axis=0), preferred_element_type=jnp.float32)
                    for n in range(2):
                        part = product[:, n * SLAB:(n + 1) * SLAB]
                        g = half * TILES + i + n
                        total[g] = part if fresh else total[g] + part

        for p in range(len(PIECES)):
            push(p, 0, 0, 0)
        def own(half):
            for i in range(TILES):
                rows[0, half * TILES + i] = tile(half, own_block, i)

        own(y)
        groups = dict(END_GROUPS if end_case else MID_GROUPS)
        fresh = True
        for place, code in enumerate(END_ORDER if end_case else MID_ORDER):
            p, dx, dy, k = code // 16, code // 8 % 2, code // 4 % 2, code % 4
            sx, sy, sz = source(dx, dy, k)
            copy(p, sx, sy, sz, core, mate, send_sem.at[p], recv_sem.at[p, sx, sy, sz]).wait_recv()
            push(p, dx, dy, k)
            if place in groups:
                if fresh:
                    own(1 - y)
                first_product(groups[place], fresh)
                fresh = False

        def drain(p, count, semaphore):
            ref = reach.at[0, pl.ds(0, count * PIECES[p][2] // GROUP)]
            pltpu.make_async_remote_copy(
                src_ref=ref, dst_ref=ref, send_sem=semaphore, recv_sem=semaphore, device_id=mate, device_id_type=MESH
            ).wait_send()

        for p in range(len(PIECES)):
            drain(p, sent[p], send_sem.at[p])
            drain(p, 16, pass_sem.at[p])

    @pl.when(end)
    def _():
        gather(True)

    @pl.when(jnp.logical_not(end))
    def _():
        gather(False)

    def capped(sums, old):
        return jnp.minimum(sums + old.astype(jnp.float32), 1.0).astype(jnp.bfloat16)

    for g in range(2 * TILES):
        rows[0, g] = capped(total[g], rows[0, g])

    def block(now, half, first, put):
        known = jnp.concatenate([rows[now, g] for g in range(2 * TILES)], axis=1)
        right = jnp.concatenate([reach[half, :, first + i].reshape(N, SLAB) for i in range(WIDTH)], axis=1)
        product = jnp.dot(known, right, preferred_element_type=jnp.float32)
        for i in range(WIDTH):
            put(i, capped(product[:, i * SLAB:(i + 1) * SLAB], rows[now, half * TILES + first + i]))

    def step(now):
        for half in range(2):
            for first in range(0, TILES, WIDTH):
                def put(i, value):
                    rows[1 - now, half * TILES + first + i] = value

                block(now, half, first, put)

    def two_steps(_, carry):
        step(0)
        step(1)
        return carry

    lax.fori_loop(0, (STEPS - 2) // 2, two_steps, 0)
    step(0)

    for first in range(0, TILES, WIDTH):
        def put(i, value):
            out_ref[:, (first + i) * SLAB:(first + i + 1) * SLAB] = value

        block(1, y, first, put)


def solution(mesh):
    layout = P(('row', 'depth'), 'col')
    sends = len(PIECES)

    def local(slab):
        return pl.pallas_call(
            kernel,
            out_shape=pltpu.VMEM((SLAB, HALF), jnp.bfloat16),
            in_specs=[pl.BlockSpec(memory_space=pl.ANY)],
            out_specs=pl.BlockSpec(memory_space=pltpu.VMEM),
            scratch_shapes=[
                pltpu.VMEM((2, N // GROUP, TILES, GROUP, SLAB), jnp.bfloat16),
                pltpu.VMEM((2, 2 * TILES, SLAB, SLAB), jnp.bfloat16),
                pltpu.VMEM((2 * TILES, SLAB, SLAB), jnp.float32),
                pltpu.SemaphoreType.DMA((TILES,)),
                pltpu.SemaphoreType.DMA((sends,)),
                pltpu.SemaphoreType.DMA((sends, 2, 2, 4)),
                pltpu.SemaphoreType.DMA((sends,)),
                pltpu.SemaphoreType.DMA((sends, 2, 2, 4)),
            ],
            compiler_params=pltpu.CompilerParams(collective_id=0, has_side_effects=True),
        )(slab.reshape(GROUPS, GROUP, HALF))

    return jax.shard_map(local, mesh=mesh, in_specs=(layout,), out_specs=layout, check_vma=False)
```

```python
import jax
import jax.numpy as jnp
from jax import lax
from jax.experimental import pallas as pl
from jax.experimental.pallas import tpu as pltpu
from jax.sharding import PartitionSpec as P

N = 2048
SLAB = 128
HALF = 1024
STEPS = 15
MESH = pl.DeviceIdType.MESH

PIECES = (('zxy', 0, 48), ('zyx', 48, 48), ('yxz', 96, 32))
END_ORDER = (
    8, 4, 1, 24, 20, 17, 40, 36, 33, 9, 2, 12, 5, 18, 28, 25, 21, 41, 37, 34, 44, 13, 6, 10, 3, 26, 22, 19, 29, 35,
    14, 38, 42, 11, 7, 30, 23, 43, 39, 27, 45, 15, 47, 31, 46,
)
MID_ORDER = (
    1, 8, 4, 2, 17, 24, 20, 18, 33, 40, 36, 34, 3, 9, 10, 5, 41, 37, 19, 6, 12, 35, 38, 42, 25, 26, 28, 21, 22, 39,
    43, 45, 44, 7, 11, 47, 13, 14, 27, 46, 23, 29, 30, 15, 31,
)

END_GROUPS = ((10, (0, 1, 8, 4)), (24, (2, 9, 5, 12)), (36, (3, 10, 6)), (42, (11, 7, 13)), (44, (14, 15)))
MID_GROUPS = ((13, (0, 1, 8, 2, 4)), (29, (3, 9)), (34, (10, 5, 6, 12)), (43, (11, 7, 13)), (44, (14, 15)))


def forwards(order, dx, dy, k, end):
    far = {'x': dx == 1, 'y': dy == 1, 'z': k != 0}
    last = max([i for i, axis in enumerate(order) if far[axis]], default=-1)
    hops = []
    for i, axis in enumerate(order):
        if axis == 'z' and i > last:
            hops += ['in'] if end else ['in', 'out']
        elif axis == 'z' and i == last and not end:
            hops += ['in'] if k == 1 else ['out']
        elif i > last:
            hops.append(axis)
    return hops


def kernel(in_ref, out_ref, reach, rows, total, in_sem, send_sem, recv_sem, pass_sem, got_sem):
    z, y, row = lax.axis_index('depth'), lax.axis_index('col'), lax.axis_index('row')
    x, core = row // 2, row % 2
    upper = z >= 2
    z_in = jnp.where(upper, z - 1, z + 1)
    z_out = jnp.where(upper, z + 1, z - 1)
    end = (z == 0) | (z == 3)
    x_row = (1 - x) * 2 + core
    mate_row = x * 2 + 1 - core
    peers = {
        'x': {'depth': z, 'col': y, 'row': x_row},
        'y': {'depth': z, 'col': 1 - y, 'row': row},
        'in': {'depth': z_in, 'col': y, 'row': row},
        'out': {'depth': z_out, 'col': y, 'row': row},
    }
    mate = {'depth': z, 'col': y, 'row': mate_row}

    def slab_at(sx, sy, sz, score):
        return sy, (sx * 2 + score) * 4 + sz

    own_half, own_block = slab_at(x, y, z, core)
    own_row = pl.multiple_of(own_block * SLAB, SLAB)
    load = pltpu.make_async_copy(in_ref, reach.at[own_half, pl.ds(own_row, SLAB), :], in_sem)
    load.start()

    barrier = pltpu.get_barrier_semaphore()
    for name in ('x', 'y', 'in'):
        pl.semaphore_signal(barrier, inc=1, device_id=peers[name], device_id_type=MESH)
    pl.semaphore_signal(barrier, inc=1, device_id=mate, device_id_type=MESH)

    @pl.when(jnp.logical_not(end))
    def _():
        pl.semaphore_signal(barrier, inc=1, device_id=peers['out'], device_id_type=MESH)
        pl.semaphore_wait(barrier, 5)

    @pl.when(end)
    def _():
        pl.semaphore_wait(barrier, 4)

    load.wait()

    def piece_ref(p, sx, sy, sz, score):
        half, block = slab_at(sx, sy, sz, score)
        start = pl.multiple_of(block * SLAB + PIECES[p][1], 16)
        return reach.at[half, pl.ds(start, PIECES[p][2]), :]

    def copy(p, sx, sy, sz, score, peer, send, recv):
        ref = piece_ref(p, sx, sy, sz, score)
        return pltpu.make_async_remote_copy(
            src_ref=ref, dst_ref=ref, send_sem=send, recv_sem=recv, device_id=peer, device_id_type=MESH
        )

    def gather(end_case):
        places = (0, 1, 2, 3) if end_case else (1, 0, 2, 3)

        def source(dx, dy, k):
            sx = (1 - x) if dx else x
            sy = (1 - y) if dy else y
            if k == 0:
                return sx, sy, z
            place = places[k]
            return sx, sy, jnp.where(upper, 3 - place, place)

        sent = [0] * len(PIECES)

        def push(p, dx, dy, k):
            sx, sy, sz = source(dx, dy, k)
            for hop in forwards(PIECES[p][0], dx, dy, k, end_case):
                sent[p] += 1
                copy(p, sx, sy, sz, core, peers[hop], send_sem.at[p], recv_sem.at[p, sx, sy, sz]).start()
            copy(p, sx, sy, sz, core, mate, pass_sem.at[p], got_sem.at[p, sx, sy, sz]).start()

        def first_product(units, fresh):
            terms = {0: [], 1: []}
            for unit in units:
                dx, dy, k = unit // 8, unit // 4 % 2, unit % 4
                sx, sy, sz = source(dx, dy, k)
                for p in range(len(PIECES)):
                    copy(p, sx, sy, sz, 1 - core, mate, pass_sem.at[p], got_sem.at[p, sx, sy, sz]).wait_recv()
                left, right = [], []
                for score in range(2):
                    spot = pl.multiple_of((score * 4 + sz) * SLAB, SLAB)
                    left.append(rows[0, sx, :, pl.ds(spot, SLAB)])
                    right.append(pl.ds(pl.multiple_of(sx * HALF + spot, SLAB), SLAB))
                terms[dy].append((jnp.concatenate(left, axis=1), right))
            for dy in range(2):
                if not terms[dy]:
                    continue
                half = (1 - y) if dy else y
                left = jnp.concatenate([term[0] for term in terms[dy]], axis=1)
                for start in range(0, HALF, 256):
                    right = [reach[half, spot, start:start + 256] for term in terms[dy] for spot in term[1]]
                    product = jnp.dot(left, jnp.concatenate(right, axis=0), preferred_element_type=jnp.float32)
                    if fresh:
                        total[half, :, start:start + 256] = product
                    else:
                        total[half, :, start:start + 256] += product

        for p in range(len(PIECES)):
            push(p, 0, 0, 0)
        rows[0, y] = reach[y, pl.ds(own_row, SLAB), :]
        groups = dict(END_GROUPS if end_case else MID_GROUPS)
        fresh = True
        for place, code in enumerate(END_ORDER if end_case else MID_ORDER):
            p, dx, dy, k = code // 16, code // 8 % 2, code // 4 % 2, code % 4
            sx, sy, sz = source(dx, dy, k)
            copy(p, sx, sy, sz, core, mate, send_sem.at[p], recv_sem.at[p, sx, sy, sz]).wait_recv()
            push(p, dx, dy, k)
            if place in groups:
                if fresh:
                    rows[0, 1 - y] = reach[1 - y, pl.ds(own_row, SLAB), :]
                first_product(groups[place], fresh)
                fresh = False

        def drain(p, count, semaphore):
            ref = reach.at[0, pl.ds(0, count * PIECES[p][2]), :]
            pltpu.make_async_remote_copy(
                src_ref=ref, dst_ref=ref, send_sem=semaphore, recv_sem=semaphore, device_id=mate, device_id_type=MESH
            ).wait_send()

        for p in range(len(PIECES)):
            drain(p, sent[p], send_sem.at[p])
            drain(p, 16, pass_sem.at[p])

    @pl.when(end)
    def _():
        gather(True)

    @pl.when(jnp.logical_not(end))
    def _():
        gather(False)

    for half in range(2):
        for start in range(0, HALF, 256):
            part = (0, half, slice(None), slice(start, start + 256))
            grown = total[half, :, start:start + 256] + rows[part].astype(jnp.float32)
            rows[part] = jnp.minimum(grown, 1.0).astype(jnp.bfloat16)

    def block(now, half, start, width=256):
        known = jnp.concatenate([rows[now, 0], rows[now, 1]], axis=1)
        product = jnp.dot(known, reach[half, :, start:start + width], preferred_element_type=jnp.float32)
        old = rows[now, half, :, start:start + width].astype(jnp.float32)
        return jnp.minimum(product + old, 1.0).astype(jnp.bfloat16)

    def step(now):
        for half in range(2):
            rows[1 - now, half] = block(now, half, 0, HALF)

    for count in range(STEPS - 2):
        step(count % 2)

    for start in range(0, HALF, 1024):
        out_ref[:, start:start + 1024] = block(1, y, start, 1024)


def solution(mesh):
    layout = P(('row', 'depth'), 'col')
    sends = len(PIECES)

    def local(slab):
        return pl.pallas_call(
            kernel,
            out_shape=pltpu.VMEM((SLAB, HALF), jnp.bfloat16),
            in_specs=[pl.BlockSpec(memory_space=pl.ANY)],
            out_specs=pl.BlockSpec(memory_space=pltpu.VMEM),
            scratch_shapes=[
                pltpu.VMEM((2, N, HALF), jnp.bfloat16),
                pltpu.VMEM((2, 2, SLAB, HALF), jnp.bfloat16),
                pltpu.VMEM((2, SLAB, HALF), jnp.float32),
                pltpu.SemaphoreType.DMA,
                pltpu.SemaphoreType.DMA((sends,)),
                pltpu.SemaphoreType.DMA((sends, 2, 2, 4)),
                pltpu.SemaphoreType.DMA((sends,)),
                pltpu.SemaphoreType.DMA((sends, 2, 2, 4)),
            ],
            compiler_params=pltpu.CompilerParams(collective_id=0, has_side_effects=True),
        )(slab)

    return jax.shard_map(local, mesh=mesh, in_specs=(layout,), out_specs=layout, check_vma=False)
```

```python
import jax
import jax.numpy as jnp
from jax import lax
from jax.experimental import pallas as pl
from jax.experimental.pallas import tpu as pltpu
from jax.sharding import PartitionSpec as P

N = 2048
SLAB = 128
HALF = 1024
STEPS = 15
MESH = pl.DeviceIdType.MESH

PIECES = (('zxy', 0, 48), ('zyx', 48, 48), ('yxz', 96, 32))
END_ORDER = (
    8, 4, 1, 24, 20, 17, 40, 36, 33, 9, 2, 12, 5, 18, 28, 25, 21, 41, 37, 34, 44, 13, 6, 10, 3, 26, 22, 19, 29, 35,
    14, 38, 42, 11, 7, 30, 23, 43, 39, 27, 45, 15, 47, 31, 46,
)
MID_ORDER = (
    1, 8, 4, 2, 17, 24, 20, 18, 33, 40, 36, 34, 3, 9, 10, 5, 41, 37, 19, 6, 12, 35, 38, 42, 25, 26, 28, 21, 22, 39,
    43, 45, 44, 7, 11, 47, 13, 14, 27, 46, 23, 29, 30, 15, 31,
)

END_GROUPS = ((10, (0, 1, 8, 4)), (24, (2, 9, 5, 12)), (36, (3, 10, 6)), (42, (11, 7, 13)), (44, (14, 15)))
MID_GROUPS = ((13, (0, 1, 8, 2, 4)), (29, (3, 9)), (34, (10, 5, 6, 12)), (43, (11, 7, 13)), (44, (14, 15)))
END_SECOND = 42
MID_SECOND = 43


def forwards(order, dx, dy, k, end):
    far = {'x': dx == 1, 'y': dy == 1, 'z': k != 0}
    last = max([i for i, axis in enumerate(order) if far[axis]], default=-1)
    hops = []
    for i, axis in enumerate(order):
        if axis == 'z' and i > last:
            hops += ['in'] if end else ['in', 'out']
        elif axis == 'z' and i == last and not end:
            hops += ['in'] if k == 1 else ['out']
        elif i > last:
            hops.append(axis)
    return hops


def kernel(in_ref, out_ref, reach, rows, total, more, in_sem, send_sem, recv_sem, pass_sem, got_sem):
    z, y, row = lax.axis_index('depth'), lax.axis_index('col'), lax.axis_index('row')
    x, core = row // 2, row % 2
    upper = z >= 2
    z_in = jnp.where(upper, z - 1, z + 1)
    z_out = jnp.where(upper, z + 1, z - 1)
    end = (z == 0) | (z == 3)
    x_row = (1 - x) * 2 + core
    mate_row = x * 2 + 1 - core
    peers = {
        'x': {'depth': z, 'col': y, 'row': x_row},
        'y': {'depth': z, 'col': 1 - y, 'row': row},
        'in': {'depth': z_in, 'col': y, 'row': row},
        'out': {'depth': z_out, 'col': y, 'row': row},
    }
    mate = {'depth': z, 'col': y, 'row': mate_row}

    def slab_at(sx, sy, sz, score):
        return sy, (sx * 2 + score) * 4 + sz

    own_half, own_block = slab_at(x, y, z, core)
    own_row = pl.multiple_of(own_block * SLAB, SLAB)
    load = pltpu.make_async_copy(in_ref, reach.at[own_half, pl.ds(own_row, SLAB), :], in_sem)
    load.start()

    barrier = pltpu.get_barrier_semaphore()
    for name in ('x', 'y', 'in'):
        pl.semaphore_signal(barrier, inc=1, device_id=peers[name], device_id_type=MESH)
    pl.semaphore_signal(barrier, inc=1, device_id=mate, device_id_type=MESH)

    @pl.when(jnp.logical_not(end))
    def _():
        pl.semaphore_signal(barrier, inc=1, device_id=peers['out'], device_id_type=MESH)
        pl.semaphore_wait(barrier, 5)

    @pl.when(end)
    def _():
        pl.semaphore_wait(barrier, 4)

    load.wait()

    def piece_ref(p, sx, sy, sz, score):
        half, block = slab_at(sx, sy, sz, score)
        start = pl.multiple_of(block * SLAB + PIECES[p][1], 16)
        return reach.at[half, pl.ds(start, PIECES[p][2]), :]

    def copy(p, sx, sy, sz, score, peer, send, recv):
        ref = piece_ref(p, sx, sy, sz, score)
        return pltpu.make_async_remote_copy(
            src_ref=ref, dst_ref=ref, send_sem=send, recv_sem=recv, device_id=peer, device_id_type=MESH
        )

    def gather(end_case):
        places = (0, 1, 2, 3) if end_case else (1, 0, 2, 3)

        def source(dx, dy, k):
            sx = (1 - x) if dx else x
            sy = (1 - y) if dy else y
            if k == 0:
                return sx, sy, z
            place = places[k]
            return sx, sy, jnp.where(upper, 3 - place, place)

        sent = [0] * len(PIECES)

        def push(p, dx, dy, k):
            sx, sy, sz = source(dx, dy, k)
            for hop in forwards(PIECES[p][0], dx, dy, k, end_case):
                sent[p] += 1
                copy(p, sx, sy, sz, core, peers[hop], send_sem.at[p], recv_sem.at[p, sx, sy, sz]).start()
            copy(p, sx, sy, sz, core, mate, pass_sem.at[p], got_sem.at[p, sx, sy, sz]).start()

        def first_product(units, fresh):
            terms = {0: [], 1: []}
            for unit in units:
                dx, dy, k = unit // 8, unit // 4 % 2, unit % 4
                sx, sy, sz = source(dx, dy, k)
                for p in range(len(PIECES)):
                    copy(p, sx, sy, sz, 1 - core, mate, pass_sem.at[p], got_sem.at[p, sx, sy, sz]).wait_recv()
                left, right = [], []
                for score in range(2):
                    spot = pl.multiple_of((score * 4 + sz) * SLAB, SLAB)
                    left.append(rows[0, sx, :, pl.ds(spot, SLAB)])
                    right.append(pl.ds(pl.multiple_of(sx * HALF + spot, SLAB), SLAB))
                terms[dy].append((jnp.concatenate(left, axis=1), right))
            for dy in range(2):
                if not terms[dy]:
                    continue
                half = (1 - y) if dy else y
                left = jnp.concatenate([term[0] for term in terms[dy]], axis=1)
                for start in range(0, HALF, 256):
                    right = [reach[half, spot, start:start + 256] for term in terms[dy] for spot in term[1]]
                    product = jnp.dot(left, jnp.concatenate(right, axis=0), preferred_element_type=jnp.float32)
                    if fresh:
                        total[half, :, start:start + 256] = product
                    else:
                        total[half, :, start:start + 256] += product

        def columns(sz, score):
            return pl.ds(pl.multiple_of((score * 4 + sz) * SLAB, SLAB), SLAB)

        def partial(places, start):
            left, right = [], []
            for k in places:
                _, _, sz = source(0, 0, k)
                for score in range(2):
                    spot = columns(sz, score)
                    left.append(rows[1, y, :, spot])
                    first = pl.multiple_of(y * HALF + (score * 4 + sz) * SLAB, SLAB)
                    right.append(reach[1 - y, pl.ds(first, SLAB), start:start + 256])
            return jnp.dot(
                jnp.concatenate(left, axis=1), jnp.concatenate(right, axis=0), preferred_element_type=jnp.float32
            )

        def second_product():
            for start in range(0, HALF, 256):
                grown = total[y, :, start:start + 256] + rows[0, y, :, start:start + 256].astype(jnp.float32)
                rows[1, y, :, start:start + 256] = jnp.minimum(grown, 1.0).astype(jnp.bfloat16)
            known = pl.ds(pl.multiple_of(y * HALF, HALF), HALF)
            for start in range(0, HALF, 256):
                more[y, :, start:start + 256] = jnp.dot(
                    rows[1, y], reach[y, known, start:start + 256], preferred_element_type=jnp.float32
                )

            @pl.when(x == y)
            def _():
                for start in range(0, HALF, 256):
                    more[1 - y, :, start:start + 256] = jnp.dot(
                        rows[1, y], reach[1 - y, known, start:start + 256], preferred_element_type=jnp.float32
                    )

            @pl.when(x != y)
            def _():
                for start in range(0, HALF, 256):
                    more[1 - y, :, start:start + 256] = partial((0, 1), start)

        for p in range(len(PIECES)):
            push(p, 0, 0, 0)
        rows[0, y] = reach[y, pl.ds(own_row, SLAB), :]
        groups = dict(END_GROUPS if end_case else MID_GROUPS)
        fresh = True
        for place, code in enumerate(END_ORDER if end_case else MID_ORDER):
            p, dx, dy, k = code // 16, code // 8 % 2, code // 4 % 2, code % 4
            sx, sy, sz = source(dx, dy, k)
            copy(p, sx, sy, sz, core, mate, send_sem.at[p], recv_sem.at[p, sx, sy, sz]).wait_recv()
            push(p, dx, dy, k)
            if place in groups:
                if fresh:
                    rows[0, 1 - y] = reach[1 - y, pl.ds(own_row, SLAB), :]
                first_product(groups[place], fresh)
                fresh = False
            if place == (END_SECOND if end_case else MID_SECOND):
                second_product()

        @pl.when(x != y)
        def _():
            for start in range(0, HALF, 256):
                more[1 - y, :, start:start + 256] += partial((2, 3), start)

        def drain(p, count, semaphore):
            ref = reach.at[0, pl.ds(0, count * PIECES[p][2]), :]
            pltpu.make_async_remote_copy(
                src_ref=ref, dst_ref=ref, send_sem=semaphore, recv_sem=semaphore, device_id=mate, device_id_type=MESH
            ).wait_send()

        for p in range(len(PIECES)):
            drain(p, sent[p], send_sem.at[p])
            drain(p, 16, pass_sem.at[p])

    @pl.when(end)
    def _():
        gather(True)

    @pl.when(jnp.logical_not(end))
    def _():
        gather(False)

    for start in range(0, HALF, 256):
        grown = total[1 - y, :, start:start + 256] + rows[0, 1 - y, :, start:start + 256].astype(jnp.float32)
        rows[1, 1 - y, :, start:start + 256] = jnp.minimum(grown, 1.0).astype(jnp.bfloat16)

    known = pl.ds(pl.multiple_of((1 - y) * HALF, HALF), HALF)
    for half in range(2):
        for start in range(0, HALF, 256):
            product = jnp.dot(
                rows[1, 1 - y], reach[half, known, start:start + 256], preferred_element_type=jnp.float32
            )
            grown = product + more[half, :, start:start + 256] + rows[1, half, :, start:start + 256].astype(jnp.float32)
            rows[0, half, :, start:start + 256] = jnp.minimum(grown, 1.0).astype(jnp.bfloat16)

    def block(now, half, start, width=256):
        known = jnp.concatenate([rows[now, 0], rows[now, 1]], axis=1)
        product = jnp.dot(known, reach[half, :, start:start + width], preferred_element_type=jnp.float32)
        old = rows[now, half, :, start:start + width].astype(jnp.float32)
        return jnp.minimum(product + old, 1.0).astype(jnp.bfloat16)

    def step(now):
        for half in range(2):
            rows[1 - now, half] = block(now, half, 0, HALF)

    for count in range(STEPS - 3):
        step(count % 2)

    for start in range(0, HALF, 1024):
        out_ref[:, start:start + 1024] = block(0, y, start, 1024)


def solution(mesh):
    layout = P(('row', 'depth'), 'col')
    sends = len(PIECES)

    def local(slab):
        return pl.pallas_call(
            kernel,
            out_shape=pltpu.VMEM((SLAB, HALF), jnp.bfloat16),
            in_specs=[pl.BlockSpec(memory_space=pl.ANY)],
            out_specs=pl.BlockSpec(memory_space=pltpu.VMEM),
            scratch_shapes=[
                pltpu.VMEM((2, N, HALF), jnp.bfloat16),
                pltpu.VMEM((2, 2, SLAB, HALF), jnp.bfloat16),
                pltpu.VMEM((2, SLAB, HALF), jnp.float32),
                pltpu.VMEM((2, SLAB, HALF), jnp.float32),
                pltpu.SemaphoreType.DMA,
                pltpu.SemaphoreType.DMA((sends,)),
                pltpu.SemaphoreType.DMA((sends, 2, 2, 4)),
                pltpu.SemaphoreType.DMA((sends,)),
                pltpu.SemaphoreType.DMA((sends, 2, 2, 4)),
            ],
            compiler_params=pltpu.CompilerParams(collective_id=0, has_side_effects=True),
        )(slab)

    return jax.shard_map(local, mesh=mesh, in_specs=(layout,), out_specs=layout, check_vma=False)
```

```python
import jax
import jax.numpy as jnp
from jax import lax
from jax.experimental import pallas as pl
from jax.experimental.pallas import tpu as pltpu
from jax.sharding import PartitionSpec as P

N = 2048
SLAB = 128
HALF = 1024
STEPS = 15
MESH = pl.DeviceIdType.MESH

PIECES = (('zxy', 0, 48), ('zyx', 48, 48), ('yxz', 96, 32))
END_ORDER = (
    8, 4, 1, 24, 20, 17, 40, 36, 33, 9, 2, 12, 5, 18, 28, 25, 21, 41, 37, 34, 44, 13, 6, 10, 3, 26, 22, 19, 29, 35,
    14, 38, 42, 11, 7, 30, 23, 43, 39, 27, 45, 15, 47, 31, 46,
)
MID_ORDER = (
    1, 8, 4, 2, 17, 24, 20, 18, 33, 40, 36, 34, 3, 9, 10, 5, 41, 37, 19, 6, 12, 35, 38, 42, 25, 26, 28, 21, 22, 39,
    43, 45, 44, 7, 11, 47, 13, 14, 27, 46, 23, 29, 30, 15, 31,
)

END_GROUPS = ((10, (0, 1, 8, 4)), (24, (2, 9, 5, 12)), (36, (3, 10, 6)), (44, (11, 7, 13)))
MID_GROUPS = ((13, (0, 1, 8, 2, 4)), (29, (3, 9)), (34, (10, 5, 6, 12)), (43, (11, 7, 13)))
LAST_GROUP = (14, 15)
END_SECOND = 44
MID_SECOND = 43


def forwards(order, dx, dy, k, end):
    far = {'x': dx == 1, 'y': dy == 1, 'z': k != 0}
    last = max([i for i, axis in enumerate(order) if far[axis]], default=-1)
    hops = []
    for i, axis in enumerate(order):
        if axis == 'z' and i > last:
            hops += ['in'] if end else ['in', 'out']
        elif axis == 'z' and i == last and not end:
            hops += ['in'] if k == 1 else ['out']
        elif i > last:
            hops.append(axis)
    return hops


def kernel(in_ref, out_ref, reach, rows, total, more, in_sem, send_sem, recv_sem, pass_sem, got_sem):
    z, y, row = lax.axis_index('depth'), lax.axis_index('col'), lax.axis_index('row')
    x, core = row // 2, row % 2
    upper = z >= 2
    z_in = jnp.where(upper, z - 1, z + 1)
    z_out = jnp.where(upper, z + 1, z - 1)
    end = (z == 0) | (z == 3)
    x_row = (1 - x) * 2 + core
    mate_row = x * 2 + 1 - core
    peers = {
        'x': {'depth': z, 'col': y, 'row': x_row},
        'y': {'depth': z, 'col': 1 - y, 'row': row},
        'in': {'depth': z_in, 'col': y, 'row': row},
        'out': {'depth': z_out, 'col': y, 'row': row},
    }
    mate = {'depth': z, 'col': y, 'row': mate_row}

    def slab_at(sx, sy, sz, score):
        return sy, (sx * 2 + score) * 4 + sz

    own_half, own_block = slab_at(x, y, z, core)
    own_row = pl.multiple_of(own_block * SLAB, SLAB)
    load = pltpu.make_async_copy(in_ref, reach.at[own_half, pl.ds(own_row, SLAB), :], in_sem)
    load.start()

    barrier = pltpu.get_barrier_semaphore()
    for name in ('x', 'y', 'in'):
        pl.semaphore_signal(barrier, inc=1, device_id=peers[name], device_id_type=MESH)
    pl.semaphore_signal(barrier, inc=1, device_id=mate, device_id_type=MESH)

    @pl.when(jnp.logical_not(end))
    def _():
        pl.semaphore_signal(barrier, inc=1, device_id=peers['out'], device_id_type=MESH)
        pl.semaphore_wait(barrier, 5)

    @pl.when(end)
    def _():
        pl.semaphore_wait(barrier, 4)

    load.wait()

    def piece_ref(p, sx, sy, sz, score):
        half, block = slab_at(sx, sy, sz, score)
        start = pl.multiple_of(block * SLAB + PIECES[p][1], 16)
        return reach.at[half, pl.ds(start, PIECES[p][2]), :]

    def copy(p, sx, sy, sz, score, peer, send, recv):
        ref = piece_ref(p, sx, sy, sz, score)
        return pltpu.make_async_remote_copy(
            src_ref=ref, dst_ref=ref, send_sem=send, recv_sem=recv, device_id=peer, device_id_type=MESH
        )

    def gather(end_case):
        places = (0, 1, 2, 3) if end_case else (1, 0, 2, 3)

        def source(dx, dy, k):
            sx = (1 - x) if dx else x
            sy = (1 - y) if dy else y
            if k == 0:
                return sx, sy, z
            place = places[k]
            return sx, sy, jnp.where(upper, 3 - place, place)

        sent = [0] * len(PIECES)

        def push(p, dx, dy, k):
            sx, sy, sz = source(dx, dy, k)
            for hop in forwards(PIECES[p][0], dx, dy, k, end_case):
                sent[p] += 1
                copy(p, sx, sy, sz, core, peers[hop], send_sem.at[p], recv_sem.at[p, sx, sy, sz]).start()
            copy(p, sx, sy, sz, core, mate, pass_sem.at[p], got_sem.at[p, sx, sy, sz]).start()

        def first_product(units, fresh):
            terms = {0: [], 1: []}
            for unit in units:
                dx, dy, k = unit // 8, unit // 4 % 2, unit % 4
                sx, sy, sz = source(dx, dy, k)
                for p in range(len(PIECES)):
                    copy(p, sx, sy, sz, 1 - core, mate, pass_sem.at[p], got_sem.at[p, sx, sy, sz]).wait_recv()
                left, right = [], []
                for score in range(2):
                    spot = pl.multiple_of((score * 4 + sz) * SLAB, SLAB)
                    left.append(rows[0, sx, :, pl.ds(spot, SLAB)])
                    right.append(pl.ds(pl.multiple_of(sx * HALF + spot, SLAB), SLAB))
                terms[dy].append((jnp.concatenate(left, axis=1), right))
            for dy in range(2):
                if not terms[dy]:
                    continue
                half = (1 - y) if dy else y
                left = jnp.concatenate([term[0] for term in terms[dy]], axis=1)
                for start in range(0, HALF, 256):
                    right = [reach[half, spot, start:start + 256] for term in terms[dy] for spot in term[1]]
                    product = jnp.dot(left, jnp.concatenate(right, axis=0), preferred_element_type=jnp.float32)
                    if fresh:
                        total[half, :, start:start + 256] = product
                    else:
                        total[half, :, start:start + 256] += product

        def columns(sz, score):
            return pl.ds(pl.multiple_of((score * 4 + sz) * SLAB, SLAB), SLAB)

        def partial(places, start):
            left, right = [], []
            for k in places:
                _, _, sz = source(0, 0, k)
                for score in range(2):
                    spot = columns(sz, score)
                    left.append(rows[1, y, :, spot])
                    first = pl.multiple_of(y * HALF + (score * 4 + sz) * SLAB, SLAB)
                    right.append(reach[1 - y, pl.ds(first, SLAB), start:start + 256])
            return jnp.dot(
                jnp.concatenate(left, axis=1), jnp.concatenate(right, axis=0), preferred_element_type=jnp.float32
            )

        def second_product():
            for start in range(0, HALF, 256):
                grown = total[y, :, start:start + 256] + rows[0, y, :, start:start + 256].astype(jnp.float32)
                rows[1, y, :, start:start + 256] = jnp.minimum(grown, 1.0).astype(jnp.bfloat16)
            known = pl.ds(pl.multiple_of(y * HALF, HALF), HALF)
            for start in range(0, HALF, 256):
                more[y, :, start:start + 256] = jnp.dot(
                    rows[1, y], reach[y, known, start:start + 256], preferred_element_type=jnp.float32
                )

            @pl.when(x == y)
            def _():
                for start in range(0, HALF, 256):
                    more[1 - y, :, start:start + 256] = jnp.dot(
                        rows[1, y], reach[1 - y, known, start:start + 256], preferred_element_type=jnp.float32
                    )

            @pl.when(x != y)
            def _():
                for start in range(0, HALF, 256):
                    more[1 - y, :, start:start + 256] = partial((0, 1), start)

        for p in range(len(PIECES)):
            push(p, 0, 0, 0)
        rows[0, y] = reach[y, pl.ds(own_row, SLAB), :]
        groups = dict(END_GROUPS if end_case else MID_GROUPS)
        fresh = True
        for place, code in enumerate(END_ORDER if end_case else MID_ORDER):
            p, dx, dy, k = code // 16, code // 8 % 2, code // 4 % 2, code % 4
            sx, sy, sz = source(dx, dy, k)
            copy(p, sx, sy, sz, core, mate, send_sem.at[p], recv_sem.at[p, sx, sy, sz]).wait_recv()
            push(p, dx, dy, k)
            if place in groups:
                if fresh:
                    rows[0, 1 - y] = reach[1 - y, pl.ds(own_row, SLAB), :]
                first_product(groups[place], fresh)
                fresh = False
            if place == (END_SECOND if end_case else MID_SECOND):
                second_product()

        first_product(LAST_GROUP, False)

        @pl.when(x != y)
        def _():
            for start in range(0, HALF, 256):
                more[1 - y, :, start:start + 256] += partial((2, 3), start)

        def drain(p, count, semaphore):
            ref = reach.at[0, pl.ds(0, count * PIECES[p][2]), :]
            pltpu.make_async_remote_copy(
                src_ref=ref, dst_ref=ref, send_sem=semaphore, recv_sem=semaphore, device_id=mate, device_id_type=MESH
            ).wait_send()

        for p in range(len(PIECES)):
            drain(p, sent[p], send_sem.at[p])
            drain(p, 16, pass_sem.at[p])

    @pl.when(end)
    def _():
        gather(True)

    @pl.when(jnp.logical_not(end))
    def _():
        gather(False)

    for start in range(0, HALF, 256):
        grown = total[1 - y, :, start:start + 256] + rows[0, 1 - y, :, start:start + 256].astype(jnp.float32)
        rows[1, 1 - y, :, start:start + 256] = jnp.minimum(grown, 1.0).astype(jnp.bfloat16)

    known = pl.ds(pl.multiple_of((1 - y) * HALF, HALF), HALF)
    for half in range(2):
        for start in range(0, HALF, 256):
            product = jnp.dot(
                rows[1, 1 - y], reach[half, known, start:start + 256], preferred_element_type=jnp.float32
            )
            grown = product + more[half, :, start:start + 256] + rows[1, half, :, start:start + 256].astype(jnp.float32)
            rows[0, half, :, start:start + 256] = jnp.minimum(grown, 1.0).astype(jnp.bfloat16)

    def block(now, half, start, width=256):
        known = jnp.concatenate([rows[now, 0], rows[now, 1]], axis=1)
        product = jnp.dot(known, reach[half, :, start:start + width], preferred_element_type=jnp.float32)
        old = rows[now, half, :, start:start + width].astype(jnp.float32)
        return jnp.minimum(product + old, 1.0).astype(jnp.bfloat16)

    def step(now):
        for half in range(2):
            rows[1 - now, half] = block(now, half, 0, HALF)

    for count in range(STEPS - 3):
        step(count % 2)

    for start in range(0, HALF, 1024):
        out_ref[:, start:start + 1024] = block(0, y, start, 1024)


def solution(mesh):
    layout = P(('row', 'depth'), 'col')
    sends = len(PIECES)

    def local(slab):
        return pl.pallas_call(
            kernel,
            out_shape=pltpu.VMEM((SLAB, HALF), jnp.bfloat16),
            in_specs=[pl.BlockSpec(memory_space=pl.ANY)],
            out_specs=pl.BlockSpec(memory_space=pltpu.VMEM),
            scratch_shapes=[
                pltpu.VMEM((2, N, HALF), jnp.bfloat16),
                pltpu.VMEM((2, 2, SLAB, HALF), jnp.bfloat16),
                pltpu.VMEM((2, SLAB, HALF), jnp.float32),
                pltpu.VMEM((2, SLAB, HALF), jnp.float32),
                pltpu.SemaphoreType.DMA,
                pltpu.SemaphoreType.DMA((sends,)),
                pltpu.SemaphoreType.DMA((sends, 2, 2, 4)),
                pltpu.SemaphoreType.DMA((sends,)),
                pltpu.SemaphoreType.DMA((sends, 2, 2, 4)),
            ],
            compiler_params=pltpu.CompilerParams(collective_id=0, has_side_effects=True),
        )(slab)

    return jax.shard_map(local, mesh=mesh, in_specs=(layout,), out_specs=layout, check_vma=False)
```

```python
import jax
import jax.numpy as jnp
from jax import lax
from jax.experimental import pallas as pl
from jax.experimental.pallas import tpu as pltpu
from jax.sharding import PartitionSpec as P

N = 2048
SLAB = 128
HALF = 1024
STEPS = 15
MESH = pl.DeviceIdType.MESH

PIECES = (('zxy', 0, 48), ('zyx', 48, 48), ('yxz', 96, 32))
END_ORDER = (
    8, 4, 1, 24, 20, 17, 40, 36, 33, 9, 2, 12, 5, 18, 28, 25, 21, 41, 37, 34, 44, 13, 6, 10, 3, 26, 22, 19, 29, 35,
    14, 38, 42, 11, 7, 30, 23, 43, 39, 27, 45, 15, 47, 31, 46,
)
MID_ORDER = (
    1, 8, 4, 2, 17, 24, 20, 18, 33, 40, 36, 34, 3, 9, 10, 5, 41, 37, 19, 6, 12, 35, 38, 42, 25, 26, 28, 21, 22, 39,
    43, 45, 44, 7, 11, 47, 13, 14, 27, 46, 23, 29, 30, 15, 31,
)

END_GROUPS = ((10, (0, 1, 8, 4)), (24, (2, 9, 5, 12)), (36, (3, 10, 6)), (41, (11, 7)), (43, (13,)))
MID_GROUPS = ((13, (0, 1, 8, 2, 4)), (29, (3, 9)), (34, (10, 5, 6, 12)), (43, (11, 7, 13)))
LAST_GROUP = (14, 15)
END_SECOND = 41
MID_SECOND = 43


def forwards(order, dx, dy, k, end):
    far = {'x': dx == 1, 'y': dy == 1, 'z': k != 0}
    last = max([i for i, axis in enumerate(order) if far[axis]], default=-1)
    hops = []
    for i, axis in enumerate(order):
        if axis == 'z' and i > last:
            hops += ['in'] if end else ['in', 'out']
        elif axis == 'z' and i == last and not end:
            hops += ['in'] if k == 1 else ['out']
        elif i > last:
            hops.append(axis)
    return hops


def kernel(in_ref, out_ref, reach, rows, total, more, in_sem, send_sem, recv_sem, pass_sem, got_sem):
    z, y, row = lax.axis_index('depth'), lax.axis_index('col'), lax.axis_index('row')
    x, core = row // 2, row % 2
    upper = z >= 2
    z_in = jnp.where(upper, z - 1, z + 1)
    z_out = jnp.where(upper, z + 1, z - 1)
    end = (z == 0) | (z == 3)
    x_row = (1 - x) * 2 + core
    mate_row = x * 2 + 1 - core
    peers = {
        'x': {'depth': z, 'col': y, 'row': x_row},
        'y': {'depth': z, 'col': 1 - y, 'row': row},
        'in': {'depth': z_in, 'col': y, 'row': row},
        'out': {'depth': z_out, 'col': y, 'row': row},
    }
    mate = {'depth': z, 'col': y, 'row': mate_row}

    def slab_at(sx, sy, sz, score):
        return sy, (sx * 2 + score) * 4 + sz

    own_half, own_block = slab_at(x, y, z, core)
    own_row = pl.multiple_of(own_block * SLAB, SLAB)
    load = pltpu.make_async_copy(in_ref, reach.at[own_half, pl.ds(own_row, SLAB), :], in_sem)
    load.start()

    barrier = pltpu.get_barrier_semaphore()
    for name in ('x', 'y', 'in'):
        pl.semaphore_signal(barrier, inc=1, device_id=peers[name], device_id_type=MESH)
    pl.semaphore_signal(barrier, inc=1, device_id=mate, device_id_type=MESH)

    @pl.when(jnp.logical_not(end))
    def _():
        pl.semaphore_signal(barrier, inc=1, device_id=peers['out'], device_id_type=MESH)
        pl.semaphore_wait(barrier, 5)

    @pl.when(end)
    def _():
        pl.semaphore_wait(barrier, 4)

    load.wait()

    def piece_ref(p, sx, sy, sz, score):
        half, block = slab_at(sx, sy, sz, score)
        start = pl.multiple_of(block * SLAB + PIECES[p][1], 16)
        return reach.at[half, pl.ds(start, PIECES[p][2]), :]

    def copy(p, sx, sy, sz, score, peer, send, recv):
        ref = piece_ref(p, sx, sy, sz, score)
        return pltpu.make_async_remote_copy(
            src_ref=ref, dst_ref=ref, send_sem=send, recv_sem=recv, device_id=peer, device_id_type=MESH
        )

    def gather(end_case):
        places = (0, 1, 2, 3) if end_case else (1, 0, 2, 3)

        def source(dx, dy, k):
            sx = (1 - x) if dx else x
            sy = (1 - y) if dy else y
            if k == 0:
                return sx, sy, z
            place = places[k]
            return sx, sy, jnp.where(upper, 3 - place, place)

        sent = [0] * len(PIECES)

        def push(p, dx, dy, k):
            sx, sy, sz = source(dx, dy, k)
            for hop in forwards(PIECES[p][0], dx, dy, k, end_case):
                sent[p] += 1
                copy(p, sx, sy, sz, core, peers[hop], send_sem.at[p], recv_sem.at[p, sx, sy, sz]).start()
            copy(p, sx, sy, sz, core, mate, pass_sem.at[p], got_sem.at[p, sx, sy, sz]).start()

        def first_product(units, fresh):
            terms = {0: [], 1: []}
            for unit in units:
                dx, dy, k = unit // 8, unit // 4 % 2, unit % 4
                sx, sy, sz = source(dx, dy, k)
                for p in range(len(PIECES)):
                    copy(p, sx, sy, sz, 1 - core, mate, pass_sem.at[p], got_sem.at[p, sx, sy, sz]).wait_recv()
                left, right = [], []
                for score in range(2):
                    spot = pl.multiple_of((score * 4 + sz) * SLAB, SLAB)
                    left.append(rows[0, sx, :, pl.ds(spot, SLAB)])
                    right.append(pl.ds(pl.multiple_of(sx * HALF + spot, SLAB), SLAB))
                terms[dy].append((jnp.concatenate(left, axis=1), right))
            for dy in range(2):
                if not terms[dy]:
                    continue
                half = (1 - y) if dy else y
                left = jnp.concatenate([term[0] for term in terms[dy]], axis=1)
                for start in range(0, HALF, 256):
                    right = [reach[half, spot, start:start + 256] for term in terms[dy] for spot in term[1]]
                    product = jnp.dot(left, jnp.concatenate(right, axis=0), preferred_element_type=jnp.float32)
                    if fresh:
                        total[half, :, start:start + 256] = product
                    else:
                        total[half, :, start:start + 256] += product

        def columns(sz, score):
            return pl.ds(pl.multiple_of((score * 4 + sz) * SLAB, SLAB), SLAB)

        def partial(places, start):
            left, right = [], []
            for k in places:
                _, _, sz = source(0, 0, k)
                for score in range(2):
                    spot = columns(sz, score)
                    left.append(rows[1, y, :, spot])
                    first = pl.multiple_of(y * HALF + (score * 4 + sz) * SLAB, SLAB)
                    right.append(reach[1 - y, pl.ds(first, SLAB), start:start + 256])
            return jnp.dot(
                jnp.concatenate(left, axis=1), jnp.concatenate(right, axis=0), preferred_element_type=jnp.float32
            )

        def second_product():
            for start in range(0, HALF, 256):
                grown = total[y, :, start:start + 256] + rows[0, y, :, start:start + 256].astype(jnp.float32)
                rows[1, y, :, start:start + 256] = jnp.minimum(grown, 1.0).astype(jnp.bfloat16)
            known = pl.ds(pl.multiple_of(y * HALF, HALF), HALF)
            for start in range(0, HALF, 256):
                more[y, :, start:start + 256] = jnp.dot(
                    rows[1, y], reach[y, known, start:start + 256], preferred_element_type=jnp.float32
                )

            @pl.when(x == y)
            def _():
                for start in range(0, HALF, 256):
                    more[1 - y, :, start:start + 256] = jnp.dot(
                        rows[1, y], reach[1 - y, known, start:start + 256], preferred_element_type=jnp.float32
                    )

            @pl.when(x != y)
            def _():
                for start in range(0, HALF, 256):
                    more[1 - y, :, start:start + 256] = partial((0,), start)

        for p in range(len(PIECES)):
            push(p, 0, 0, 0)
        rows[0, y] = reach[y, pl.ds(own_row, SLAB), :]
        groups = dict(END_GROUPS if end_case else MID_GROUPS)
        fresh = True
        for place, code in enumerate(END_ORDER if end_case else MID_ORDER):
            p, dx, dy, k = code // 16, code // 8 % 2, code // 4 % 2, code % 4
            sx, sy, sz = source(dx, dy, k)
            copy(p, sx, sy, sz, core, mate, send_sem.at[p], recv_sem.at[p, sx, sy, sz]).wait_recv()
            push(p, dx, dy, k)
            if place in groups:
                if fresh:
                    rows[0, 1 - y] = reach[1 - y, pl.ds(own_row, SLAB), :]
                first_product(groups[place], fresh)
                fresh = False
            if place == (END_SECOND if end_case else MID_SECOND):
                second_product()

        first_product(LAST_GROUP, False)

        @pl.when(x != y)
        def _():
            for start in range(0, HALF, 256):
                more[1 - y, :, start:start + 256] += partial((1, 2, 3), start)

        def drain(p, count, semaphore):
            ref = reach.at[0, pl.ds(0, count * PIECES[p][2]), :]
            pltpu.make_async_remote_copy(
                src_ref=ref, dst_ref=ref, send_sem=semaphore, recv_sem=semaphore, device_id=mate, device_id_type=MESH
            ).wait_send()

        for p in range(len(PIECES)):
            drain(p, sent[p], send_sem.at[p])
            drain(p, 16, pass_sem.at[p])

    @pl.when(end)
    def _():
        gather(True)

    @pl.when(jnp.logical_not(end))
    def _():
        gather(False)

    for start in range(0, HALF, 256):
        grown = total[1 - y, :, start:start + 256] + rows[0, 1 - y, :, start:start + 256].astype(jnp.float32)
        rows[1, 1 - y, :, start:start + 256] = jnp.minimum(grown, 1.0).astype(jnp.bfloat16)

    known = pl.ds(pl.multiple_of((1 - y) * HALF, HALF), HALF)
    for half in range(2):
        for start in range(0, HALF, 256):
            product = jnp.dot(
                rows[1, 1 - y], reach[half, known, start:start + 256], preferred_element_type=jnp.float32
            )
            grown = product + more[half, :, start:start + 256] + rows[1, half, :, start:start + 256].astype(jnp.float32)
            rows[0, half, :, start:start + 256] = jnp.minimum(grown, 1.0).astype(jnp.bfloat16)

    def block(now, half, start, width=256):
        known = jnp.concatenate([rows[now, 0], rows[now, 1]], axis=1)
        product = jnp.dot(known, reach[half, :, start:start + width], preferred_element_type=jnp.float32)
        old = rows[now, half, :, start:start + width].astype(jnp.float32)
        return jnp.minimum(product + old, 1.0).astype(jnp.bfloat16)

    def step(now):
        for half in range(2):
            rows[1 - now, half] = block(now, half, 0, HALF)

    for count in range(STEPS - 3):
        step(count % 2)

    for start in range(0, HALF, 1024):
        out_ref[:, start:start + 1024] = block(0, y, start, 1024)


def solution(mesh):
    layout = P(('row', 'depth'), 'col')
    sends = len(PIECES)

    def local(slab):
        return pl.pallas_call(
            kernel,
            out_shape=pltpu.VMEM((SLAB, HALF), jnp.bfloat16),
            in_specs=[pl.BlockSpec(memory_space=pl.ANY)],
            out_specs=pl.BlockSpec(memory_space=pltpu.VMEM),
            scratch_shapes=[
                pltpu.VMEM((2, N, HALF), jnp.bfloat16),
                pltpu.VMEM((2, 2, SLAB, HALF), jnp.bfloat16),
                pltpu.VMEM((2, SLAB, HALF), jnp.float32),
                pltpu.VMEM((2, SLAB, HALF), jnp.float32),
                pltpu.SemaphoreType.DMA,
                pltpu.SemaphoreType.DMA((sends,)),
                pltpu.SemaphoreType.DMA((sends, 2, 2, 4)),
                pltpu.SemaphoreType.DMA((sends,)),
                pltpu.SemaphoreType.DMA((sends, 2, 2, 4)),
            ],
            compiler_params=pltpu.CompilerParams(collective_id=0, has_side_effects=True),
        )(slab)

    return jax.shard_map(local, mesh=mesh, in_specs=(layout,), out_specs=layout, check_vma=False)
```

```python
import jax
import jax.numpy as jnp
from jax import lax
from jax.experimental import pallas as pl
from jax.experimental.pallas import tpu as pltpu
from jax.sharding import PartitionSpec as P

N = 2048
SLAB = 128
HALF = 1024
STEPS = 15
MESH = pl.DeviceIdType.MESH

PIECES = (('zxy', 0, 48), ('zyx', 48, 48), ('yxz', 96, 32))
END_ORDER = (
    8, 4, 1, 24, 20, 17, 40, 36, 33, 9, 2, 12, 5, 18, 28, 25, 21, 41, 37, 34, 44, 13, 6, 10, 3, 26, 22, 19, 29, 35,
    14, 38, 42, 11, 7, 30, 23, 43, 39, 27, 45, 15, 47, 31, 46,
)
MID_ORDER = (
    1, 8, 4, 2, 17, 24, 20, 18, 33, 40, 36, 34, 3, 9, 10, 5, 41, 37, 19, 6, 12, 35, 38, 42, 25, 26, 28, 21, 22, 39,
    43, 45, 44, 7, 11, 47, 13, 14, 27, 46, 23, 29, 30, 15, 31,
)

END_GROUPS = ((10, (0, 1, 8, 4)), (24, (2, 9, 5, 12)), (36, (3, 10, 6)), (41, (11, 7)), (43, (13,)))
MID_GROUPS = ((13, (0, 1, 8, 2, 4)), (29, (3, 9)), (34, (10, 5, 6, 12)), (43, (11, 7, 13)))
LAST_GROUP = (14, 15)
END_SECOND = 41
MID_SECOND = 43


def forwards(order, dx, dy, k, end):
    far = {'x': dx == 1, 'y': dy == 1, 'z': k != 0}
    last = max([i for i, axis in enumerate(order) if far[axis]], default=-1)
    hops = []
    for i, axis in enumerate(order):
        if axis == 'z' and i > last:
            hops += ['in'] if end else ['in', 'out']
        elif axis == 'z' and i == last and not end:
            hops += ['in'] if k == 1 else ['out']
        elif i > last:
            hops.append(axis)
    return hops


def kernel(in_ref, out_ref, reach, rows, total, more, in_sem, send_sem, recv_sem, pass_sem, got_sem, ready):
    z, y, row = lax.axis_index('depth'), lax.axis_index('col'), lax.axis_index('row')
    x, core = row // 2, row % 2
    upper = z >= 2
    z_in = jnp.where(upper, z - 1, z + 1)
    z_out = jnp.where(upper, z + 1, z - 1)
    end = (z == 0) | (z == 3)
    x_row = (1 - x) * 2 + core
    mate_row = x * 2 + 1 - core
    peers = {
        'x': {'depth': z, 'col': y, 'row': x_row},
        'y': {'depth': z, 'col': 1 - y, 'row': row},
        'in': {'depth': z_in, 'col': y, 'row': row},
        'out': {'depth': z_out, 'col': y, 'row': row},
    }
    mate = {'depth': z, 'col': y, 'row': mate_row}

    def slab_at(sx, sy, sz, score):
        return sy, (sx * 2 + score) * 4 + sz

    own_half, own_block = slab_at(x, y, z, core)
    own_row = pl.multiple_of(own_block * SLAB, SLAB)
    load = pltpu.make_async_copy(in_ref, reach.at[own_half, pl.ds(own_row, SLAB), :], in_sem)
    load.start()

    steps = (
        (x == 0, x == 1, peers['x']),
        (y == 0, y == 1, peers['y']),
        (z < 3, None, {'depth': z + 1, 'col': y, 'row': row}),
        (None, z > 0, {'depth': z - 1, 'col': y, 'row': row}),
    )
    barrier = pltpu.get_barrier_semaphore()
    pl.semaphore_signal(barrier, inc=1, device_id=mate, device_id_type=MESH)
    for outwards, _, peer in steps:
        if outwards is not None:
            @pl.when(outwards)
            def _():
                pl.semaphore_signal(barrier, inc=1, device_id=peer, device_id_type=MESH)

    pl.semaphore_wait(barrier, 1 + x + y + jnp.where(z > 0, 1, 0))
    for _, inwards, peer in steps:
        if inwards is not None:
            @pl.when(inwards)
            def _():
                pl.semaphore_signal(ready, inc=1, device_id=peer, device_id_type=MESH)

    is_inwards = {'x': x == 1, 'y': y == 1, 'in': upper, 'out': jnp.logical_not(upper)}
    further = (1 - x) + (1 - y) + jnp.where(z < 3, 1, 0)

    load.wait()

    def piece_ref(p, sx, sy, sz, score):
        half, block = slab_at(sx, sy, sz, score)
        start = pl.multiple_of(block * SLAB + PIECES[p][1], 16)
        return reach.at[half, pl.ds(start, PIECES[p][2]), :]

    def copy(p, sx, sy, sz, score, peer, send, recv):
        ref = piece_ref(p, sx, sy, sz, score)
        return pltpu.make_async_remote_copy(
            src_ref=ref, dst_ref=ref, send_sem=send, recv_sem=recv, device_id=peer, device_id_type=MESH
        )

    def gather(end_case):
        places = (0, 1, 2, 3) if end_case else (1, 0, 2, 3)

        def source(dx, dy, k):
            sx = (1 - x) if dx else x
            sy = (1 - y) if dy else y
            if k == 0:
                return sx, sy, z
            place = places[k]
            return sx, sy, jnp.where(upper, 3 - place, place)

        sent = [0] * len(PIECES)

        def push(p, dx, dy, k):
            sx, sy, sz = source(dx, dy, k)
            for hop in forwards(PIECES[p][0], dx, dy, k, end_case):
                sent[p] += 1
                copy(p, sx, sy, sz, core, peers[hop], send_sem.at[p], recv_sem.at[p, sx, sy, sz]).start()
            copy(p, sx, sy, sz, core, mate, pass_sem.at[p], got_sem.at[p, sx, sy, sz]).start()

        def first_product(units, fresh):
            terms = {0: [], 1: []}
            for unit in units:
                dx, dy, k = unit // 8, unit // 4 % 2, unit % 4
                sx, sy, sz = source(dx, dy, k)
                for p in range(len(PIECES)):
                    copy(p, sx, sy, sz, 1 - core, mate, pass_sem.at[p], got_sem.at[p, sx, sy, sz]).wait_recv()
                left, right = [], []
                for score in range(2):
                    spot = pl.multiple_of((score * 4 + sz) * SLAB, SLAB)
                    left.append(rows[0, sx, :, pl.ds(spot, SLAB)])
                    right.append(pl.ds(pl.multiple_of(sx * HALF + spot, SLAB), SLAB))
                terms[dy].append((jnp.concatenate(left, axis=1), right))
            for dy in range(2):
                if not terms[dy]:
                    continue
                half = (1 - y) if dy else y
                left = jnp.concatenate([term[0] for term in terms[dy]], axis=1)
                for start in range(0, HALF, 256):
                    right = [reach[half, spot, start:start + 256] for term in terms[dy] for spot in term[1]]
                    product = jnp.dot(left, jnp.concatenate(right, axis=0), preferred_element_type=jnp.float32)
                    if fresh:
                        total[half, :, start:start + 256] = product
                    else:
                        total[half, :, start:start + 256] += product

        def columns(sz, score):
            return pl.ds(pl.multiple_of((score * 4 + sz) * SLAB, SLAB), SLAB)

        def partial(places, start):
            left, right = [], []
            for k in places:
                _, _, sz = source(0, 0, k)
                for score in range(2):
                    spot = columns(sz, score)
                    left.append(rows[1, y, :, spot])
                    first = pl.multiple_of(y * HALF + (score * 4 + sz) * SLAB, SLAB)
                    right.append(reach[1 - y, pl.ds(first, SLAB), start:start + 256])
            return jnp.dot(
                jnp.concatenate(left, axis=1), jnp.concatenate(right, axis=0), preferred_element_type=jnp.float32
            )

        def second_product():
            for start in range(0, HALF, 256):
                grown = total[y, :, start:start + 256] + rows[0, y, :, start:start + 256].astype(jnp.float32)
                rows[1, y, :, start:start + 256] = jnp.minimum(grown, 1.0).astype(jnp.bfloat16)
            known = pl.ds(pl.multiple_of(y * HALF, HALF), HALF)
            for start in range(0, HALF, 256):
                more[y, :, start:start + 256] = jnp.dot(
                    rows[1, y], reach[y, known, start:start + 256], preferred_element_type=jnp.float32
                )

            @pl.when(x == y)
            def _():
                for start in range(0, HALF, 256):
                    more[1 - y, :, start:start + 256] = jnp.dot(
                        rows[1, y], reach[1 - y, known, start:start + 256], preferred_element_type=jnp.float32
                    )

            @pl.when(x != y)
            def _():
                for start in range(0, HALF, 256):
                    more[1 - y, :, start:start + 256] = partial((0,), start)

        def first_push(inwards):
            for p in range(len(PIECES)):
                for hop in forwards(PIECES[p][0], 0, 0, 0, end_case):
                    @pl.when(is_inwards[hop] if inwards else jnp.logical_not(is_inwards[hop]))
                    def _():
                        copy(p, x, y, z, core, peers[hop], send_sem.at[p], recv_sem.at[p, x, y, z]).start()

        first_push(True)
        for p in range(len(PIECES)):
            sent[p] += len(forwards(PIECES[p][0], 0, 0, 0, end_case))
            copy(p, x, y, z, core, mate, pass_sem.at[p], got_sem.at[p, x, y, z]).start()

        @pl.when(further > 0)
        def _():
            pl.semaphore_wait(ready, further)

        first_push(False)
        rows[0, y] = reach[y, pl.ds(own_row, SLAB), :]
        groups = dict(END_GROUPS if end_case else MID_GROUPS)
        fresh = True
        for place, code in enumerate(END_ORDER if end_case else MID_ORDER):
            p, dx, dy, k = code // 16, code // 8 % 2, code // 4 % 2, code % 4
            sx, sy, sz = source(dx, dy, k)
            copy(p, sx, sy, sz, core, mate, send_sem.at[p], recv_sem.at[p, sx, sy, sz]).wait_recv()
            push(p, dx, dy, k)
            if place in groups:
                if fresh:
                    rows[0, 1 - y] = reach[1 - y, pl.ds(own_row, SLAB), :]
                first_product(groups[place], fresh)
                fresh = False
            if place == (END_SECOND if end_case else MID_SECOND):
                second_product()

        first_product(LAST_GROUP, False)

        @pl.when(x != y)
        def _():
            for start in range(0, HALF, 256):
                more[1 - y, :, start:start + 256] += partial((1, 2, 3), start)

        def drain(p, count, semaphore):
            ref = reach.at[0, pl.ds(0, count * PIECES[p][2]), :]
            pltpu.make_async_remote_copy(
                src_ref=ref, dst_ref=ref, send_sem=semaphore, recv_sem=semaphore, device_id=mate, device_id_type=MESH
            ).wait_send()

        for p in range(len(PIECES)):
            drain(p, sent[p], send_sem.at[p])
            drain(p, 16, pass_sem.at[p])

    @pl.when(end)
    def _():
        gather(True)

    @pl.when(jnp.logical_not(end))
    def _():
        gather(False)

    for start in range(0, HALF, 256):
        grown = total[1 - y, :, start:start + 256] + rows[0, 1 - y, :, start:start + 256].astype(jnp.float32)
        rows[1, 1 - y, :, start:start + 256] = jnp.minimum(grown, 1.0).astype(jnp.bfloat16)

    known = pl.ds(pl.multiple_of((1 - y) * HALF, HALF), HALF)
    for half in range(2):
        for start in range(0, HALF, 256):
            product = jnp.dot(
                rows[1, 1 - y], reach[half, known, start:start + 256], preferred_element_type=jnp.float32
            )
            grown = product + more[half, :, start:start + 256] + rows[1, half, :, start:start + 256].astype(jnp.float32)
            rows[0, half, :, start:start + 256] = jnp.minimum(grown, 1.0).astype(jnp.bfloat16)

    def block(now, half, start, width=256):
        known = jnp.concatenate([rows[now, 0], rows[now, 1]], axis=1)
        product = jnp.dot(known, reach[half, :, start:start + width], preferred_element_type=jnp.float32)
        old = rows[now, half, :, start:start + width].astype(jnp.float32)
        return jnp.minimum(product + old, 1.0).astype(jnp.bfloat16)

    def step(now):
        for half in range(2):
            rows[1 - now, half] = block(now, half, 0, HALF)

    for count in range(STEPS - 3):
        step(count % 2)

    for start in range(0, HALF, 1024):
        out_ref[:, start:start + 1024] = block(0, y, start, 1024)


def solution(mesh):
    layout = P(('row', 'depth'), 'col')
    sends = len(PIECES)

    def local(slab):
        return pl.pallas_call(
            kernel,
            out_shape=pltpu.VMEM((SLAB, HALF), jnp.bfloat16),
            in_specs=[pl.BlockSpec(memory_space=pl.ANY)],
            out_specs=pl.BlockSpec(memory_space=pltpu.VMEM),
            scratch_shapes=[
                pltpu.VMEM((2, N, HALF), jnp.bfloat16),
                pltpu.VMEM((2, 2, SLAB, HALF), jnp.bfloat16),
                pltpu.VMEM((2, SLAB, HALF), jnp.float32),
                pltpu.VMEM((2, SLAB, HALF), jnp.float32),
                pltpu.SemaphoreType.DMA,
                pltpu.SemaphoreType.DMA((sends,)),
                pltpu.SemaphoreType.DMA((sends, 2, 2, 4)),
                pltpu.SemaphoreType.DMA((sends,)),
                pltpu.SemaphoreType.DMA((sends, 2, 2, 4)),
                pltpu.SemaphoreType.REGULAR,
            ],
            compiler_params=pltpu.CompilerParams(collective_id=0, has_side_effects=True),
        )(slab)

    return jax.shard_map(local, mesh=mesh, in_specs=(layout,), out_specs=layout, check_vma=False)
```

```python
import jax
import jax.numpy as jnp
from jax import lax
from jax.experimental import pallas as pl
from jax.experimental.pallas import tpu as pltpu
from jax.sharding import PartitionSpec as P

N = 2048
SLAB = 128
HALF = 1024
STEPS = 15
MESH = pl.DeviceIdType.MESH

PIECES = (('zxy', 0, 48), ('zyx', 48, 48), ('yxz', 96, 32))
END_ORDER = (
    8, 4, 1, 24, 20, 17, 40, 36, 33, 9, 2, 12, 5, 18, 28, 25, 21, 41, 37, 34, 44, 13, 6, 10, 3, 26, 22, 19, 29, 35,
    14, 38, 42, 11, 7, 30, 23, 43, 39, 27, 45, 15, 47, 31, 46,
)
MID_ORDER = (
    1, 8, 4, 2, 17, 24, 20, 18, 33, 40, 36, 34, 3, 9, 10, 5, 41, 37, 19, 6, 12, 35, 38, 42, 25, 26, 28, 21, 22, 39,
    43, 45, 44, 7, 11, 47, 13, 14, 27, 46, 23, 29, 30, 15, 31,
)

END_GROUPS = ((10, (0, 1, 8, 4)), (24, (2, 9, 5, 12)), (36, (3, 10, 6)), (41, (11, 7)), (43, (13,)))
MID_GROUPS = ((13, (0, 1, 8, 2, 4)), (29, (3, 9)), (34, (10, 5, 6, 12)), (43, (11, 7, 13)))
LAST_GROUP = (14, 15)
END_SECOND = 41
MID_SECOND = 43


def forwards(order, dx, dy, k, end):
    far = {'x': dx == 1, 'y': dy == 1, 'z': k != 0}
    last = max([i for i, axis in enumerate(order) if far[axis]], default=-1)
    hops = []
    for i, axis in enumerate(order):
        if axis == 'z' and i > last:
            hops += ['in'] if end else ['in', 'out']
        elif axis == 'z' and i == last and not end:
            hops += ['in'] if k == 1 else ['out']
        elif i > last:
            hops.append(axis)
    return hops


def kernel(in_ref, out_ref, reach, rows, total, more, in_sem, send_sem, recv_sem, pass_sem, got_sem, ready):
    z, y, row = lax.axis_index('depth'), lax.axis_index('col'), lax.axis_index('row')
    x, core = row // 2, row % 2
    upper = z >= 2
    z_in = jnp.where(upper, z - 1, z + 1)
    z_out = jnp.where(upper, z + 1, z - 1)
    end = (z == 0) | (z == 3)
    x_row = (1 - x) * 2 + core
    mate_row = x * 2 + 1 - core
    peers = {
        'x': {'depth': z, 'col': y, 'row': x_row},
        'y': {'depth': z, 'col': 1 - y, 'row': row},
        'in': {'depth': z_in, 'col': y, 'row': row},
        'out': {'depth': z_out, 'col': y, 'row': row},
    }
    mate = {'depth': z, 'col': y, 'row': mate_row}

    def slab_at(sx, sy, sz, score):
        return sy, (sx * 2 + score) * 4 + sz

    own_half, own_block = slab_at(x, y, z, core)
    own_row = pl.multiple_of(own_block * SLAB, SLAB)
    load = pltpu.make_async_copy(in_ref, reach.at[own_half, pl.ds(own_row, SLAB), :], in_sem)
    load.start()

    steps = (
        (x == 0, x == 1, peers['x']),
        (y == 0, y == 1, peers['y']),
        (z < 3, None, {'depth': z + 1, 'col': y, 'row': row}),
        (None, z > 0, {'depth': z - 1, 'col': y, 'row': row}),
    )
    barrier = pltpu.get_barrier_semaphore()
    pl.semaphore_signal(barrier, inc=1, device_id=mate, device_id_type=MESH)
    for outwards, _, peer in steps:
        if outwards is not None:
            @pl.when(outwards)
            def _():
                pl.semaphore_signal(barrier, inc=1, device_id=peer, device_id_type=MESH)

    pl.semaphore_wait(barrier, 1 + x + y + jnp.where(z > 0, 1, 0))
    for _, inwards, peer in steps:
        if inwards is not None:
            @pl.when(inwards)
            def _():
                pl.semaphore_signal(ready, inc=1, device_id=peer, device_id_type=MESH)

    is_inwards = {'x': x == 1, 'y': y == 1, 'in': upper, 'out': jnp.logical_not(upper)}
    further = (1 - x) + (1 - y) + jnp.where(z < 3, 1, 0)

    load.wait()

    def piece_ref(p, sx, sy, sz, score):
        half, block = slab_at(sx, sy, sz, score)
        start = pl.multiple_of(block * SLAB + PIECES[p][1], 16)
        return reach.at[half, pl.ds(start, PIECES[p][2]), :]

    def copy(p, sx, sy, sz, score, peer, send, recv):
        ref = piece_ref(p, sx, sy, sz, score)
        return pltpu.make_async_remote_copy(
            src_ref=ref, dst_ref=ref, send_sem=send, recv_sem=recv, device_id=peer, device_id_type=MESH
        )

    def await_mate(units, source):
        for unit in units:
            sx, sy, sz = source(unit // 8, unit // 4 % 2, unit % 4)
            for p in range(len(PIECES)):
                copy(p, sx, sy, sz, 1 - core, mate, pass_sem.at[p], got_sem.at[p, sx, sy, sz]).wait_recv()

    def first_product(units, fresh, source):
        terms = {0: [], 1: []}
        for unit in units:
            dx, dy, k = unit // 8, unit // 4 % 2, unit % 4
            sx, sy, sz = source(dx, dy, k)
            left, right = [], []
            for score in range(2):
                spot = pl.multiple_of((score * 4 + sz) * SLAB, SLAB)
                left.append(rows[0, sx, :, pl.ds(spot, SLAB)])
                right.append(pl.ds(pl.multiple_of(sx * HALF + spot, SLAB), SLAB))
            terms[dy].append((jnp.concatenate(left, axis=1), right))
        for dy in range(2):
            if not terms[dy]:
                continue
            half = (1 - y) if dy else y
            left = jnp.concatenate([term[0] for term in terms[dy]], axis=1)
            for start in range(0, HALF, 256):
                right = [reach[half, spot, start:start + 256] for term in terms[dy] for spot in term[1]]
                product = jnp.dot(left, jnp.concatenate(right, axis=0), preferred_element_type=jnp.float32)
                if fresh:
                    total[half, :, start:start + 256] = product
                else:
                    total[half, :, start:start + 256] += product

    def columns(sz, score):
        return pl.ds(pl.multiple_of((score * 4 + sz) * SLAB, SLAB), SLAB)

    def partial(places, start, source):
        left, right = [], []
        for k in places:
            _, _, sz = source(0, 0, k)
            for score in range(2):
                spot = columns(sz, score)
                left.append(rows[1, y, :, spot])
                first = pl.multiple_of(y * HALF + (score * 4 + sz) * SLAB, SLAB)
                right.append(reach[1 - y, pl.ds(first, SLAB), start:start + 256])
        return jnp.dot(
            jnp.concatenate(left, axis=1), jnp.concatenate(right, axis=0), preferred_element_type=jnp.float32
        )

    counts = []

    def gather(end_case):
        places = (0, 1, 2, 3) if end_case else (1, 0, 2, 3)

        def source(dx, dy, k):
            sx = (1 - x) if dx else x
            sy = (1 - y) if dy else y
            if k == 0:
                return sx, sy, z
            place = places[k]
            return sx, sy, jnp.where(upper, 3 - place, place)

        sent = [0] * len(PIECES)

        def push(p, dx, dy, k):
            sx, sy, sz = source(dx, dy, k)
            for hop in forwards(PIECES[p][0], dx, dy, k, end_case):
                sent[p] += 1
                copy(p, sx, sy, sz, core, peers[hop], send_sem.at[p], recv_sem.at[p, sx, sy, sz]).start()
            copy(p, sx, sy, sz, core, mate, pass_sem.at[p], got_sem.at[p, sx, sy, sz]).start()

        def second_product():
            for start in range(0, HALF, 256):
                grown = total[y, :, start:start + 256] + rows[0, y, :, start:start + 256].astype(jnp.float32)
                rows[1, y, :, start:start + 256] = jnp.minimum(grown, 1.0).astype(jnp.bfloat16)
            known = pl.ds(pl.multiple_of(y * HALF, HALF), HALF)
            for start in range(0, HALF, 256):
                more[y, :, start:start + 256] = jnp.dot(
                    rows[1, y], reach[y, known, start:start + 256], preferred_element_type=jnp.float32
                )

            @pl.when(x == y)
            def _():
                for start in range(0, HALF, 256):
                    more[1 - y, :, start:start + 256] = jnp.dot(
                        rows[1, y], reach[1 - y, known, start:start + 256], preferred_element_type=jnp.float32
                    )

            @pl.when(x != y)
            def _():
                for start in range(0, HALF, 256):
                    more[1 - y, :, start:start + 256] = partial((0,), start, source)

        def first_push(inwards):
            for p in range(len(PIECES)):
                for hop in forwards(PIECES[p][0], 0, 0, 0, end_case):
                    @pl.when(is_inwards[hop] if inwards else jnp.logical_not(is_inwards[hop]))
                    def _():
                        copy(p, x, y, z, core, peers[hop], send_sem.at[p], recv_sem.at[p, x, y, z]).start()

        first_push(True)
        for p in range(len(PIECES)):
            sent[p] += len(forwards(PIECES[p][0], 0, 0, 0, end_case))
            copy(p, x, y, z, core, mate, pass_sem.at[p], got_sem.at[p, x, y, z]).start()

        @pl.when(further > 0)
        def _():
            pl.semaphore_wait(ready, further)

        first_push(False)
        rows[0, y] = reach[y, pl.ds(own_row, SLAB), :]
        groups = dict(END_GROUPS if end_case else MID_GROUPS)
        fresh = True
        for place, code in enumerate(END_ORDER if end_case else MID_ORDER):
            p, dx, dy, k = code // 16, code // 8 % 2, code // 4 % 2, code % 4
            sx, sy, sz = source(dx, dy, k)
            copy(p, sx, sy, sz, core, mate, send_sem.at[p], recv_sem.at[p, sx, sy, sz]).wait_recv()
            push(p, dx, dy, k)
            if place in groups:
                if fresh:
                    rows[0, 1 - y] = reach[1 - y, pl.ds(own_row, SLAB), :]
                await_mate(groups[place], source)
                first_product(groups[place], fresh, source)
                fresh = False
            if place == (END_SECOND if end_case else MID_SECOND):
                second_product()

        counts.append(sent)

    @pl.when(end)
    def _():
        gather(True)

    @pl.when(jnp.logical_not(end))
    def _():
        gather(False)

    def last_source(dx, dy, k):
        place = k if k > 1 else jnp.where(end, 1, 0)
        return (1 - x) if dx else x, (1 - y) if dy else y, jnp.where(upper, 3 - place, place)

    await_mate(LAST_GROUP, last_source)

    @pl.when(x != y)
    def _():
        for start in range(0, HALF, 256):
            more[1 - y, :, start:start + 256] += partial((1, 2, 3), start, last_source)

    first_product(LAST_GROUP, False, last_source)
    for start in range(0, HALF, 256):
        grown = total[1 - y, :, start:start + 256] + rows[0, 1 - y, :, start:start + 256].astype(jnp.float32)
        rows[1, 1 - y, :, start:start + 256] = jnp.minimum(grown, 1.0).astype(jnp.bfloat16)

    known = pl.ds(pl.multiple_of((1 - y) * HALF, HALF), HALF)
    for half in range(2):
        for start in range(0, HALF, 256):
            product = jnp.dot(
                rows[1, 1 - y], reach[half, known, start:start + 256], preferred_element_type=jnp.float32
            )
            grown = product + more[half, :, start:start + 256] + rows[1, half, :, start:start + 256].astype(jnp.float32)
            rows[0, half, :, start:start + 256] = jnp.minimum(grown, 1.0).astype(jnp.bfloat16)

    def block(now, half, start, width=256):
        known = jnp.concatenate([rows[now, 0], rows[now, 1]], axis=1)
        product = jnp.dot(known, reach[half, :, start:start + width], preferred_element_type=jnp.float32)
        old = rows[now, half, :, start:start + width].astype(jnp.float32)
        return jnp.minimum(product + old, 1.0).astype(jnp.bfloat16)

    def step(now):
        for half in range(2):
            rows[1 - now, half] = block(now, half, 0, HALF)

    for count in range(STEPS - 3):
        step(count % 2)

    for start in range(0, HALF, 1024):
        out_ref[:, start:start + 1024] = block(0, y, start, 1024)

    def drain(p, count, semaphore):
        ref = reach.at[0, pl.ds(0, count * PIECES[p][2]), :]
        pltpu.make_async_remote_copy(
            src_ref=ref, dst_ref=ref, send_sem=semaphore, recv_sem=semaphore, device_id=mate, device_id_type=MESH
        ).wait_send()

    def drain_all(sent):
        for p in range(len(PIECES)):
            drain(p, sent[p], send_sem.at[p])
            drain(p, 16, pass_sem.at[p])

    @pl.when(end)
    def _():
        drain_all(counts[0])

    @pl.when(jnp.logical_not(end))
    def _():
        drain_all(counts[1])


def solution(mesh):
    layout = P(('row', 'depth'), 'col')
    sends = len(PIECES)

    def local(slab):
        return pl.pallas_call(
            kernel,
            out_shape=pltpu.VMEM((SLAB, HALF), jnp.bfloat16),
            in_specs=[pl.BlockSpec(memory_space=pl.ANY)],
            out_specs=pl.BlockSpec(memory_space=pltpu.VMEM),
            scratch_shapes=[
                pltpu.VMEM((2, N, HALF), jnp.bfloat16),
                pltpu.VMEM((2, 2, SLAB, HALF), jnp.bfloat16),
                pltpu.VMEM((2, SLAB, HALF), jnp.float32),
                pltpu.VMEM((2, SLAB, HALF), jnp.float32),
                pltpu.SemaphoreType.DMA,
                pltpu.SemaphoreType.DMA((sends,)),
                pltpu.SemaphoreType.DMA((sends, 2, 2, 4)),
                pltpu.SemaphoreType.DMA((sends,)),
                pltpu.SemaphoreType.DMA((sends, 2, 2, 4)),
                pltpu.SemaphoreType.REGULAR,
            ],
            compiler_params=pltpu.CompilerParams(collective_id=0, has_side_effects=True),
        )(slab)

    return jax.shard_map(local, mesh=mesh, in_specs=(layout,), out_specs=layout, check_vma=False)
```

```python
import jax
import jax.numpy as jnp
from jax import lax
from jax.experimental import pallas as pl
from jax.experimental.pallas import tpu as pltpu
from jax.sharding import PartitionSpec as P

N = 2048
SLAB = 128
HALF = 1024
STEPS = 15
MESH = pl.DeviceIdType.MESH

PIECES = (('zxy', 0, 48), ('zyx', 48, 48), ('yxz', 96, 32))
END_ORDER = (
    8, 4, 1, 24, 20, 17, 40, 36, 33, 9, 2, 12, 5, 18, 28, 25, 21, 41, 37, 34, 44, 13, 6, 10, 3, 26, 22, 19, 29, 35,
    14, 38, 42, 11, 7, 30, 23, 43, 39, 27, 45, 15, 47, 31, 46,
)
MID_ORDER = (
    1, 8, 4, 2, 17, 24, 20, 18, 33, 40, 36, 34, 3, 9, 10, 5, 41, 37, 19, 6, 12, 35, 38, 42, 25, 26, 28, 21, 22, 39,
    43, 45, 44, 7, 11, 47, 13, 14, 27, 46, 23, 29, 30, 15, 31,
)

END_GROUPS = ((10, (0, 1, 8, 4)), (24, (2, 9, 5, 12)), (36, (3, 10, 6)), (41, (11, 7)), (43, (13,)))
MID_GROUPS = ((13, (0, 1, 8, 2, 4)), (29, (3, 9)), (34, (10, 5, 6, 12)), (43, (11, 7, 13)))
END_SECOND = 41
MID_SECOND = 43


def forwards(order, dx, dy, k, end):
    far = {'x': dx == 1, 'y': dy == 1, 'z': k != 0}
    last = max([i for i, axis in enumerate(order) if far[axis]], default=-1)
    hops = []
    for i, axis in enumerate(order):
        if axis == 'z' and i > last:
            hops += ['in'] if end else ['in', 'out']
        elif axis == 'z' and i == last and not end:
            hops += ['in'] if k == 1 else ['out']
        elif i > last:
            hops.append(axis)
    return hops


def kernel(in_ref, out_ref, reach, rows, total, more, in_sem, send_sem, recv_sem, pass_sem, got_sem, ready):
    z, y, row = lax.axis_index('depth'), lax.axis_index('col'), lax.axis_index('row')
    x, core = row // 2, row % 2
    upper = z >= 2
    z_in = jnp.where(upper, z - 1, z + 1)
    z_out = jnp.where(upper, z + 1, z - 1)
    end = (z == 0) | (z == 3)
    x_row = (1 - x) * 2 + core
    mate_row = x * 2 + 1 - core
    peers = {
        'x': {'depth': z, 'col': y, 'row': x_row},
        'y': {'depth': z, 'col': 1 - y, 'row': row},
        'in': {'depth': z_in, 'col': y, 'row': row},
        'out': {'depth': z_out, 'col': y, 'row': row},
    }
    mate = {'depth': z, 'col': y, 'row': mate_row}

    def slab_at(sx, sy, sz, score):
        return sy, (sx * 2 + score) * 4 + sz

    own_half, own_block = slab_at(x, y, z, core)
    own_row = pl.multiple_of(own_block * SLAB, SLAB)
    load = pltpu.make_async_copy(in_ref, reach.at[own_half, pl.ds(own_row, SLAB), :], in_sem)
    load.start()

    steps = (
        (x == 0, x == 1, peers['x']),
        (y == 0, y == 1, peers['y']),
        (z < 3, None, {'depth': z + 1, 'col': y, 'row': row}),
        (None, z > 0, {'depth': z - 1, 'col': y, 'row': row}),
    )
    barrier = pltpu.get_barrier_semaphore()
    pl.semaphore_signal(barrier, inc=1, device_id=mate, device_id_type=MESH)
    for outwards, _, peer in steps:
        if outwards is not None:
            @pl.when(outwards)
            def _():
                pl.semaphore_signal(barrier, inc=1, device_id=peer, device_id_type=MESH)

    pl.semaphore_wait(barrier, 1 + x + y + jnp.where(z > 0, 1, 0))
    for _, inwards, peer in steps:
        if inwards is not None:
            @pl.when(inwards)
            def _():
                pl.semaphore_signal(ready, inc=1, device_id=peer, device_id_type=MESH)

    is_inwards = {'x': x == 1, 'y': y == 1, 'in': upper, 'out': jnp.logical_not(upper)}
    further = (1 - x) + (1 - y) + jnp.where(z < 3, 1, 0)

    load.wait()

    def piece_ref(p, sx, sy, sz, score):
        half, block = slab_at(sx, sy, sz, score)
        start = pl.multiple_of(block * SLAB + PIECES[p][1], 16)
        return reach.at[half, pl.ds(start, PIECES[p][2]), :]

    def copy(p, sx, sy, sz, score, peer, send, recv):
        ref = piece_ref(p, sx, sy, sz, score)
        return pltpu.make_async_remote_copy(
            src_ref=ref, dst_ref=ref, send_sem=send, recv_sem=recv, device_id=peer, device_id_type=MESH
        )

    def parts(unit):
        return unit if isinstance(unit, tuple) else (unit // 8, unit // 4 % 2, unit % 4)

    def await_mate(units, source):
        for unit in units:
            sx, sy, sz = source(*parts(unit))
            for p in range(len(PIECES)):
                copy(p, sx, sy, sz, 1 - core, mate, pass_sem.at[p], got_sem.at[p, sx, sy, sz]).wait_recv()

    def first_product(units, fresh, source):
        terms = {0: [], 1: []}
        for unit in units:
            dx, dy, k = parts(unit)
            sx, sy, sz = source(dx, dy, k)
            left, right = [], []
            for score in range(2):
                spot = pl.multiple_of((score * 4 + sz) * SLAB, SLAB)
                left.append(rows[0, sx, :, pl.ds(spot, SLAB)])
                right.append(pl.ds(pl.multiple_of(sx * HALF + spot, SLAB), SLAB))
            terms[dy].append((jnp.concatenate(left, axis=1), right))
        for dy in range(2):
            if not terms[dy]:
                continue
            half = (1 - y) if dy else y
            left = jnp.concatenate([term[0] for term in terms[dy]], axis=1)
            for start in range(0, HALF, 256):
                right = [reach[half, spot, start:start + 256] for term in terms[dy] for spot in term[1]]
                product = jnp.dot(left, jnp.concatenate(right, axis=0), preferred_element_type=jnp.float32)
                if fresh:
                    total[half, :, start:start + 256] = product
                else:
                    total[half, :, start:start + 256] += product

    def columns(sz, score):
        return pl.ds(pl.multiple_of((score * 4 + sz) * SLAB, SLAB), SLAB)

    def partial(places, start, source):
        left, right = [], []
        for k in places:
            _, _, sz = source(0, 0, k)
            for score in range(2):
                spot = columns(sz, score)
                left.append(rows[1, y, :, spot])
                first = pl.multiple_of(y * HALF + (score * 4 + sz) * SLAB, SLAB)
                right.append(reach[1 - y, pl.ds(first, SLAB), start:start + 256])
        return jnp.dot(
            jnp.concatenate(left, axis=1), jnp.concatenate(right, axis=0), preferred_element_type=jnp.float32
        )

    counts = []

    def gather(end_case):
        places = (0, 1, 2, 3) if end_case else (1, 0, 2, 3)

        def source(dx, dy, k):
            sx = (1 - x) if dx else x
            sy = (1 - y) if dy else y
            if k == 0:
                return sx, sy, z
            place = places[k]
            return sx, sy, jnp.where(upper, 3 - place, place)

        sent = [0] * len(PIECES)

        def push(p, dx, dy, k):
            sx, sy, sz = source(dx, dy, k)
            for hop in forwards(PIECES[p][0], dx, dy, k, end_case):
                sent[p] += 1
                copy(p, sx, sy, sz, core, peers[hop], send_sem.at[p], recv_sem.at[p, sx, sy, sz]).start()
            copy(p, sx, sy, sz, core, mate, pass_sem.at[p], got_sem.at[p, sx, sy, sz]).start()

        def second_product():
            for start in range(0, HALF, 256):
                grown = total[y, :, start:start + 256] + rows[0, y, :, start:start + 256].astype(jnp.float32)
                rows[1, y, :, start:start + 256] = jnp.minimum(grown, 1.0).astype(jnp.bfloat16)
            known = pl.ds(pl.multiple_of(y * HALF, HALF), HALF)
            for start in range(0, HALF, 256):
                more[y, :, start:start + 256] = jnp.dot(
                    rows[1, y], reach[y, known, start:start + 256], preferred_element_type=jnp.float32
                )

            @pl.when(x == y)
            def _():
                for start in range(0, HALF, 256):
                    more[1 - y, :, start:start + 256] = jnp.dot(
                        rows[1, y], reach[1 - y, known, start:start + 256], preferred_element_type=jnp.float32
                    )

            @pl.when(x != y)
            def _():
                for start in range(0, HALF, 256):
                    more[1 - y, :, start:start + 256] = partial((0,), start, source)

        def first_push(inwards):
            for p in range(len(PIECES)):
                for hop in forwards(PIECES[p][0], 0, 0, 0, end_case):
                    @pl.when(is_inwards[hop] if inwards else jnp.logical_not(is_inwards[hop]))
                    def _():
                        copy(p, x, y, z, core, peers[hop], send_sem.at[p], recv_sem.at[p, x, y, z]).start()

        first_push(True)
        for p in range(len(PIECES)):
            sent[p] += len(forwards(PIECES[p][0], 0, 0, 0, end_case))
            copy(p, x, y, z, core, mate, pass_sem.at[p], got_sem.at[p, x, y, z]).start()

        @pl.when(further > 0)
        def _():
            pl.semaphore_wait(ready, further)

        first_push(False)
        rows[0, y] = reach[y, pl.ds(own_row, SLAB), :]
        groups = dict(END_GROUPS if end_case else MID_GROUPS)
        fresh = True
        for place, code in enumerate(END_ORDER if end_case else MID_ORDER):
            p, dx, dy, k = code // 16, code // 8 % 2, code // 4 % 2, code % 4
            sx, sy, sz = source(dx, dy, k)
            copy(p, sx, sy, sz, core, mate, send_sem.at[p], recv_sem.at[p, sx, sy, sz]).wait_recv()
            push(p, dx, dy, k)
            if place in groups:
                if fresh:
                    rows[0, 1 - y] = reach[1 - y, pl.ds(own_row, SLAB), :]
                await_mate(groups[place], source)
                first_product(groups[place], fresh, source)
                fresh = False
            if place == (END_SECOND if end_case else MID_SECOND):
                second_product()

        counts.append(sent)

    @pl.when(end)
    def _():
        gather(True)

    @pl.when(jnp.logical_not(end))
    def _():
        gather(False)

    def last_source(dx, dy, k):
        place = jnp.where(end, 1, 0) if isinstance(k, int) else k
        return (1 - x) if dx else x, (1 - y) if dy else y, jnp.where(upper, 3 - place, place)

    def more_of(places):
        @pl.when(x != y)
        def _():
            for start in range(0, HALF, 256):
                more[1 - y, :, start:start + 256] += partial(places, start, last_source)

    early, late = jnp.where(end, 3, 2), jnp.where(end, 2, 3)
    await_mate([(1, 1, early)], last_source)
    first_product([(1, 1, early)], False, last_source)
    more_of((1, early))
    await_mate([(1, 1, late)], last_source)
    more_of((late,))
    first_product([(1, 1, late)], False, last_source)
    for start in range(0, HALF, 256):
        grown = total[1 - y, :, start:start + 256] + rows[0, 1 - y, :, start:start + 256].astype(jnp.float32)
        rows[1, 1 - y, :, start:start + 256] = jnp.minimum(grown, 1.0).astype(jnp.bfloat16)

    known = pl.ds(pl.multiple_of((1 - y) * HALF, HALF), HALF)
    for half in range(2):
        for start in range(0, HALF, 256):
            product = jnp.dot(
                rows[1, 1 - y], reach[half, known, start:start + 256], preferred_element_type=jnp.float32
            )
            grown = product + more[half, :, start:start + 256] + rows[1, half, :, start:start + 256].astype(jnp.float32)
            rows[0, half, :, start:start + 256] = jnp.minimum(grown, 1.0).astype(jnp.bfloat16)

    def block(now, half, start, width=256):
        known = jnp.concatenate([rows[now, 0], rows[now, 1]], axis=1)
        product = jnp.dot(known, reach[half, :, start:start + width], preferred_element_type=jnp.float32)
        old = rows[now, half, :, start:start + width].astype(jnp.float32)
        return jnp.minimum(product + old, 1.0).astype(jnp.bfloat16)

    def step(now):
        for half in range(2):
            rows[1 - now, half] = block(now, half, 0, HALF)

    for count in range(STEPS - 3):
        step(count % 2)

    for start in range(0, HALF, 1024):
        out_ref[:, start:start + 1024] = block(0, y, start, 1024)

    def drain(p, count, semaphore):
        ref = reach.at[0, pl.ds(0, count * PIECES[p][2]), :]
        pltpu.make_async_remote_copy(
            src_ref=ref, dst_ref=ref, send_sem=semaphore, recv_sem=semaphore, device_id=mate, device_id_type=MESH
        ).wait_send()

    def drain_all(sent):
        for p in range(len(PIECES)):
            drain(p, sent[p], send_sem.at[p])
            drain(p, 16, pass_sem.at[p])

    @pl.when(end)
    def _():
        drain_all(counts[0])

    @pl.when(jnp.logical_not(end))
    def _():
        drain_all(counts[1])


def solution(mesh):
    layout = P(('row', 'depth'), 'col')
    sends = len(PIECES)

    def local(slab):
        return pl.pallas_call(
            kernel,
            out_shape=pltpu.VMEM((SLAB, HALF), jnp.bfloat16),
            in_specs=[pl.BlockSpec(memory_space=pl.ANY)],
            out_specs=pl.BlockSpec(memory_space=pltpu.VMEM),
            scratch_shapes=[
                pltpu.VMEM((2, N, HALF), jnp.bfloat16),
                pltpu.VMEM((2, 2, SLAB, HALF), jnp.bfloat16),
                pltpu.VMEM((2, SLAB, HALF), jnp.float32),
                pltpu.VMEM((2, SLAB, HALF), jnp.float32),
                pltpu.SemaphoreType.DMA,
                pltpu.SemaphoreType.DMA((sends,)),
                pltpu.SemaphoreType.DMA((sends, 2, 2, 4)),
                pltpu.SemaphoreType.DMA((sends,)),
                pltpu.SemaphoreType.DMA((sends, 2, 2, 4)),
                pltpu.SemaphoreType.REGULAR,
            ],
            compiler_params=pltpu.CompilerParams(collective_id=0, has_side_effects=True),
        )(slab)

    return jax.shard_map(local, mesh=mesh, in_specs=(layout,), out_specs=layout, check_vma=False)
```

```python
import jax
import jax.numpy as jnp
from jax import lax
from jax.experimental import pallas as pl
from jax.experimental.pallas import tpu as pltpu
from jax.sharding import PartitionSpec as P

N = 2048
SLAB = 128
HALF = 1024
STEPS = 15
MESH = pl.DeviceIdType.MESH

PIECES = (('zxy', 0, 48), ('zyx', 48, 48), ('yxz', 96, 32))
END_ORDER = (
    8, 4, 1, 24, 20, 17, 40, 36, 33, 9, 2, 12, 5, 18, 28, 25, 21, 41, 37, 34, 44, 13, 6, 10, 3, 26, 22, 19, 29, 35,
    14, 38, 42, 11, 7, 30, 23, 43, 39, 27, 45, 15, 47, 31, 46,
)
MID_ORDER = (
    1, 8, 4, 2, 17, 24, 20, 18, 33, 40, 36, 34, 3, 9, 10, 5, 41, 37, 19, 6, 12, 35, 38, 42, 25, 26, 28, 21, 22, 39,
    43, 45, 44, 7, 11, 47, 13, 14, 27, 46, 23, 29, 30, 15, 31,
)

END_GROUPS = ((10, (0, 1, 8, 4)), (24, (2, 9, 5, 12)), (36, (3, 10, 6)), (41, (11, 7)), (44, (13,)))
MID_GROUPS = ((13, (0, 1, 8, 2, 4)), (29, (3, 9)), (34, (10, 5, 6, 12)), (43, (11, 7, 13)))
END_SECOND = 41
MID_SECOND = 43


def forwards(order, dx, dy, k, end):
    far = {'x': dx == 1, 'y': dy == 1, 'z': k != 0}
    last = max([i for i, axis in enumerate(order) if far[axis]], default=-1)
    hops = []
    for i, axis in enumerate(order):
        if axis == 'z' and i > last:
            hops += ['in'] if end else ['in', 'out']
        elif axis == 'z' and i == last and not end:
            hops += ['in'] if k == 1 else ['out']
        elif i > last:
            hops.append(axis)
    return hops


def kernel(in_ref, out_ref, reach, rows, total, more, in_sem, send_sem, recv_sem, pass_sem, got_sem, ready):
    z, y, row = lax.axis_index('depth'), lax.axis_index('col'), lax.axis_index('row')
    x, core = row // 2, row % 2
    upper = z >= 2
    z_in = jnp.where(upper, z - 1, z + 1)
    z_out = jnp.where(upper, z + 1, z - 1)
    end = (z == 0) | (z == 3)
    x_row = (1 - x) * 2 + core
    mate_row = x * 2 + 1 - core
    peers = {
        'x': {'depth': z, 'col': y, 'row': x_row},
        'y': {'depth': z, 'col': 1 - y, 'row': row},
        'in': {'depth': z_in, 'col': y, 'row': row},
        'out': {'depth': z_out, 'col': y, 'row': row},
    }
    mate = {'depth': z, 'col': y, 'row': mate_row}

    def slab_at(sx, sy, sz, score):
        return sy, (sx * 2 + score) * 4 + sz

    own_half, own_block = slab_at(x, y, z, core)
    own_row = pl.multiple_of(own_block * SLAB, SLAB)
    load = pltpu.make_async_copy(in_ref, reach.at[own_half, pl.ds(own_row, SLAB), :], in_sem)
    load.start()

    steps = (
        (x == 0, x == 1, peers['x']),
        (y == 0, y == 1, peers['y']),
        (z < 3, None, {'depth': z + 1, 'col': y, 'row': row}),
        (None, z > 0, {'depth': z - 1, 'col': y, 'row': row}),
    )
    barrier = pltpu.get_barrier_semaphore()
    pl.semaphore_signal(barrier, inc=1, device_id=mate, device_id_type=MESH)
    for outwards, _, peer in steps:
        if outwards is not None:
            @pl.when(outwards)
            def _():
                pl.semaphore_signal(barrier, inc=1, device_id=peer, device_id_type=MESH)

    pl.semaphore_wait(barrier, 1 + x + y + jnp.where(z > 0, 1, 0))
    for _, inwards, peer in steps:
        if inwards is not None:
            @pl.when(inwards)
            def _():
                pl.semaphore_signal(ready, inc=1, device_id=peer, device_id_type=MESH)

    is_inwards = {'x': x == 1, 'y': y == 1, 'in': upper, 'out': jnp.logical_not(upper)}
    further = (1 - x) + (1 - y) + jnp.where(z < 3, 1, 0)

    load.wait()

    def piece_ref(p, sx, sy, sz, score):
        half, block = slab_at(sx, sy, sz, score)
        start = pl.multiple_of(block * SLAB + PIECES[p][1], 16)
        return reach.at[half, pl.ds(start, PIECES[p][2]), :]

    def copy(p, sx, sy, sz, score, peer, send, recv):
        ref = piece_ref(p, sx, sy, sz, score)
        return pltpu.make_async_remote_copy(
            src_ref=ref, dst_ref=ref, send_sem=send, recv_sem=recv, device_id=peer, device_id_type=MESH
        )

    def parts(unit):
        return unit if isinstance(unit, tuple) else (unit // 8, unit // 4 % 2, unit % 4)

    def await_mate(units, source):
        for unit in units:
            sx, sy, sz = source(*parts(unit))
            for p in range(len(PIECES)):
                copy(p, sx, sy, sz, 1 - core, mate, pass_sem.at[p], got_sem.at[p, sx, sy, sz]).wait_recv()

    def first_product(units, fresh, source):
        terms = {0: [], 1: []}
        for unit in units:
            dx, dy, k = parts(unit)
            sx, sy, sz = source(dx, dy, k)
            left, right = [], []
            for score in range(2):
                spot = pl.multiple_of((score * 4 + sz) * SLAB, SLAB)
                left.append(rows[0, sx, :, pl.ds(spot, SLAB)])
                right.append(pl.ds(pl.multiple_of(sx * HALF + spot, SLAB), SLAB))
            terms[dy].append((jnp.concatenate(left, axis=1), right))
        for dy in range(2):
            if not terms[dy]:
                continue
            half = (1 - y) if dy else y
            left = jnp.concatenate([term[0] for term in terms[dy]], axis=1)
            for start in range(0, HALF, 256):
                right = [reach[half, spot, start:start + 256] for term in terms[dy] for spot in term[1]]
                product = jnp.dot(left, jnp.concatenate(right, axis=0), preferred_element_type=jnp.float32)
                if fresh:
                    total[half, :, start:start + 256] = product
                else:
                    total[half, :, start:start + 256] += product

    def columns(sz, score):
        return pl.ds(pl.multiple_of((score * 4 + sz) * SLAB, SLAB), SLAB)

    def partial(places, start, source):
        left, right = [], []
        for k in places:
            _, _, sz = source(0, 0, k)
            for score in range(2):
                spot = columns(sz, score)
                left.append(rows[1, y, :, spot])
                first = pl.multiple_of(y * HALF + (score * 4 + sz) * SLAB, SLAB)
                right.append(reach[1 - y, pl.ds(first, SLAB), start:start + 256])
        return jnp.dot(
            jnp.concatenate(left, axis=1), jnp.concatenate(right, axis=0), preferred_element_type=jnp.float32
        )

    flipped = (x == 0) & (y == 1)
    counts = []

    def gather(end_case):
        places = (0, 1, 2, 3) if end_case else (1, 0, 2, 3)

        def source(dx, dy, k):
            sx = (1 - x) if dx else x
            sy = (1 - y) if dy else y
            if k == 0:
                return sx, sy, z
            place = places[k]
            return sx, sy, jnp.where(upper, 3 - place, place)

        sent = [0] * len(PIECES)

        def push(p, dx, dy, k):
            sx, sy, sz = source(dx, dy, k)
            for hop in forwards(PIECES[p][0], dx, dy, k, end_case):
                sent[p] += 1
                copy(p, sx, sy, sz, core, peers[hop], send_sem.at[p], recv_sem.at[p, sx, sy, sz]).start()
            copy(p, sx, sy, sz, core, mate, pass_sem.at[p], got_sem.at[p, sx, sy, sz]).start()

        def second_product():
            for start in range(0, HALF, 256):
                grown = total[y, :, start:start + 256] + rows[0, y, :, start:start + 256].astype(jnp.float32)
                rows[1, y, :, start:start + 256] = jnp.minimum(grown, 1.0).astype(jnp.bfloat16)
            known = pl.ds(pl.multiple_of(y * HALF, HALF), HALF)
            for start in range(0, HALF, 256):
                more[y, :, start:start + 256] = jnp.dot(
                    rows[1, y], reach[y, known, start:start + 256], preferred_element_type=jnp.float32
                )

            @pl.when(x == y)
            def _():
                for start in range(0, HALF, 256):
                    more[1 - y, :, start:start + 256] = jnp.dot(
                        rows[1, y], reach[1 - y, known, start:start + 256], preferred_element_type=jnp.float32
                    )

            @pl.when(x != y)
            def _():
                for start in range(0, HALF, 256):
                    more[1 - y, :, start:start + 256] = partial((0,), start, source)

        def first_push(inwards):
            for p in range(len(PIECES)):
                for hop in forwards(PIECES[p][0], 0, 0, 0, end_case):
                    @pl.when(is_inwards[hop] if inwards else jnp.logical_not(is_inwards[hop]))
                    def _():
                        copy(p, x, y, z, core, peers[hop], send_sem.at[p], recv_sem.at[p, x, y, z]).start()

        first_push(True)
        for p in range(len(PIECES)):
            sent[p] += len(forwards(PIECES[p][0], 0, 0, 0, end_case))
            copy(p, x, y, z, core, mate, pass_sem.at[p], got_sem.at[p, x, y, z]).start()

        @pl.when(further > 0)
        def _():
            pl.semaphore_wait(ready, further)

        first_push(False)
        rows[0, y] = reach[y, pl.ds(own_row, SLAB), :]
        def take(code):
            p, dx, dy, k = code // 16, code // 8 % 2, code // 4 % 2, code % 4
            sx, sy, sz = source(dx, dy, k)
            copy(p, sx, sy, sz, core, mate, send_sem.at[p], recv_sem.at[p, sx, sy, sz]).wait_recv()
            push(p, dx, dy, k)

        groups = dict(END_GROUPS if end_case else MID_GROUPS)
        fresh = True
        for place, code in enumerate(END_ORDER if end_case else MID_ORDER):
            if end_case and place == 43:
                @pl.when(flipped)
                def _():
                    take(END_ORDER[44])
                    take(END_ORDER[43])

                @pl.when(jnp.logical_not(flipped))
                def _():
                    take(END_ORDER[43])
                    take(END_ORDER[44])
            elif not (end_case and place == 44):
                take(code)
            if place in groups:
                if fresh:
                    rows[0, 1 - y] = reach[1 - y, pl.ds(own_row, SLAB), :]
                await_mate(groups[place], source)
                first_product(groups[place], fresh, source)
                fresh = False
            if place == (END_SECOND if end_case else MID_SECOND):
                second_product()

        counts.append(sent)

    @pl.when(end)
    def _():
        gather(True)

    @pl.when(jnp.logical_not(end))
    def _():
        gather(False)

    def last_source(dx, dy, k):
        place = jnp.where(end, 1, 0) if isinstance(k, int) else k
        return (1 - x) if dx else x, (1 - y) if dy else y, jnp.where(upper, 3 - place, place)

    def more_of(places):
        @pl.when(x != y)
        def _():
            for start in range(0, HALF, 256):
                more[1 - y, :, start:start + 256] += partial(places, start, last_source)

    last_is_second = end & jnp.logical_not(flipped)
    early, late = jnp.where(last_is_second, 3, 2), jnp.where(last_is_second, 2, 3)
    await_mate([(1, 1, early)], last_source)
    first_product([(1, 1, early)], False, last_source)
    more_of((1, early))
    await_mate([(1, 1, late)], last_source)
    more_of((late,))
    first_product([(1, 1, late)], False, last_source)
    for start in range(0, HALF, 256):
        grown = total[1 - y, :, start:start + 256] + rows[0, 1 - y, :, start:start + 256].astype(jnp.float32)
        rows[1, 1 - y, :, start:start + 256] = jnp.minimum(grown, 1.0).astype(jnp.bfloat16)

    known = pl.ds(pl.multiple_of((1 - y) * HALF, HALF), HALF)
    for half in range(2):
        for start in range(0, HALF, 256):
            product = jnp.dot(
                rows[1, 1 - y], reach[half, known, start:start + 256], preferred_element_type=jnp.float32
            )
            grown = product + more[half, :, start:start + 256] + rows[1, half, :, start:start + 256].astype(jnp.float32)
            rows[0, half, :, start:start + 256] = jnp.minimum(grown, 1.0).astype(jnp.bfloat16)

    def block(now, half, start, width=256):
        known = jnp.concatenate([rows[now, 0], rows[now, 1]], axis=1)
        product = jnp.dot(known, reach[half, :, start:start + width], preferred_element_type=jnp.float32)
        old = rows[now, half, :, start:start + width].astype(jnp.float32)
        return jnp.minimum(product + old, 1.0).astype(jnp.bfloat16)

    def step(now):
        for half in range(2):
            rows[1 - now, half] = block(now, half, 0, HALF)

    for count in range(STEPS - 3):
        step(count % 2)

    for start in range(0, HALF, 1024):
        out_ref[:, start:start + 1024] = block(0, y, start, 1024)

    def drain(p, count, semaphore):
        ref = reach.at[0, pl.ds(0, count * PIECES[p][2]), :]
        pltpu.make_async_remote_copy(
            src_ref=ref, dst_ref=ref, send_sem=semaphore, recv_sem=semaphore, device_id=mate, device_id_type=MESH
        ).wait_send()

    def drain_all(sent):
        for p in range(len(PIECES)):
            drain(p, sent[p], send_sem.at[p])
            drain(p, 16, pass_sem.at[p])

    @pl.when(end)
    def _():
        drain_all(counts[0])

    @pl.when(jnp.logical_not(end))
    def _():
        drain_all(counts[1])


def solution(mesh):
    layout = P(('row', 'depth'), 'col')
    sends = len(PIECES)

    def local(slab):
        return pl.pallas_call(
            kernel,
            out_shape=pltpu.VMEM((SLAB, HALF), jnp.bfloat16),
            in_specs=[pl.BlockSpec(memory_space=pl.ANY)],
            out_specs=pl.BlockSpec(memory_space=pltpu.VMEM),
            scratch_shapes=[
                pltpu.VMEM((2, N, HALF), jnp.bfloat16),
                pltpu.VMEM((2, 2, SLAB, HALF), jnp.bfloat16),
                pltpu.VMEM((2, SLAB, HALF), jnp.float32),
                pltpu.VMEM((2, SLAB, HALF), jnp.float32),
                pltpu.SemaphoreType.DMA,
                pltpu.SemaphoreType.DMA((sends,)),
                pltpu.SemaphoreType.DMA((sends, 2, 2, 4)),
                pltpu.SemaphoreType.DMA((sends,)),
                pltpu.SemaphoreType.DMA((sends, 2, 2, 4)),
                pltpu.SemaphoreType.REGULAR,
            ],
            compiler_params=pltpu.CompilerParams(collective_id=0, has_side_effects=True),
        )(slab)

    return jax.shard_map(local, mesh=mesh, in_specs=(layout,), out_specs=layout, check_vma=False)
```

```python
import jax
import jax.numpy as jnp
from jax import lax
from jax.experimental import pallas as pl
from jax.experimental.pallas import tpu as pltpu
from jax.sharding import PartitionSpec as P

N = 2048
SLAB = 128
HALF = 1024
STEPS = 15
MESH = pl.DeviceIdType.MESH

PIECES = (('zxy', 0, 48), ('zyx', 48, 48), ('yxz', 96, 32))
END_ORDER = (
    8, 4, 1, 24, 20, 17, 40, 36, 33, 9, 2, 12, 5, 18, 28, 25, 21, 41, 37, 34, 44, 13, 6, 10, 3, 26, 22, 19, 29, 35,
    14, 38, 42, 11, 7, 30, 23, 43, 39, 27, 45, 15, 47, 31, 46,
)
MID_ORDER = (
    1, 8, 4, 2, 17, 24, 20, 18, 33, 40, 36, 34, 3, 9, 10, 5, 41, 37, 19, 6, 12, 35, 38, 42, 25, 26, 28, 21, 22, 39,
    43, 45, 44, 7, 11, 47, 13, 14, 27, 46, 23, 29, 30, 15, 31,
)

END_GROUPS = ((10, (0, 1, 8, 4)), (24, (2, 9, 5, 12)), (36, (3, 10, 6)), (41, (11, 7)), (44, (13,)))
MID_GROUPS = ((13, (0, 1, 8, 2, 4)), (29, (3, 9)), (34, (10, 5, 6, 12)), (43, (11, 7, 13)))
END_SECOND = 41
MID_SECOND = 43


def forwards(order, dx, dy, k, end):
    far = {'x': dx == 1, 'y': dy == 1, 'z': k != 0}
    last = max([i for i, axis in enumerate(order) if far[axis]], default=-1)
    hops = []
    for i, axis in enumerate(order):
        if axis == 'z' and i > last:
            hops += ['in'] if end else ['in', 'out']
        elif axis == 'z' and i == last and not end:
            hops += ['in'] if k == 1 else ['out']
        elif i > last:
            hops.append(axis)
    return hops


def kernel(in_ref, out_ref, reach, rows, total, more, in_sem, send_sem, recv_sem, pass_sem, got_sem, ready):
    z, y, row = lax.axis_index('depth'), lax.axis_index('col'), lax.axis_index('row')
    x, core = row // 2, row % 2
    upper = z >= 2
    z_in = jnp.where(upper, z - 1, z + 1)
    z_out = jnp.where(upper, z + 1, z - 1)
    end = (z == 0) | (z == 3)
    x_row = (1 - x) * 2 + core
    mate_row = x * 2 + 1 - core
    peers = {
        'x': {'depth': z, 'col': y, 'row': x_row},
        'y': {'depth': z, 'col': 1 - y, 'row': row},
        'in': {'depth': z_in, 'col': y, 'row': row},
        'out': {'depth': z_out, 'col': y, 'row': row},
    }
    mate = {'depth': z, 'col': y, 'row': mate_row}

    def slab_at(sx, sy, sz, score):
        return sy, (sx * 2 + score) * 4 + sz

    own_half, own_block = slab_at(x, y, z, core)
    own_row = pl.multiple_of(own_block * SLAB, SLAB)
    load = pltpu.make_async_copy(in_ref, reach.at[own_half, pl.ds(own_row, SLAB), :], in_sem)
    load.start()

    steps = (
        (x == 0, x == 1, peers['x']),
        (y == 0, y == 1, peers['y']),
        (z < 3, None, {'depth': z + 1, 'col': y, 'row': row}),
        (None, z > 0, {'depth': z - 1, 'col': y, 'row': row}),
    )
    barrier = pltpu.get_barrier_semaphore()
    pl.semaphore_signal(barrier, inc=1, device_id=mate, device_id_type=MESH)
    for outwards, _, peer in steps:
        if outwards is not None:
            @pl.when(outwards)
            def _():
                pl.semaphore_signal(barrier, inc=1, device_id=peer, device_id_type=MESH)

    pl.semaphore_wait(barrier, 1 + x + y + jnp.where(z > 0, 1, 0))
    for _, inwards, peer in steps:
        if inwards is not None:
            @pl.when(inwards)
            def _():
                pl.semaphore_signal(ready, inc=1, device_id=peer, device_id_type=MESH)

    is_inwards = {'x': x == 1, 'y': y == 1, 'in': upper, 'out': jnp.logical_not(upper)}
    further = (1 - x) + (1 - y) + jnp.where(z < 3, 1, 0)

    load.wait()

    def piece_ref(p, sx, sy, sz, score):
        half, block = slab_at(sx, sy, sz, score)
        start = pl.multiple_of(block * SLAB + PIECES[p][1], 16)
        return reach.at[half, pl.ds(start, PIECES[p][2]), :]

    def copy(p, sx, sy, sz, score, peer, send, recv):
        ref = piece_ref(p, sx, sy, sz, score)
        return pltpu.make_async_remote_copy(
            src_ref=ref, dst_ref=ref, send_sem=send, recv_sem=recv, device_id=peer, device_id_type=MESH
        )

    def parts(unit):
        return unit if isinstance(unit, tuple) else (unit // 8, unit // 4 % 2, unit % 4)

    def await_mate(units, source):
        for unit in units:
            sx, sy, sz = source(*parts(unit))
            for p in range(len(PIECES)):
                copy(p, sx, sy, sz, 1 - core, mate, pass_sem.at[p], got_sem.at[p, sx, sy, sz]).wait_recv()

    def first_product(units, fresh, source):
        terms = {0: [], 1: []}
        for unit in units:
            dx, dy, k = parts(unit)
            sx, sy, sz = source(dx, dy, k)
            left, right = [], []
            for score in range(2):
                spot = pl.multiple_of((score * 4 + sz) * SLAB, SLAB)
                left.append(rows[0, sx, :, pl.ds(spot, SLAB)])
                right.append(pl.ds(pl.multiple_of(sx * HALF + spot, SLAB), SLAB))
            terms[dy].append((jnp.concatenate(left, axis=1), right))
        for dy in range(2):
            if not terms[dy]:
                continue
            half = (1 - y) if dy else y
            left = jnp.concatenate([term[0] for term in terms[dy]], axis=1)
            for start in range(0, HALF, 256):
                right = [reach[half, spot, start:start + 256] for term in terms[dy] for spot in term[1]]
                product = jnp.dot(left, jnp.concatenate(right, axis=0), preferred_element_type=jnp.float32)
                if fresh:
                    total[half, :, start:start + 256] = product
                else:
                    total[half, :, start:start + 256] += product

    def columns(sz, score):
        return pl.ds(pl.multiple_of((score * 4 + sz) * SLAB, SLAB), SLAB)

    def partial(places, start, source):
        left, right = [], []
        for k in places:
            _, _, sz = source(0, 0, k)
            for score in range(2):
                spot = columns(sz, score)
                left.append(rows[1, y, :, spot])
                first = pl.multiple_of(y * HALF + (score * 4 + sz) * SLAB, SLAB)
                right.append(reach[1 - y, pl.ds(first, SLAB), start:start + 256])
        return jnp.dot(
            jnp.concatenate(left, axis=1), jnp.concatenate(right, axis=0), preferred_element_type=jnp.float32
        )

    flipped = (x == 0) & (y == 1)
    counts = []

    def gather(end_case):
        places = (0, 1, 2, 3) if end_case else (1, 0, 2, 3)

        def source(dx, dy, k):
            sx = (1 - x) if dx else x
            sy = (1 - y) if dy else y
            if k == 0:
                return sx, sy, z
            place = places[k]
            return sx, sy, jnp.where(upper, 3 - place, place)

        sent = [0] * len(PIECES)

        def push(p, dx, dy, k):
            sx, sy, sz = source(dx, dy, k)
            for hop in forwards(PIECES[p][0], dx, dy, k, end_case):
                sent[p] += 1
                copy(p, sx, sy, sz, core, peers[hop], send_sem.at[p], recv_sem.at[p, sx, sy, sz]).start()
            copy(p, sx, sy, sz, core, mate, pass_sem.at[p], got_sem.at[p, sx, sy, sz]).start()

        def second_product():
            for start in range(0, HALF, 256):
                grown = total[y, :, start:start + 256] + rows[0, y, :, start:start + 256].astype(jnp.float32)
                rows[1, y, :, start:start + 256] = jnp.minimum(grown, 1.0).astype(jnp.bfloat16)
            known = pl.ds(pl.multiple_of(y * HALF, HALF), HALF)
            for start in range(0, HALF, 256):
                more[y, :, start:start + 256] = jnp.dot(
                    rows[1, y], reach[y, known, start:start + 256], preferred_element_type=jnp.float32
                )

            @pl.when(x == y)
            def _():
                for start in range(0, HALF, 256):
                    more[1 - y, :, start:start + 256] = jnp.dot(
                        rows[1, y], reach[1 - y, known, start:start + 256], preferred_element_type=jnp.float32
                    )

            @pl.when(x != y)
            def _():
                for start in range(0, HALF, 256):
                    more[1 - y, :, start:start + 256] = partial((0,), start, source)

        def first_push(inwards):
            for p in range(len(PIECES)):
                for hop in forwards(PIECES[p][0], 0, 0, 0, end_case):
                    @pl.when(is_inwards[hop] if inwards else jnp.logical_not(is_inwards[hop]))
                    def _():
                        copy(p, x, y, z, core, peers[hop], send_sem.at[p], recv_sem.at[p, x, y, z]).start()

        first_push(True)
        for p in range(len(PIECES)):
            sent[p] += len(forwards(PIECES[p][0], 0, 0, 0, end_case))
            copy(p, x, y, z, core, mate, pass_sem.at[p], got_sem.at[p, x, y, z]).start()

        @pl.when(further > 0)
        def _():
            pl.semaphore_wait(ready, further)

        first_push(False)
        rows[0, y] = reach[y, pl.ds(own_row, SLAB), :]
        def take(code):
            p, dx, dy, k = code // 16, code // 8 % 2, code // 4 % 2, code % 4
            sx, sy, sz = source(dx, dy, k)
            copy(p, sx, sy, sz, core, mate, send_sem.at[p], recv_sem.at[p, sx, sy, sz]).wait_recv()
            push(p, dx, dy, k)

        groups = dict(END_GROUPS if end_case else MID_GROUPS)
        fresh = True
        for place, code in enumerate(END_ORDER if end_case else MID_ORDER):
            if end_case and place == 43:
                @pl.when(flipped)
                def _():
                    take(END_ORDER[44])
                    take(END_ORDER[43])

                @pl.when(jnp.logical_not(flipped))
                def _():
                    take(END_ORDER[43])
                    take(END_ORDER[44])
            elif not (end_case and place == 44):
                take(code)
            if place in groups:
                if fresh:
                    rows[0, 1 - y] = reach[1 - y, pl.ds(own_row, SLAB), :]
                await_mate(groups[place], source)
                first_product(groups[place], fresh, source)
                fresh = False
            if place == (END_SECOND if end_case else MID_SECOND):
                second_product()

        counts.append(sent)

    @pl.when(end)
    def _():
        gather(True)

    @pl.when(jnp.logical_not(end))
    def _():
        gather(False)

    def last_source(dx, dy, k):
        place = jnp.where(end, 1, 0) if isinstance(k, int) else k
        return (1 - x) if dx else x, (1 - y) if dy else y, jnp.where(upper, 3 - place, place)

    def more_of(places):
        @pl.when(x != y)
        def _():
            for start in range(0, HALF, 256):
                more[1 - y, :, start:start + 256] += partial(places, start, last_source)

    last_is_second = end & jnp.logical_not(flipped)
    early, late = jnp.where(last_is_second, 3, 2), jnp.where(last_is_second, 2, 3)
    await_mate([(1, 1, early)], last_source)
    first_product([(1, 1, early)], False, last_source)
    more_of((1, early))
    await_mate([(1, 1, late)], last_source)
    more_of((late,))
    first_product([(1, 1, late)], False, last_source)
    for start in range(0, HALF, 256):
        grown = total[1 - y, :, start:start + 256] + rows[0, 1 - y, :, start:start + 256].astype(jnp.float32)
        rows[1, 1 - y, :, start:start + 256] = jnp.minimum(grown, 1.0).astype(jnp.bfloat16)

    known = pl.ds(pl.multiple_of((1 - y) * HALF, HALF), HALF)
    for half in range(2):
        for start in range(0, HALF, 256):
            product = jnp.dot(
                rows[1, 1 - y], reach[half, known, start:start + 256], preferred_element_type=jnp.float32
            )
            grown = product + more[half, :, start:start + 256] + rows[1, half, :, start:start + 256].astype(jnp.float32)
            rows[0, half, :, start:start + 256] = jnp.minimum(grown, 1.0).astype(jnp.bfloat16)

    def block(now, half, start, width=256):
        known = jnp.concatenate([rows[now, 0], rows[now, 1]], axis=1)
        product = jnp.dot(known, reach[half, :, start:start + width], preferred_element_type=jnp.float32)
        old = rows[now, half, :, start:start + width].astype(jnp.float32)
        return jnp.minimum(product + old, 1.0).astype(jnp.bfloat16)

    def step(now):
        for half in range(2):
            for start in range(0, HALF, 512):
                rows[1 - now, half, :, start:start + 512] = block(now, half, start, 512)

    for count in range(STEPS - 3):
        step(count % 2)

    for start in range(0, HALF, 1024):
        out_ref[:, start:start + 1024] = block(0, y, start, 1024)

    def drain(p, count, semaphore):
        ref = reach.at[0, pl.ds(0, count * PIECES[p][2]), :]
        pltpu.make_async_remote_copy(
            src_ref=ref, dst_ref=ref, send_sem=semaphore, recv_sem=semaphore, device_id=mate, device_id_type=MESH
        ).wait_send()

    def drain_all(sent):
        for p in range(len(PIECES)):
            drain(p, sent[p], send_sem.at[p])
            drain(p, 16, pass_sem.at[p])

    @pl.when(end)
    def _():
        drain_all(counts[0])

    @pl.when(jnp.logical_not(end))
    def _():
        drain_all(counts[1])


def solution(mesh):
    layout = P(('row', 'depth'), 'col')
    sends = len(PIECES)

    def local(slab):
        return pl.pallas_call(
            kernel,
            out_shape=pltpu.VMEM((SLAB, HALF), jnp.bfloat16),
            in_specs=[pl.BlockSpec(memory_space=pl.ANY)],
            out_specs=pl.BlockSpec(memory_space=pltpu.VMEM),
            scratch_shapes=[
                pltpu.VMEM((2, N, HALF), jnp.bfloat16),
                pltpu.VMEM((2, 2, SLAB, HALF), jnp.bfloat16),
                pltpu.VMEM((2, SLAB, HALF), jnp.float32),
                pltpu.VMEM((2, SLAB, HALF), jnp.float32),
                pltpu.SemaphoreType.DMA,
                pltpu.SemaphoreType.DMA((sends,)),
                pltpu.SemaphoreType.DMA((sends, 2, 2, 4)),
                pltpu.SemaphoreType.DMA((sends,)),
                pltpu.SemaphoreType.DMA((sends, 2, 2, 4)),
                pltpu.SemaphoreType.REGULAR,
            ],
            compiler_params=pltpu.CompilerParams(collective_id=0, has_side_effects=True),
        )(slab)

    return jax.shard_map(local, mesh=mesh, in_specs=(layout,), out_specs=layout, check_vma=False)
```

```python
import jax
import jax.numpy as jnp
from jax import lax
from jax.experimental import pallas as pl
from jax.experimental.pallas import tpu as pltpu
from jax.sharding import PartitionSpec as P

N = 2048
SLAB = 128
HALF = 1024
STEPS = 15
MESH = pl.DeviceIdType.MESH

PIECES = (('zxy', 0, 48), ('zyx', 48, 48), ('yxz', 96, 32))
END_ORDER = (
    8, 4, 1, 24, 20, 17, 40, 36, 33, 9, 2, 12, 5, 18, 28, 25, 21, 41, 37, 34, 44, 13, 6, 10, 3, 26, 22, 19, 29, 35,
    14, 38, 42, 11, 7, 30, 23, 43, 39, 27, 45, 15, 47, 31, 46,
)
MID_ORDER = (
    1, 8, 4, 2, 17, 24, 20, 18, 33, 40, 36, 34, 3, 9, 10, 5, 41, 37, 19, 6, 12, 35, 38, 42, 25, 26, 28, 21, 22, 39,
    43, 45, 44, 7, 11, 47, 13, 14, 27, 46, 23, 29, 30, 15, 31,
)

END_GROUPS = ((14, (0, 1, 8, 4)), (24, (2, 9, 5, 12)), (36, (3, 10, 6)), (41, (11, 7)), (44, (13,)))
MID_GROUPS = ((17, (0, 1, 8, 2, 4)), (29, (3, 9)), (34, (10, 5, 6, 12)), (43, (11, 7, 13)))
END_SECOND = 41
MID_SECOND = 43


def forwards(order, dx, dy, k, end):
    far = {'x': dx == 1, 'y': dy == 1, 'z': k != 0}
    last = max([i for i, axis in enumerate(order) if far[axis]], default=-1)
    hops = []
    for i, axis in enumerate(order):
        if axis == 'z' and i > last:
            hops += ['in'] if end else ['in', 'out']
        elif axis == 'z' and i == last and not end:
            hops += ['in'] if k == 1 else ['out']
        elif i > last:
            hops.append(axis)
    return hops


def kernel(in_ref, out_ref, reach, rows, total, more, in_sem, send_sem, recv_sem, pass_sem, got_sem, ready):
    z, y, row = lax.axis_index('depth'), lax.axis_index('col'), lax.axis_index('row')
    x, core = row // 2, row % 2
    upper = z >= 2
    z_in = jnp.where(upper, z - 1, z + 1)
    z_out = jnp.where(upper, z + 1, z - 1)
    end = (z == 0) | (z == 3)
    x_row = (1 - x) * 2 + core
    mate_row = x * 2 + 1 - core
    peers = {
        'x': {'depth': z, 'col': y, 'row': x_row},
        'y': {'depth': z, 'col': 1 - y, 'row': row},
        'in': {'depth': z_in, 'col': y, 'row': row},
        'out': {'depth': z_out, 'col': y, 'row': row},
    }
    mate = {'depth': z, 'col': y, 'row': mate_row}

    def slab_at(sx, sy, sz, score):
        return sy, (sx * 2 + score) * 4 + sz

    own_half, own_block = slab_at(x, y, z, core)
    own_row = pl.multiple_of(own_block * SLAB, SLAB)
    load = pltpu.make_async_copy(in_ref, reach.at[own_half, pl.ds(own_row, SLAB), :], in_sem)
    load.start()

    steps = (
        (x == 0, x == 1, peers['x']),
        (y == 0, y == 1, peers['y']),
        (z < 3, None, {'depth': z + 1, 'col': y, 'row': row}),
        (None, z > 0, {'depth': z - 1, 'col': y, 'row': row}),
    )
    barrier = pltpu.get_barrier_semaphore()
    pl.semaphore_signal(barrier, inc=1, device_id=mate, device_id_type=MESH)
    for outwards, _, peer in steps:
        if outwards is not None:
            @pl.when(outwards)
            def _():
                pl.semaphore_signal(barrier, inc=1, device_id=peer, device_id_type=MESH)

    pl.semaphore_wait(barrier, 1 + x + y + jnp.where(z > 0, 1, 0))
    for _, inwards, peer in steps:
        if inwards is not None:
            @pl.when(inwards)
            def _():
                pl.semaphore_signal(ready, inc=1, device_id=peer, device_id_type=MESH)

    is_inwards = {'x': x == 1, 'y': y == 1, 'in': upper, 'out': jnp.logical_not(upper)}
    further = (1 - x) + (1 - y) + jnp.where(z < 3, 1, 0)

    load.wait()

    def piece_ref(p, sx, sy, sz, score):
        half, block = slab_at(sx, sy, sz, score)
        start = pl.multiple_of(block * SLAB + PIECES[p][1], 16)
        return reach.at[half, pl.ds(start, PIECES[p][2]), :]

    def copy(p, sx, sy, sz, score, peer, send, recv):
        ref = piece_ref(p, sx, sy, sz, score)
        return pltpu.make_async_remote_copy(
            src_ref=ref, dst_ref=ref, send_sem=send, recv_sem=recv, device_id=peer, device_id_type=MESH
        )

    def parts(unit):
        return unit if isinstance(unit, tuple) else (unit // 8, unit // 4 % 2, unit % 4)

    def await_mate(units, source):
        for unit in units:
            sx, sy, sz = source(*parts(unit))
            for p in range(len(PIECES)):
                copy(p, sx, sy, sz, 1 - core, mate, pass_sem.at[p], got_sem.at[p, sx, sy, sz]).wait_recv()

    def first_product(units, fresh, source):
        terms = {0: [], 1: []}
        for unit in units:
            dx, dy, k = parts(unit)
            sx, sy, sz = source(dx, dy, k)
            left, right = [], []
            for score in range(2):
                spot = pl.multiple_of((score * 4 + sz) * SLAB, SLAB)
                left.append(rows[0, sx, :, pl.ds(spot, SLAB)])
                right.append(pl.ds(pl.multiple_of(sx * HALF + spot, SLAB), SLAB))
            terms[dy].append((jnp.concatenate(left, axis=1), right))
        for dy in range(2):
            if not terms[dy]:
                continue
            half = (1 - y) if dy else y
            left = jnp.concatenate([term[0] for term in terms[dy]], axis=1)
            for start in range(0, HALF, 256):
                right = [reach[half, spot, start:start + 256] for term in terms[dy] for spot in term[1]]
                product = jnp.dot(left, jnp.concatenate(right, axis=0), preferred_element_type=jnp.float32)
                if fresh:
                    total[half, :, start:start + 256] = product
                else:
                    total[half, :, start:start + 256] += product

    def columns(sz, score):
        return pl.ds(pl.multiple_of((score * 4 + sz) * SLAB, SLAB), SLAB)

    def partial(places, start, source):
        left, right = [], []
        for k in places:
            _, _, sz = source(0, 0, k)
            for score in range(2):
                spot = columns(sz, score)
                left.append(rows[1, y, :, spot])
                first = pl.multiple_of(y * HALF + (score * 4 + sz) * SLAB, SLAB)
                right.append(reach[1 - y, pl.ds(first, SLAB), start:start + 256])
        return jnp.dot(
            jnp.concatenate(left, axis=1), jnp.concatenate(right, axis=0), preferred_element_type=jnp.float32
        )

    flipped = (x == 0) & (y == 1)
    counts = []

    def gather(end_case):
        places = (0, 1, 2, 3) if end_case else (1, 0, 2, 3)

        def source(dx, dy, k):
            sx = (1 - x) if dx else x
            sy = (1 - y) if dy else y
            if k == 0:
                return sx, sy, z
            place = places[k]
            return sx, sy, jnp.where(upper, 3 - place, place)

        sent = [0] * len(PIECES)

        def push(p, dx, dy, k):
            sx, sy, sz = source(dx, dy, k)
            for hop in forwards(PIECES[p][0], dx, dy, k, end_case):
                sent[p] += 1
                copy(p, sx, sy, sz, core, peers[hop], send_sem.at[p], recv_sem.at[p, sx, sy, sz]).start()
            copy(p, sx, sy, sz, core, mate, pass_sem.at[p], got_sem.at[p, sx, sy, sz]).start()

        def second_product():
            for start in range(0, HALF, 256):
                grown = total[y, :, start:start + 256] + rows[0, y, :, start:start + 256].astype(jnp.float32)
                rows[1, y, :, start:start + 256] = jnp.minimum(grown, 1.0).astype(jnp.bfloat16)
            known = pl.ds(pl.multiple_of(y * HALF, HALF), HALF)
            for start in range(0, HALF, 256):
                more[y, :, start:start + 256] = jnp.dot(
                    rows[1, y], reach[y, known, start:start + 256], preferred_element_type=jnp.float32
                )

            @pl.when(x == y)
            def _():
                for start in range(0, HALF, 256):
                    more[1 - y, :, start:start + 256] = jnp.dot(
                        rows[1, y], reach[1 - y, known, start:start + 256], preferred_element_type=jnp.float32
                    )

            @pl.when(x != y)
            def _():
                for start in range(0, HALF, 256):
                    more[1 - y, :, start:start + 256] = partial((0,), start, source)

        def first_push(inwards):
            for p in range(len(PIECES)):
                for hop in forwards(PIECES[p][0], 0, 0, 0, end_case):
                    @pl.when(is_inwards[hop] if inwards else jnp.logical_not(is_inwards[hop]))
                    def _():
                        copy(p, x, y, z, core, peers[hop], send_sem.at[p], recv_sem.at[p, x, y, z]).start()

        first_push(True)
        for p in range(len(PIECES)):
            sent[p] += len(forwards(PIECES[p][0], 0, 0, 0, end_case))
            copy(p, x, y, z, core, mate, pass_sem.at[p], got_sem.at[p, x, y, z]).start()

        @pl.when(further > 0)
        def _():
            pl.semaphore_wait(ready, further)

        first_push(False)
        rows[0, y] = reach[y, pl.ds(own_row, SLAB), :]
        def take(code):
            p, dx, dy, k = code // 16, code // 8 % 2, code // 4 % 2, code % 4
            sx, sy, sz = source(dx, dy, k)
            copy(p, sx, sy, sz, core, mate, send_sem.at[p], recv_sem.at[p, sx, sy, sz]).wait_recv()
            push(p, dx, dy, k)

        groups = dict(END_GROUPS if end_case else MID_GROUPS)
        fresh = True
        for place, code in enumerate(END_ORDER if end_case else MID_ORDER):
            if end_case and place == 43:
                @pl.when(flipped)
                def _():
                    take(END_ORDER[44])
                    take(END_ORDER[43])

                @pl.when(jnp.logical_not(flipped))
                def _():
                    take(END_ORDER[43])
                    take(END_ORDER[44])
            elif not (end_case and place == 44):
                take(code)
            if place in groups:
                if fresh:
                    rows[0, 1 - y] = reach[1 - y, pl.ds(own_row, SLAB), :]
                await_mate(groups[place], source)
                first_product(groups[place], fresh, source)
                fresh = False
            if place == (END_SECOND if end_case else MID_SECOND):
                second_product()

        counts.append(sent)

    @pl.when(end)
    def _():
        gather(True)

    @pl.when(jnp.logical_not(end))
    def _():
        gather(False)

    def last_source(dx, dy, k):
        place = jnp.where(end, 1, 0) if isinstance(k, int) else k
        return (1 - x) if dx else x, (1 - y) if dy else y, jnp.where(upper, 3 - place, place)

    def more_of(places):
        @pl.when(x != y)
        def _():
            for start in range(0, HALF, 256):
                more[1 - y, :, start:start + 256] += partial(places, start, last_source)

    last_is_second = end & jnp.logical_not(flipped)
    early, late = jnp.where(last_is_second, 3, 2), jnp.where(last_is_second, 2, 3)
    await_mate([(1, 1, early)], last_source)
    first_product([(1, 1, early)], False, last_source)
    more_of((1, early))
    await_mate([(1, 1, late)], last_source)
    more_of((late,))
    first_product([(1, 1, late)], False, last_source)
    for start in range(0, HALF, 256):
        grown = total[1 - y, :, start:start + 256] + rows[0, 1 - y, :, start:start + 256].astype(jnp.float32)
        rows[1, 1 - y, :, start:start + 256] = jnp.minimum(grown, 1.0).astype(jnp.bfloat16)

    known = pl.ds(pl.multiple_of((1 - y) * HALF, HALF), HALF)
    for half in range(2):
        for start in range(0, HALF, 256):
            product = jnp.dot(
                rows[1, 1 - y], reach[half, known, start:start + 256], preferred_element_type=jnp.float32
            )
            grown = product + more[half, :, start:start + 256] + rows[1, half, :, start:start + 256].astype(jnp.float32)
            rows[0, half, :, start:start + 256] = jnp.minimum(grown, 1.0).astype(jnp.bfloat16)

    def block(now, half, start, width=256):
        known = jnp.concatenate([rows[now, 0], rows[now, 1]], axis=1)
        product = jnp.dot(known, reach[half, :, start:start + width], preferred_element_type=jnp.float32)
        old = rows[now, half, :, start:start + width].astype(jnp.float32)
        return jnp.minimum(product + old, 1.0).astype(jnp.bfloat16)

    def step(now):
        for half in range(2):
            rows[1 - now, half] = block(now, half, 0, HALF)

    for count in range(STEPS - 3):
        step(count % 2)

    for start in range(0, HALF, 1024):
        out_ref[:, start:start + 1024] = block(0, y, start, 1024)

    def drain(p, count, semaphore):
        ref = reach.at[0, pl.ds(0, count * PIECES[p][2]), :]
        pltpu.make_async_remote_copy(
            src_ref=ref, dst_ref=ref, send_sem=semaphore, recv_sem=semaphore, device_id=mate, device_id_type=MESH
        ).wait_send()

    def drain_all(sent):
        for p in range(len(PIECES)):
            drain(p, sent[p], send_sem.at[p])
            drain(p, 16, pass_sem.at[p])

    @pl.when(end)
    def _():
        drain_all(counts[0])

    @pl.when(jnp.logical_not(end))
    def _():
        drain_all(counts[1])


def solution(mesh):
    layout = P(('row', 'depth'), 'col')
    sends = len(PIECES)

    def local(slab):
        return pl.pallas_call(
            kernel,
            out_shape=pltpu.VMEM((SLAB, HALF), jnp.bfloat16),
            in_specs=[pl.BlockSpec(memory_space=pl.ANY)],
            out_specs=pl.BlockSpec(memory_space=pltpu.VMEM),
            scratch_shapes=[
                pltpu.VMEM((2, N, HALF), jnp.bfloat16),
                pltpu.VMEM((2, 2, SLAB, HALF), jnp.bfloat16),
                pltpu.VMEM((2, SLAB, HALF), jnp.float32),
                pltpu.VMEM((2, SLAB, HALF), jnp.float32),
                pltpu.SemaphoreType.DMA,
                pltpu.SemaphoreType.DMA((sends,)),
                pltpu.SemaphoreType.DMA((sends, 2, 2, 4)),
                pltpu.SemaphoreType.DMA((sends,)),
                pltpu.SemaphoreType.DMA((sends, 2, 2, 4)),
                pltpu.SemaphoreType.REGULAR,
            ],
            compiler_params=pltpu.CompilerParams(collective_id=0, has_side_effects=True),
        )(slab)

    return jax.shard_map(local, mesh=mesh, in_specs=(layout,), out_specs=layout, check_vma=False)
```
